32 devices in a mesh: sims: 2 (over x), rows: 4 (over y, core), fields: 4 (over z).
Axes of the slice: x: 2, y: 2, z: 4, core: 2. Of those that a mesh axis runs over, the one named last changes fastest.
Arguments:
- sky_maps: float32 [6, 32, 16384], P('sims', 'rows', 'fields'), parts along dimension 0, may hold values from -7 to 7
- band_cuts: int32 [6], replicated, may hold values from 1 to 8191, as said below
- filters: float32 [3, 32, 16384], P(None, ('rows', 'fields')), may hold values from 0.3 to 3
- wiener: float32 [2, 32, 16384], P(None, ('rows', 'fields')), may hold values from 0.3 to 3
- response: float32 [32, 16384], P(('rows', 'fields')), may hold values from 0.5 to 2
Outputs:
- phi_curl: float32 [4, 32, 16384], P('sims', 'rows', 'fields'), parts along dimension 0
The draws below stay inside these ranges and needn't reach their ends.
There are 2 independent parts, one for each index of `sims`. The reference program is written for one: setup_inputs(seed, part) draws one part's arguments, and reference() takes and returns one part's arrays. A program takes and returns all parts, laid end to end along the dimension named above; an argument that names none is the same for every part. Nothing has to cross between parts.
Inputs may be any that keep to these rules, and one draw needn't show every extreme that they name: `band_cuts`: entries 0, 2 and 4 are the smallest multipole indices of the temperature, polarization and estimate bands and lie below 512; entries 1, 3 and 5 are the largest and are at least 4096.
All inputs are finite; a program needn't handle non-finite values.
Results may differ from the reference program's by a relative error of at most 0.00019.
Values sent between devices are 32-bit elements; how exact they have to be, the bound alone decides.
A program may use at most 128 MiB of HBM per device.

```python
import math
import jax
import jax.numpy as jnp

NC = 16384
NR = 32


def draw_sky_maps(key, part):
    rough_part = jax.random.normal(key, (3, NR, NC), jnp.float32)
    return jnp.clip(rough_part, -7.0, 7.0)


def draw_band_cuts(key, part):
    low_key = jax.random.fold_in(key, 3)
    high_key = jax.random.fold_in(key, 5)
    lowest = jax.random.randint(low_key, (3,), 1, max(2, NC // 32), dtype=jnp.int32)
    highest = jax.random.randint(high_key, (3,), NC // 4, NC // 2, dtype=jnp.int32)
    return jnp.stack([lowest, highest], axis=1).reshape(6)


def steps_of(own_key, shape, split, smallest, top_value):
    factor_of, own = 1.0, jax.random.fold_in(own_key, 6)
    for dim, parts in split:
        heights = jnp.exp(jax.random.uniform(jax.random.fold_in(own, dim), (parts,), jnp.float32, smallest / len(split), top_value / len(split)))
        factor_of = factor_of * jnp.repeat(heights, shape[dim] // parts).reshape([-1 if axis == dim else 1 for axis in range(len(shape))])
    return factor_of


def setup_inputs(seed: int = 0, part: int = 0) -> dict:
    keys = jax.random.split(jax.random.key(seed), 6)
    own_keys = jax.random.split(jax.random.fold_in(keys[5], part), 6)
    return {
        "sky_maps": draw_sky_maps(jax.random.fold_in(jax.random.fold_in(keys[5], part), 71), part),
        "band_cuts": draw_band_cuts(jax.random.fold_in(keys[5], 71), part),
        "filters": jnp.clip(jnp.exp(math.log(3.0) - 2.3025851 * jax.random.uniform(keys[2], (3, NR, NC), jnp.float32) ** steps_of(keys[2], (3, NR, NC), ((1, 16),), -0.2, 0.2)), 0.3, 3.0),
        "wiener": jnp.clip(jnp.exp(math.log(3.0) - 2.3025851 * jax.random.uniform(keys[3], (2, NR, NC), jnp.float32) ** steps_of(keys[3], (2, NR, NC), ((1, 16),), -0.2, 0.2)), 0.3, 3.0),
        "response": jnp.clip(jnp.exp(math.log(2.0) - 1.3862944 * jax.random.uniform(keys[4], (NR, NC), jnp.float32) ** steps_of(keys[4], (NR, NC), ((0, 16),), -0.2, 0.2)), 0.5, 2.0),
    }


def signed_index(length):
    indices = jnp.arange(length, dtype=jnp.int32)
    return jnp.where(indices < length // 2, indices, indices - length)


def reference(sky_maps, band_cuts, filters, wiener, response):
    row_ratio = NC // NR
    freq_rows = signed_index(NR)[:, None]
    freq_cols = signed_index(NC)[None, :]
    scaled_rows = row_ratio * freq_rows
    radius_sq = freq_cols * freq_cols + scaled_rows * scaled_rows

    def band_mask(lower_cut, upper_cut):
        inside = (radius_sq >= lower_cut * lower_cut) & (radius_sq <= upper_cut * upper_cut)
        return inside.astype(jnp.float32)

    mask_temp = band_mask(band_cuts[0], band_cuts[1])
    mask_pol = band_mask(band_cuts[2], band_cuts[3])
    mask_out = band_mask(band_cuts[4], band_cuts[5])
    radius_floor = jnp.maximum(radius_sq, 1).astype(jnp.float32)
    cos_two = (freq_cols * freq_cols - scaled_rows * scaled_rows).astype(jnp.float32) / radius_floor
    sin_two = (2 * freq_cols * scaled_rows).astype(jnp.float32) / radius_floor
    along_x = (2 * freq_cols).astype(jnp.float32) / NC
    along_y = (2 * freq_rows).astype(jnp.float32) / NR
    spectra = jnp.fft.fft2(sky_maps)
    temp_modes = spectra[0]
    stokes_q = spectra[1]
    stokes_u = spectra[2]
    e_modes = -(cos_two * stokes_q + sin_two * stokes_u)
    b_modes = sin_two * stokes_q - cos_two * stokes_u
    temp_bar = mask_temp * filters[0] * temp_modes
    e_bar = mask_pol * filters[1] * e_modes
    b_bar = mask_pol * filters[2] * b_modes
    rotation = cos_two + 1j * sin_two
    raising = 1j * (along_x + 1j * along_y)
    lowering = 1j * (along_x - 1j * along_y)
    pol_wiener = -(wiener[1] * e_bar) * rotation
    leg_spectra = jnp.stack([
        temp_bar,
        raising * (wiener[0] * temp_bar),
        -(e_bar + 1j * b_bar) * rotation,
        raising * pol_wiener,
        lowering * pol_wiener,
    ])
    leg_maps = jnp.fft.ifft2(leg_spectra)
    current = leg_maps[0] * leg_maps[1] + 0.5 * (jnp.conj(leg_maps[2]) * leg_maps[3] + leg_maps[2] * jnp.conj(leg_maps[4]))
    estimate = jnp.fft.ifft2(mask_out * response * (lowering * jnp.fft.fft2(current)))
    return jnp.stack([jnp.real(estimate), jnp.imag(estimate)]).astype(jnp.float32)
```

```python
import functools
import math

import jax
import jax.numpy as jnp
import numpy as np
from jax import lax
from jax.experimental import pallas as pl
from jax.experimental.pallas import tpu as pltpu
from jax.sharding import PartitionSpec as P

NC = 16384


exact_mode = lax.Precision.HIGHEST


def split_factor(length):
    best_first = 1
    for divisor in range(1, math.isqrt(length) + 1):
        if length % divisor == 0:
            best_first = divisor
    return (best_first, length // best_first)


def phase_table(left_index, right_index, period, direction):
    product = left_index[:, None] * right_index[None, :] % period
    angles = direction * 2.0 * math.pi / period * product.astype(jnp.float32)
    return (jnp.cos(angles), jnp.sin(angles))


def complex_einsum(formula, data_pair, table_pair):
    data_real, data_imag = data_pair
    table_real, table_imag = table_pair
    real_out = jnp.einsum(formula, data_real, table_real, precision=exact_mode)
    imag_out = jnp.einsum(formula, data_real, table_imag, precision=exact_mode)
    if data_imag is not None:
        real_out = real_out - jnp.einsum(formula, data_imag, table_imag, precision=exact_mode)
        imag_out = imag_out + jnp.einsum(formula, data_imag, table_real, precision=exact_mode)
    return (real_out, imag_out)


def complex_mul(left_pair, right_pair):
    return (
        left_pair[0] * right_pair[0] - left_pair[1] * right_pair[1],
        left_pair[0] * right_pair[1] + left_pair[1] * right_pair[0],
    )


def conj_mul(left_pair, right_pair):
    return (
        left_pair[0] * right_pair[0] + left_pair[1] * right_pair[1],
        left_pair[0] * right_pair[1] - left_pair[1] * right_pair[0],
    )


def row_transform(data_pair, direction):
    batch_len, length, block_width = data_pair[0].shape
    outer_len, inner_len = split_factor(length)
    outer_ids = jnp.arange(outer_len, dtype=jnp.int32)
    inner_ids = jnp.arange(inner_len, dtype=jnp.int32)
    real_in = data_pair[0].reshape(batch_len, outer_len, inner_len, block_width)
    imag_in = None
    if data_pair[1] is not None:
        imag_in = data_pair[1].reshape(batch_len, outer_len, inner_len, block_width)
    middle = complex_einsum(
        "bjmc,jk->bkmc", (real_in, imag_in), phase_table(outer_ids, outer_ids, outer_len, direction)
    )
    twiddle = phase_table(outer_ids, inner_ids, length, direction)
    middle = complex_mul(middle, (twiddle[0][None, :, :, None], twiddle[1][None, :, :, None]))
    result = complex_einsum(
        "bkmc,mq->bqkc", middle, phase_table(inner_ids, inner_ids, inner_len, direction)
    )
    norm_factor = 1.0 if direction < 0 else 1.0 / length
    return (
        result[0].reshape(batch_len, length, block_width) * norm_factor,
        result[1].reshape(batch_len, length, block_width) * norm_factor,
    )


def block_order(groups, fields_count):
    positions = jnp.arange(groups, dtype=jnp.int32)
    blocks = positions % fields_count * (groups // fields_count) + positions // fields_count
    return (positions, blocks)


def column_forward(data_pair, groups, fields_count):
    batch_len, local_rows, total_len = data_pair[0].shape
    block_width = total_len // groups
    positions, blocks = block_order(groups, fields_count)
    column_ids = jnp.arange(block_width, dtype=jnp.int32)
    shaped = (
        data_pair[0].reshape(batch_len, local_rows, groups, block_width),
        data_pair[1].reshape(batch_len, local_rows, groups, block_width),
    )
    middle = complex_einsum("brpc,pk->brkc", shaped, phase_table(blocks, positions, groups, -1.0))
    twiddle = phase_table(positions, column_ids, total_len, -1.0)
    middle = complex_mul(middle, (twiddle[0][None, None], twiddle[1][None, None]))
    result = complex_einsum(
        "brkc,cq->brqk", middle, phase_table(column_ids, column_ids, block_width, -1.0)
    )
    return (
        result[0].reshape(batch_len, local_rows, total_len),
        result[1].reshape(batch_len, local_rows, total_len),
    )


def column_inverse(data_pair, groups, fields_count):
    batch_len, local_rows, total_len = data_pair[0].shape
    block_width = total_len // groups
    positions, blocks = block_order(groups, fields_count)
    column_ids = jnp.arange(block_width, dtype=jnp.int32)
    shaped = (
        data_pair[0].reshape(batch_len, local_rows, block_width, groups),
        data_pair[1].reshape(batch_len, local_rows, block_width, groups),
    )
    middle = complex_einsum(
        "brqk,qc->brkc", shaped, phase_table(column_ids, column_ids, block_width, 1.0)
    )
    twiddle = phase_table(positions, column_ids, total_len, 1.0)
    middle = complex_mul(middle, (twiddle[0][None, None], twiddle[1][None, None]))
    result = complex_einsum("brkc,kp->brpc", middle, phase_table(positions, blocks, groups, 1.0))
    norm_factor = 1.0 / total_len
    return (
        result[0].reshape(batch_len, local_rows, total_len) * norm_factor,
        result[1].reshape(batch_len, local_rows, total_len) * norm_factor,
    )


def body(sky_maps, band_cuts, filters, wiener, response):
    rows_count = lax.axis_size("rows")
    fields_count = lax.axis_size("fields")
    groups = rows_count * fields_count
    local_rows = filters.shape[1]
    total_rows = local_rows * groups
    row_ratio = NC // total_rows

    def forward_columns(stacked):
        return jnp.stack(column_forward((stacked[0], stacked[1]), groups, fields_count))

    def inverse_rows(stacked):
        return jnp.stack(row_transform((stacked[0], stacked[1]), 1.0))

    def inverse_columns(stacked):
        return jnp.stack(column_inverse((stacked[0], stacked[1]), groups, fields_count))

    def to_frequency(stacked):
        batch_len = stacked.shape[1]
        block_width = stacked.shape[3]
        shaped = stacked.reshape(
            2, batch_len, rows_count, fields_count, local_rows, 1, 1, block_width
        )
        arrived = lax.all_to_all(
            lax.all_to_all(shaped, "rows", split_axis=2, concat_axis=5, tiled=True),
            "fields",
            split_axis=3,
            concat_axis=6,
            tiled=True,
        )
        result = forward_columns(arrived.reshape(2, batch_len, local_rows, groups * block_width))
        return result

    def to_space(stacked):
        batch_len = stacked.shape[1]
        block_width = stacked.shape[3] // groups
        shaped = stacked.reshape(
            2, batch_len, 1, 1, local_rows, rows_count, fields_count, block_width
        )
        arrived = lax.all_to_all(
            lax.all_to_all(shaped, "rows", split_axis=5, concat_axis=2, tiled=True),
            "fields",
            split_axis=6,
            concat_axis=3,
            tiled=True,
        )
        result = inverse_rows(arrived.reshape(2, batch_len, total_rows, block_width))
        return result

    slab_spectra = jnp.stack(
        row_transform(
            (lax.all_to_all(sky_maps, "rows", split_axis=2, concat_axis=1, tiled=True), None), -1.0
        )
    )
    sky_spectra = to_frequency(slab_spectra)
    row_ids = lax.axis_index(("rows", "fields")) * local_rows + jnp.arange(
        local_rows, dtype=jnp.int32
    )
    freq_rows = jnp.where(row_ids < total_rows // 2, row_ids, row_ids - total_rows)[:, None]
    column_ids = jnp.arange(NC, dtype=jnp.int32)
    freq_cols = jnp.where(column_ids < NC // 2, column_ids, column_ids - NC)[None, :]
    scaled_rows = row_ratio * freq_rows
    radius_sq = freq_cols * freq_cols + scaled_rows * scaled_rows

    def band_mask(lower_cut, upper_cut):
        inside = (radius_sq >= lower_cut * lower_cut) & (radius_sq <= upper_cut * upper_cut)
        return inside.astype(jnp.float32)

    mask_temp = band_mask(band_cuts[0], band_cuts[1])
    mask_pol = band_mask(band_cuts[2], band_cuts[3])
    mask_out = band_mask(band_cuts[4], band_cuts[5])
    radius_floor = jnp.maximum(radius_sq, 1).astype(jnp.float32)
    cos_two = (freq_cols * freq_cols - scaled_rows * scaled_rows).astype(jnp.float32) / radius_floor
    sin_two = (2 * freq_cols * scaled_rows).astype(jnp.float32) / radius_floor
    along_x = (2 * freq_cols).astype(jnp.float32) / NC
    along_y = (2 * freq_rows).astype(jnp.float32) / total_rows
    raising = (-along_y + 0.0 * along_x, along_x + 0.0 * along_y)
    lowering = (along_y + 0.0 * along_x, along_x + 0.0 * along_y)
    rotation = (cos_two, sin_two)
    temp_modes = (sky_spectra[0, 0], sky_spectra[1, 0])
    stokes_q = (sky_spectra[0, 1], sky_spectra[1, 1])
    stokes_u = (sky_spectra[0, 2], sky_spectra[1, 2])
    e_modes = (
        -(cos_two * stokes_q[0] + sin_two * stokes_u[0]),
        -(cos_two * stokes_q[1] + sin_two * stokes_u[1]),
    )
    b_modes = (
        sin_two * stokes_q[0] - cos_two * stokes_u[0],
        sin_two * stokes_q[1] - cos_two * stokes_u[1],
    )
    temp_weight = mask_temp * filters[0]
    e_weight = mask_pol * filters[1]
    b_weight = mask_pol * filters[2]
    temp_bar = (temp_weight * temp_modes[0], temp_weight * temp_modes[1])
    e_bar = (e_weight * e_modes[0], e_weight * e_modes[1])
    b_bar = (b_weight * b_modes[0], b_weight * b_modes[1])
    grad_temp = complex_mul(raising, (wiener[0] * temp_bar[0], wiener[0] * temp_bar[1]))
    pol_sum = complex_mul((e_bar[0] - b_bar[1], e_bar[1] + b_bar[0]), rotation)
    pol_bar = (-pol_sum[0], -pol_sum[1])
    pol_rot = complex_mul((wiener[1] * e_bar[0], wiener[1] * e_bar[1]), rotation)
    pol_wiener = (-pol_rot[0], -pol_rot[1])
    spin_three = complex_mul(raising, pol_wiener)
    spin_one = complex_mul(lowering, pol_wiener)
    leg_spectra = jnp.stack(
        [
            jnp.stack([temp_bar[0], grad_temp[0], pol_bar[0], spin_three[0], spin_one[0]]),
            jnp.stack([temp_bar[1], grad_temp[1], pol_bar[1], spin_three[1], spin_one[1]]),
        ]
    )
    leg_maps = to_space(inverse_columns(leg_spectra))
    temp_leg = (leg_maps[0, 0], leg_maps[1, 0])
    grad_leg = (leg_maps[0, 1], leg_maps[1, 1])
    pol_leg = (leg_maps[0, 2], leg_maps[1, 2])
    three_leg = (leg_maps[0, 3], leg_maps[1, 3])
    one_leg = (leg_maps[0, 4], leg_maps[1, 4])
    temp_term = complex_mul(temp_leg, grad_leg)
    raise_term = conj_mul(pol_leg, three_leg)
    lower_term = conj_mul(one_leg, pol_leg)
    current = (
        temp_term[0] + 0.5 * (raise_term[0] + lower_term[0]),
        temp_term[1] + 0.5 * (raise_term[1] + lower_term[1]),
    )
    current_rows = jnp.stack(row_transform((current[0][None], current[1][None]), -1.0))
    current_modes = to_frequency(current_rows)
    out_weight = mask_out * response
    estimate_modes = complex_mul(
        lowering, (out_weight * current_modes[0, 0], out_weight * current_modes[1, 0])
    )
    estimate_stack = jnp.stack([estimate_modes[0][None], estimate_modes[1][None]])
    estimate_maps = to_space(inverse_columns(estimate_stack))
    slab_result = estimate_maps[:, 0]
    return lax.all_to_all(slab_result, "rows", split_axis=1, concat_axis=2, tiled=True)


SIDE = 128
TILE = (8, 128)
LEG_GROUPS = ((0, 2), (2, 2), (4, 1))
MESH = pl.DeviceIdType.MESH


def add_pair(a, b):
    imag = a[1] if b[1] is None else b[1] if a[1] is None else a[1] + b[1]
    return (a[0] + b[0], imag)


def sub_pair(a, b):
    imag = a[1] if b[1] is None else -b[1] if a[1] is None else a[1] - b[1]
    return (a[0] - b[0], imag)


def turn_pair(value, step, length, direction):
    real, imag = value
    if step == 0:
        return value
    if 4 * step == length:
        if imag is None:
            return (jnp.zeros_like(real), real if direction > 0 else -real)
        return (-imag, real) if direction > 0 else (imag, -real)
    angle = 2.0 * math.pi * step / length
    c, s = math.cos(angle), direction * math.sin(angle)
    if imag is None:
        return (real * c, real * s)
    if 8 * step == length:
        if direction > 0:
            return ((real - imag) * c, (real + imag) * c)
        return ((real + imag) * c, (imag - real) * c)
    if 8 * step == 3 * length:
        if direction > 0:
            return ((real + imag) * c, (imag - real) * c)
        return ((real - imag) * c, (real + imag) * c)
    return (real * c - imag * s, real * s + imag * c)


def short_transform(values, direction):
    length = len(values)
    if length == 1:
        return values
    even = short_transform(values[0::2], direction)
    odd = short_transform(values[1::2], direction)
    low, high = [], []
    for step in range(length // 2):
        turned = turn_pair(odd[step], step, length, direction)
        low.append(add_pair(even[step], turned))
        high.append(sub_pair(even[step], turned))
    return low + high


def split_number(x):
    top = x.astype(jnp.bfloat16)
    return top, (x - top.astype(jnp.float32)).astype(jnp.bfloat16)


def dot32(a, b):
    return jnp.dot(a, b, preferred_element_type=jnp.float32)


def matrix_left(table_ref, which, x):
    top, rest = split_number(x)
    m_top, m_rest = table_ref[which, 0], table_ref[which, 1]
    return dot32(m_top, top) + (dot32(m_top, rest) + dot32(m_rest, top))


def matrix_right(table_ref, which, x):
    top, rest = split_number(x)
    m_top, m_rest = table_ref[which, 0], table_ref[which, 1]
    return dot32(top, m_top) + (dot32(top, m_rest) + dot32(rest, m_top))


BITS = (0, 1)
OFFSETS = [
    (c, a1, e, a0) for a0 in BITS for c, a1, e in
    ((1, 1, 1), (1, 0, 0), (0, 1, 0), (0, 0, 1), (1, 1, 0), (0, 1, 1), (1, 0, 1), (0, 0, 0))
]
PEERS = [offset for offset in OFFSETS if any(offset)]
WEIGHT_ORDER = (0, 3, 1, 2, 4, 5)


def lens_kernel(
    cuts_ref, sky_hbm, filters_hbm, wiener_hbm, response_hbm, table_ref, twiddle_ref, out_ref,
    sky_ref, raw, weight_ref, slab_out, slab_in, relay_buf, spec_out, spec_in, weights, legs_out, legs_in,
    maps, current, cur_out, cur_in, est_out, est_in, fin_out, fin_in,
    slab_sem, relay_sem, forward_sem, spec_sem, weight_sem, legs_sem, cur_sem, est_sem, fin_sem, self_sem, load_sem,
):
    rows_count, fields_count, local_rows = 4, 4, 2
    groups = rows_count * fields_count
    total_rows = groups * local_rows
    in_rows = total_rows // rows_count
    row_ratio = NC // total_rows
    my_x, my_r, my_z = (lax.axis_index(name) for name in ("sims", "rows", "fields"))
    my_y, my_c, my_h, my_l = my_r // 2, my_r % 2, my_z // 2, my_z % 2
    x_at, y_at, c_at, h_at, l_at = ((bit, 1 - bit) for bit in (my_x, my_y, my_c, my_h, my_l))
    me = my_r * fields_count + 2 * my_x + my_l
    my_block = (2 * my_x + my_l) * rows_count + my_r
    stays = my_x == my_h

    def row_of(offset):
        return 2 * y_at[offset[1]] + c_at[offset[3]]

    def peer_of(offset):
        return row_of(offset) * fields_count + 2 * x_at[offset[0]] + l_at[offset[2]]

    def peer_block(offset):
        return (2 * x_at[offset[0]] + l_at[offset[2]]) * rows_count + row_of(offset)

    def home_source(offset):
        return row_of(offset) * fields_count + 2 * h_at[offset[0]] + l_at[offset[2]]

    def remote(src, dst, sems, x, r, z):
        return pltpu.make_async_remote_copy(
            src_ref=src, dst_ref=dst, send_sem=sems[0], recv_sem=sems[1],
            device_id={"sims": x, "rows": r, "fields": z}, device_id_type=MESH,
        )

    def send(offset, src, dst, sems):
        return remote(src, dst, sems, x_at[offset[0]], row_of(offset), 2 * my_h + l_at[offset[2]])

    def send_home(offset, src, dst, sems):
        return remote(src, dst, sems, my_h, row_of(offset), 2 * x_at[offset[0]] + l_at[offset[2]])

    def each_peer(body):
        for q, offset in enumerate(PEERS):
            body(q, offset)

    loads = [
        pltpu.make_async_copy(src, dst, load_sem.at[n])
        for n, (src, dst) in enumerate((
            (sky_hbm, sky_ref),
            (filters_hbm, raw.at[0:3]),
            (wiener_hbm, raw.at[3:5]),
            (response_hbm, raw.at[5]),
        ))
    ]
    for load in loads:
        load.start()

    barrier = pltpu.get_barrier_semaphore()
    for h in BITS:
        for c, a1, e, a0 in OFFSETS:
            if h or c or a1 or e or a0:
                pl.semaphore_signal(
                    barrier, inc=1, device_id_type=MESH,
                    device_id={"sims": x_at[c], "rows": 2 * y_at[a1] + c_at[a0], "fields": 2 * h_at[h] + l_at[e]},
                )
    loads[0].wait()
    tiles = sky_ref.shape[2] // SIDE
    for field in range(3):
        for t in range(tiles):
            slab_out[t // 8, field, :, t % 8, :] = sky_ref[field, :, t * SIDE:(t + 1) * SIDE]
    pl.semaphore_wait(barrier, 2 * groups - 1)

    ROW_OFFSETS = [(0, a1, 0, a0) for a1 in BITS for a0 in BITS]

    def slab_copy(field, offset, source_row):
        r = row_of(offset)
        return send_home(
            offset, slab_out.at[r, field], slab_in.at[source_row, field],
            (slab_sem.at[0, field, 2 * offset[1] + offset[3]], slab_sem.at[1, field, 2 * offset[1] + offset[3]]),
        )

    def own_slab(field):
        return pltpu.make_async_copy(slab_out.at[my_r, field], slab_in.at[my_r, field], self_sem.at[field])

    def relay_copy(field):
        return remote(
            slab_out.at[pl.ds(2 * y_at[1], 2), field], relay_buf.at[field],
            (relay_sem.at[0, field], relay_sem.at[1, field]), x_at[1], my_r, my_z,
        )

    def forward_copy(field, core):
        a0 = core
        return remote(
            relay_buf.at[field, c_at[a0]], slab_in.at[my_r, field],
            (forward_sem.at[field, a0], slab_sem.at[1, field, 2 + a0]),
            my_x, 2 * y_at[1] + c_at[a0], 2 * h_at[1] + my_l,
        )

    @pl.when(stays)
    def _():
        for field in range(3):
            own_slab(field).start()
            for offset in ROW_OFFSETS[1:]:
                slab_copy(field, offset, my_r).start()

    @pl.when(jnp.logical_not(stays))
    def _():
        for field in range(3):
            relay_copy(field).start()
            for offset in ROW_OFFSETS[:2]:
                slab_copy(field, offset, my_r).start()

    low_index = lax.broadcasted_iota(jnp.int32, (SIDE, SIDE), 0)
    high_index = lax.broadcasted_iota(jnp.int32, (SIDE, SIDE), 1)
    column_ids = low_index + SIDE * high_index
    freq_cols = jnp.where(column_ids < NC // 2, column_ids, column_ids - NC)

    def row_frequency(row):
        row_id = in_rows * my_r + 4 * (my_h + row - 2 * my_h * row) + 2 * my_l + my_x
        return jnp.where(row_id < total_rows // 2, row_id, row_id - total_rows)

    def owner(k):
        return k // 8 * fields_count + 2 * (k % 2) + k // 2 % 2

    def local_row(k, half):
        return 1 - half if k // 4 % 2 else half

    def spec_copy(field, row, q, offset, block):
        return send(
            offset, spec_out.at[field, row, peer_of(offset)], spec_in.at[field, row, :, block],
            (spec_sem.at[0, field, row, q], spec_sem.at[1, field, row, q]),
        )

    def own_spec(field, row):
        return pltpu.make_async_copy(
            spec_out.at[field, row, me], spec_in.at[field, row, :, my_block],
            self_sem.at[3 + field * local_rows + row],
        )

    def spec_start(field, row):
        each_peer(lambda q, offset: spec_copy(field, row, q, offset, my_block).start())
        own_spec(field, row).start()

    def row_step(field, carry):
        @pl.when(stays)
        def _():
            relay_copy(field).wait_recv()
            for core in BITS:
                forward_copy(field, core).start()
            own_slab(field).wait()

        @pl.when(jnp.logical_not(stays))
        def _():
            slab_copy(field, ROW_OFFSETS[0], my_r).wait_recv()

        for offset in ROW_OFFSETS[1:]:
            slab_copy(field, offset, row_of(offset)).wait_recv()
        values = [
            (slab_in[y // in_rows, field, y % in_rows], None) for y in range(total_rows)
        ]
        for k, (real, imag) in enumerate(short_transform(values, -1)):
            spec_out[field, local_row(k, my_h), owner(k), 0] = real
            spec_out[field, local_row(k, my_h), owner(k), 1] = (
                jnp.zeros_like(real) if imag is None else imag
            )
        spec_start(field, 0)
        return carry

    lax.fori_loop(0, 3, row_step, 0)

    def later_rows(field, carry):
        spec_start(field, 1)
        return carry

    lax.fori_loop(0, 3, later_rows, 0)

    for load in loads[1:]:
        load.wait()

    def spread(n, carry):
        for j in range(8):
            start = pl.multiple_of((n * 8 + j) * SIDE, SIDE)
            weight_ref[:, :, n * 8 + j, :] = raw[:, :, pl.ds(start, SIDE)]
        return carry

    lax.fori_loop(0, SIDE // 8, spread, 0)
    scaled_home = row_ratio * row_frequency(0)
    radius_home = freq_cols * freq_cols + scaled_home * scaled_home

    def mask(n):
        low, high = cuts_ref[2 * n], cuts_ref[2 * n + 1]
        inside = (radius_home >= low * low) & (radius_home <= high * high)
        return inside.astype(jnp.float32)

    def weight_copy(n):
        return remote(
            weights.at[n, 0], weights.at[n, 1], (weight_sem.at[0, n], weight_sem.at[1, n]),
            my_x, my_r, 2 * h_at[1] + my_l,
        )

    pol = mask(1)
    weights[0, 0] = mask(0) * weight_ref[0, my_x].T
    weights[1, 0] = pol * weight_ref[1, my_x].T
    weights[2, 0] = pol * weight_ref[2, my_x].T
    weights[3, 0] = weight_ref[3, my_x].T
    weights[4, 0] = weight_ref[4, my_x].T
    weights[5, 0] = mask(2) * weight_ref[5, my_x].T
    for n in WEIGHT_ORDER:
        weight_copy(n).start()

    def spec_wait(row):
        def step(field, carry):
            each_peer(lambda q, offset: spec_copy(field, row, q, offset, peer_block(offset)).wait_recv())
            own_spec(field, row).wait()
            return carry

        lax.fori_loop(0, 3, step, 0)

    cos_f, sin_f, cos_b, sin_b = 0, 1, 2, 3

    def side_by_side(pieces, axis):
        return pieces[0] if len(pieces) == 1 else jnp.concatenate(pieces, axis=axis)

    def long_forward(pieces):
        y = matrix_left(table_ref, 0, side_by_side(pieces, 1))
        c, s = twiddle_ref[cos_f], twiddle_ref[sin_f]
        turned = []
        for n in range(len(pieces)):
            yr, yi = y[:SIDE, n * SIDE:(n + 1) * SIDE], y[SIDE:, n * SIDE:(n + 1) * SIDE]
            turned.append(jnp.concatenate([yr * c - yi * s, yr * s + yi * c], axis=1))
        z = matrix_right(table_ref, 1, side_by_side(turned, 0))
        return [
            (z[n * SIDE:(n + 1) * SIDE, :SIDE], z[n * SIDE:(n + 1) * SIDE, SIDE:])
            for n in range(len(pieces))
        ]

    def long_inverse(pairs):
        stacks = [jnp.concatenate([pair[0], pair[1]], axis=1) for pair in pairs]
        u = matrix_right(table_ref, 0, side_by_side(stacks, 0))
        c, s = twiddle_ref[cos_b], twiddle_ref[sin_b]
        turned = []
        for n in range(len(pairs)):
            ur, ui = u[n * SIDE:(n + 1) * SIDE, :SIDE], u[n * SIDE:(n + 1) * SIDE, SIDE:]
            turned.append(jnp.concatenate([ur * c - ui * s, ur * s + ui * c], axis=0))
        x = matrix_left(table_ref, 1, side_by_side(turned, 1))
        return [
            x[:, n * SIDE:(n + 1) * SIDE].reshape((2, groups) + TILE)
            for n in range(len(pairs))
        ]

    leg_self = 3 + 3 * local_rows

    def legs_copy(row, g, q, offset, source):
        first, count = LEG_GROUPS[g]
        return send(
            offset, legs_out.at[row, first:first + count, :, peer_block(offset)],
            legs_in.at[row, source, first:first + count],
            (legs_sem.at[0, row, g, q], legs_sem.at[1, row, g, q]),
        )

    def own_legs(row, g):
        first, count = LEG_GROUPS[g]
        return pltpu.make_async_copy(
            legs_out.at[row, first:first + count, :, my_block],
            legs_in.at[row, me, first:first + count],
            self_sem.at[leg_self + row * len(LEG_GROUPS) + g],
        )

    def slopes(row):
        along_x = (2 * freq_cols).astype(jnp.float32) / NC
        along_y = (2 * row_frequency(row)).astype(jnp.float32) / total_rows
        return along_x, along_y

    def leg_step(row, carry):
        spec_wait(row)

        @pl.when(row == 1)
        def _():
            for n in WEIGHT_ORDER[:5]:
                weight_copy(n).wait_recv()

        temp, stokes_q, stokes_u = long_forward(
            [spec_in[field, row].reshape(2 * SIDE, SIDE) for field in range(3)]
        )
        scaled = row_ratio * row_frequency(row)
        radius_sq = freq_cols * freq_cols + scaled * scaled
        floor = jnp.maximum(radius_sq, 1).astype(jnp.float32)
        cos2 = (freq_cols * freq_cols - scaled * scaled).astype(jnp.float32) / floor
        sin2 = (2 * freq_cols * scaled).astype(jnp.float32) / floor
        along_x, along_y = slopes(row)
        raising, lowering = (-along_y, along_x), (along_y, along_x)
        rot = (cos2, sin2)
        w_t, w_e, w_b = weights[0, row], weights[1, row], weights[2, row]
        w_gt, w_ge = weights[3, row], weights[4, row]
        t_bar = (w_t * temp[0], w_t * temp[1])
        e_bar = tuple(-w_e * (cos2 * a + sin2 * b) for a, b in zip(stokes_q, stokes_u))
        b_bar = tuple(w_b * (sin2 * a - cos2 * b) for a, b in zip(stokes_q, stokes_u))
        g = complex_mul((w_gt * t_bar[0], w_gt * t_bar[1]), raising)
        p = complex_mul((b_bar[1] - e_bar[0], -(e_bar[1] + b_bar[0])), rot)
        w = complex_mul((-w_ge * e_bar[0], -w_ge * e_bar[1]), rot)
        h3 = complex_mul(w, raising)
        h1 = complex_mul(w, lowering)
        legs = (t_bar, g, p, h3, h1)
        for n, (first, count) in enumerate(LEG_GROUPS):
            for k, leg_map in enumerate(long_inverse(legs[first:first + count])):
                legs_out[row, first + k] = leg_map
            each_peer(lambda q, offset: legs_copy(row, n, q, offset, me).start())
            own_legs(row, n).start()
        return carry

    lax.fori_loop(0, local_rows, leg_step, 0)

    def leg_wait(g):
        def step(row, carry):
            each_peer(lambda q, offset: legs_copy(row, g, q, offset, peer_of(offset)).wait_recv())
            own_legs(row, g).wait()
            return carry

        lax.fori_loop(0, local_rows, step, 0)

    def map_step(n, carry):
        values = [
            (legs_in[local_row(k, my_h), owner(k), n, 0], legs_in[local_row(k, my_h), owner(k), n, 1])
            for k in range(total_rows)
        ]
        for y, (real, imag) in enumerate(short_transform(values, 1)):
            maps[n, 0, y] = real
            maps[n, 1, y] = imag
        return carry

    for g, (first, count) in enumerate(LEG_GROUPS):
        leg_wait(g)
        lax.fori_loop(first, first + count, map_step, 0)

    def product_step(y, carry):
        a, g, p, h3, h1 = [(maps[n, 0, y], maps[n, 1, y]) for n in range(5)]
        ag, ph, hp = complex_mul(a, g), conj_mul(p, h3), conj_mul(h1, p)
        current[0, y] = ag[0] + 0.5 * (ph[0] + hp[0])
        current[1, y] = ag[1] + 0.5 * (ph[1] + hp[1])
        return carry

    lax.fori_loop(0, total_rows, product_step, 0)

    values = [(current[0, y], current[1, y]) for y in range(total_rows)]
    for k, (real, imag) in enumerate(short_transform(values, -1)):
        cur_out[local_row(k, my_h), owner(k), 0] = real
        cur_out[local_row(k, my_h), owner(k), 1] = imag
    cur_self = leg_self + len(LEG_GROUPS) * local_rows
    est_self = cur_self + local_rows

    def cur_copy(row, q, offset, block):
        return send(
            offset, cur_out.at[row, peer_of(offset)], cur_in.at[row, :, block],
            (cur_sem.at[0, row, q], cur_sem.at[1, row, q]),
        )

    def own_cur(row):
        return pltpu.make_async_copy(
            cur_out.at[row, me], cur_in.at[row, :, my_block], self_sem.at[cur_self + row]
        )

    def cur_start(row, carry):
        each_peer(lambda q, offset: cur_copy(row, q, offset, my_block).start())
        own_cur(row).start()
        return carry

    lax.fori_loop(0, local_rows, cur_start, 0)

    def est_copy(row, q, offset, source):
        return send_home(
            offset, est_out.at[row, :, peer_block(offset)], est_in.at[row, source],
            (est_sem.at[0, row, q], est_sem.at[1, row, q]),
        )

    ORIGIN = (0, 0, 0, 0)

    def own_est(row):
        return pltpu.make_async_copy(
            est_out.at[row, :, my_block], est_in.at[row, me], self_sem.at[est_self + row]
        )

    def estimate_step(row, carry):
        each_peer(lambda q, offset: cur_copy(row, q, offset, peer_block(offset)).wait_recv())
        own_cur(row).wait()

        @pl.when(row == 1)
        def _():
            weight_copy(5).wait_recv()

        (modes,) = long_forward([cur_in[row].reshape(2 * SIDE, SIDE)])
        along_x, along_y = slopes(row)
        w = weights[5, row]
        estimate = complex_mul((w * modes[0], w * modes[1]), (along_y, along_x))
        (est_out[row],) = long_inverse([estimate])
        each_peer(lambda q, offset: est_copy(row, q, offset, me).start())

        @pl.when(stays)
        def _():
            own_est(row).start()

        @pl.when(jnp.logical_not(stays))
        def _():
            est_copy(row, groups - 1, ORIGIN, me).start()

        return carry

    lax.fori_loop(0, local_rows, estimate_step, 0)

    def est_wait(row, carry):
        each_peer(lambda q, offset: est_copy(row, q, offset, home_source(offset)).wait_recv())

        @pl.when(stays)
        def _():
            own_est(row).wait()

        @pl.when(jnp.logical_not(stays))
        def _():
            est_copy(row, groups - 1, ORIGIN, home_source(ORIGIN)).wait_recv()

        return carry

    lax.fori_loop(0, local_rows, est_wait, 0)

    values = [
        (est_in[local_row(k, my_x), owner(k), 0], est_in[local_row(k, my_x), owner(k), 1])
        for k in range(total_rows)
    ]
    for y, (real, imag) in enumerate(short_transform(values, 1)):
        fin_out[y // in_rows, 0, y % in_rows] = real
        fin_out[y // in_rows, 1, y % in_rows] = imag

    def fin_copy(q, offset, source_row):
        r = row_of(offset)
        return remote(
            fin_out.at[r], fin_in.at[source_row], (fin_sem.at[0, q], fin_sem.at[1, q]), my_x, r, my_z
        )

    for q, offset in enumerate(ROW_OFFSETS[1:]):
        fin_copy(q, offset, my_r).start()
    own_fin = pltpu.make_async_copy(
        fin_out.at[my_r], fin_in.at[my_r], self_sem.at[est_self + local_rows]
    )
    own_fin.start()

    @pl.when(stays)
    def _():
        for field in range(3):
            for offset in ROW_OFFSETS[1:]:
                slab_copy(field, offset, my_r).wait_send()
            for core in BITS:
                forward_copy(field, core).wait_send()

    @pl.when(jnp.logical_not(stays))
    def _():
        for field in range(3):
            relay_copy(field).wait_send()
            for offset in ROW_OFFSETS[:2]:
                slab_copy(field, offset, my_r).wait_send()
        for row in range(local_rows):
            est_copy(row, groups - 1, ORIGIN, me).wait_send()

    for n in WEIGHT_ORDER:
        weight_copy(n).wait_send()

    def sends_left(row, carry):
        def spec_left(field, inner):
            each_peer(lambda q, offset: spec_copy(field, row, q, offset, my_block).wait_send())
            return inner

        lax.fori_loop(0, 3, spec_left, 0)
        for g in range(len(LEG_GROUPS)):
            each_peer(lambda q, offset: legs_copy(row, g, q, offset, me).wait_send())
        each_peer(lambda q, offset: cur_copy(row, q, offset, my_block).wait_send())
        each_peer(lambda q, offset: est_copy(row, q, offset, me).wait_send())
        return carry

    lax.fori_loop(0, local_rows, sends_left, 0)
    for q, offset in enumerate(ROW_OFFSETS[1:]):
        fin_copy(q, offset, row_of(offset)).wait_recv()
    own_fin.wait()
    for part in range(2):
        for t in range(tiles):
            out_ref[part, :, t * SIDE:(t + 1) * SIDE] = fin_in[t // 8, part, :, t % 8, :]

    for q, offset in enumerate(ROW_OFFSETS[1:]):
        fin_copy(q, offset, my_r).wait_send()


def long_tables(total_rows):
    index = np.arange(SIDE)
    angle = 2.0 * np.pi * (index[:, None] * index[None, :] % SIDE) / SIDE
    c, s = np.cos(angle), np.sin(angle)
    forward = np.block([[c, s], [-s, c]]).astype(np.float32)
    tables = np.stack([forward, forward.T])
    top = tables.astype(jnp.bfloat16)
    rest = (tables - top.astype(np.float32)).astype(jnp.bfloat16)
    turn = 2.0 * np.pi * (index[:, None] * index[None, :]) / NC
    scale = 1.0 / (NC * total_rows)
    twiddle = np.stack(
        [np.cos(turn), -np.sin(turn), scale * np.cos(turn), scale * np.sin(turn)]
    ).astype(np.float32)
    return np.stack([top, rest], axis=1), twiddle


def fused_body(rows_count, fields_count, sky_maps, band_cuts, filters, wiener, response):
    groups = rows_count * fields_count
    local_rows = response.shape[0]
    total_rows = local_rows * groups
    in_rows = total_rows // rows_count
    table, twiddle = long_tables(total_rows)
    vmem = pl.BlockSpec(memory_space=pltpu.VMEM)
    f32 = jnp.float32
    dma = pltpu.SemaphoreType.DMA
    slab = pltpu.VMEM((rows_count, 3, in_rows) + TILE, f32)
    chunk = pltpu.VMEM((local_rows, groups, 2) + TILE, f32)
    lines = pltpu.VMEM((local_rows, 2, groups) + TILE, f32)
    final = pltpu.VMEM((rows_count, 2, in_rows) + TILE, f32)
    return pl.pallas_call(
        lens_kernel,
        out_shape=jax.ShapeDtypeStruct((2,) + sky_maps.shape[1:], f32),
        in_specs=[pl.BlockSpec(memory_space=pltpu.SMEM)]
        + [pl.BlockSpec(memory_space=pl.ANY)] * 4
        + [vmem] * 2,
        out_specs=vmem,
        scratch_shapes=[
            pltpu.VMEM(sky_maps.shape, f32),
            pltpu.VMEM((6, local_rows, NC), f32),
            pltpu.VMEM((6, local_rows, SIDE, SIDE), f32),
            slab, slab,
            pltpu.VMEM((3, 2, in_rows) + TILE, f32),
            pltpu.VMEM((3, local_rows, groups, 2) + TILE, f32),
            pltpu.VMEM((3, local_rows, 2, groups) + TILE, f32),
            pltpu.VMEM((6, local_rows, SIDE, SIDE), f32),
            pltpu.VMEM((local_rows, 5, 2, groups) + TILE, f32),
            pltpu.VMEM((local_rows, groups, 5, 2) + TILE, f32),
            pltpu.VMEM((5, 2, total_rows) + TILE, f32),
            pltpu.VMEM((2, total_rows) + TILE, f32),
            chunk, lines, lines, chunk, final, final,
            dma((2, 3, rows_count)), dma((2, 3)), dma((3, 2)), dma((2, 3, local_rows, groups - 1)), dma((2, 6)),
            dma((2, local_rows, len(LEG_GROUPS), groups - 1)),
            dma((2, local_rows, groups - 1)), dma((2, local_rows, groups)),
            dma((2, rows_count)), dma((4 + (5 + len(LEG_GROUPS)) * local_rows,)),
            dma((4,)),
        ],
        compiler_params=pltpu.CompilerParams(
            collective_id=0, has_side_effects=True, vmem_limit_bytes=60 * 1024 * 1024
        ),
        name="lens",
    )(band_cuts, sky_maps, filters, wiener, response, jnp.asarray(table), jnp.asarray(twiddle))


def solution(mesh):
    placed = (
        P("sims", "rows", "fields"),
        P(),
        P(None, ("rows", "fields"), None),
        P(None, ("rows", "fields"), None),
        P(("rows", "fields"), None),
    )
    rows_count, fields_count = mesh.shape["rows"], mesh.shape["fields"]
    groups = rows_count * fields_count

    def choose(sky_maps, *rest):
        fits = (
            NC == SIDE * SIDE
            and (mesh.shape["sims"], rows_count, fields_count) == (2, 4, 4)
            and NC // groups == TILE[0] * TILE[1]
            and sky_maps.shape[0] == 3
            and sky_maps.shape[1] * rows_count == 32
        )
        if fits:
            return fused_body(rows_count, fields_count, sky_maps, *rest)
        return body(sky_maps, *rest)

    return jax.shard_map(
        choose, mesh=mesh, in_specs=placed, out_specs=P("sims", "rows", "fields"), check_vma=False
    )
```

```python
import functools
import math

import jax
import jax.numpy as jnp
import numpy as np
from jax import lax
from jax.experimental import pallas as pl
from jax.experimental.pallas import tpu as pltpu
from jax.sharding import PartitionSpec as P

NC = 16384


exact_mode = lax.Precision.HIGHEST


def split_factor(length):
    best_first = 1
    for divisor in range(1, math.isqrt(length) + 1):
        if length % divisor == 0:
            best_first = divisor
    return (best_first, length // best_first)


def phase_table(left_index, right_index, period, direction):
    product = left_index[:, None] * right_index[None, :] % period
    angles = direction * 2.0 * math.pi / period * product.astype(jnp.float32)
    return (jnp.cos(angles), jnp.sin(angles))


def complex_einsum(formula, data_pair, table_pair):
    data_real, data_imag = data_pair
    table_real, table_imag = table_pair
    real_out = jnp.einsum(formula, data_real, table_real, precision=exact_mode)
    imag_out = jnp.einsum(formula, data_real, table_imag, precision=exact_mode)
    if data_imag is not None:
        real_out = real_out - jnp.einsum(formula, data_imag, table_imag, precision=exact_mode)
        imag_out = imag_out + jnp.einsum(formula, data_imag, table_real, precision=exact_mode)
    return (real_out, imag_out)


def complex_mul(left_pair, right_pair):
    return (
        left_pair[0] * right_pair[0] - left_pair[1] * right_pair[1],
        left_pair[0] * right_pair[1] + left_pair[1] * right_pair[0],
    )


def conj_mul(left_pair, right_pair):
    return (
        left_pair[0] * right_pair[0] + left_pair[1] * right_pair[1],
        left_pair[0] * right_pair[1] - left_pair[1] * right_pair[0],
    )


def row_transform(data_pair, direction):
    batch_len, length, block_width = data_pair[0].shape
    outer_len, inner_len = split_factor(length)
    outer_ids = jnp.arange(outer_len, dtype=jnp.int32)
    inner_ids = jnp.arange(inner_len, dtype=jnp.int32)
    real_in = data_pair[0].reshape(batch_len, outer_len, inner_len, block_width)
    imag_in = None
    if data_pair[1] is not None:
        imag_in = data_pair[1].reshape(batch_len, outer_len, inner_len, block_width)
    middle = complex_einsum(
        "bjmc,jk->bkmc", (real_in, imag_in), phase_table(outer_ids, outer_ids, outer_len, direction)
    )
    twiddle = phase_table(outer_ids, inner_ids, length, direction)
    middle = complex_mul(middle, (twiddle[0][None, :, :, None], twiddle[1][None, :, :, None]))
    result = complex_einsum(
        "bkmc,mq->bqkc", middle, phase_table(inner_ids, inner_ids, inner_len, direction)
    )
    norm_factor = 1.0 if direction < 0 else 1.0 / length
    return (
        result[0].reshape(batch_len, length, block_width) * norm_factor,
        result[1].reshape(batch_len, length, block_width) * norm_factor,
    )


def block_order(groups, fields_count):
    positions = jnp.arange(groups, dtype=jnp.int32)
    blocks = positions % fields_count * (groups // fields_count) + positions // fields_count
    return (positions, blocks)


def column_forward(data_pair, groups, fields_count):
    batch_len, local_rows, total_len = data_pair[0].shape
    block_width = total_len // groups
    positions, blocks = block_order(groups, fields_count)
    column_ids = jnp.arange(block_width, dtype=jnp.int32)
    shaped = (
        data_pair[0].reshape(batch_len, local_rows, groups, block_width),
        data_pair[1].reshape(batch_len, local_rows, groups, block_width),
    )
    middle = complex_einsum("brpc,pk->brkc", shaped, phase_table(blocks, positions, groups, -1.0))
    twiddle = phase_table(positions, column_ids, total_len, -1.0)
    middle = complex_mul(middle, (twiddle[0][None, None], twiddle[1][None, None]))
    result = complex_einsum(
        "brkc,cq->brqk", middle, phase_table(column_ids, column_ids, block_width, -1.0)
    )
    return (
        result[0].reshape(batch_len, local_rows, total_len),
        result[1].reshape(batch_len, local_rows, total_len),
    )


def column_inverse(data_pair, groups, fields_count):
    batch_len, local_rows, total_len = data_pair[0].shape
    block_width = total_len // groups
    positions, blocks = block_order(groups, fields_count)
    column_ids = jnp.arange(block_width, dtype=jnp.int32)
    shaped = (
        data_pair[0].reshape(batch_len, local_rows, block_width, groups),
        data_pair[1].reshape(batch_len, local_rows, block_width, groups),
    )
    middle = complex_einsum(
        "brqk,qc->brkc", shaped, phase_table(column_ids, column_ids, block_width, 1.0)
    )
    twiddle = phase_table(positions, column_ids, total_len, 1.0)
    middle = complex_mul(middle, (twiddle[0][None, None], twiddle[1][None, None]))
    result = complex_einsum("brkc,kp->brpc", middle, phase_table(positions, blocks, groups, 1.0))
    norm_factor = 1.0 / total_len
    return (
        result[0].reshape(batch_len, local_rows, total_len) * norm_factor,
        result[1].reshape(batch_len, local_rows, total_len) * norm_factor,
    )


def body(sky_maps, band_cuts, filters, wiener, response):
    rows_count = lax.axis_size("rows")
    fields_count = lax.axis_size("fields")
    groups = rows_count * fields_count
    local_rows = filters.shape[1]
    total_rows = local_rows * groups
    row_ratio = NC // total_rows

    def forward_columns(stacked):
        return jnp.stack(column_forward((stacked[0], stacked[1]), groups, fields_count))

    def inverse_rows(stacked):
        return jnp.stack(row_transform((stacked[0], stacked[1]), 1.0))

    def inverse_columns(stacked):
        return jnp.stack(column_inverse((stacked[0], stacked[1]), groups, fields_count))

    def to_frequency(stacked):
        batch_len = stacked.shape[1]
        block_width = stacked.shape[3]
        shaped = stacked.reshape(
            2, batch_len, rows_count, fields_count, local_rows, 1, 1, block_width
        )
        arrived = lax.all_to_all(
            lax.all_to_all(shaped, "rows", split_axis=2, concat_axis=5, tiled=True),
            "fields",
            split_axis=3,
            concat_axis=6,
            tiled=True,
        )
        result = forward_columns(arrived.reshape(2, batch_len, local_rows, groups * block_width))
        return result

    def to_space(stacked):
        batch_len = stacked.shape[1]
        block_width = stacked.shape[3] // groups
        shaped = stacked.reshape(
            2, batch_len, 1, 1, local_rows, rows_count, fields_count, block_width
        )
        arrived = lax.all_to_all(
            lax.all_to_all(shaped, "rows", split_axis=5, concat_axis=2, tiled=True),
            "fields",
            split_axis=6,
            concat_axis=3,
            tiled=True,
        )
        result = inverse_rows(arrived.reshape(2, batch_len, total_rows, block_width))
        return result

    slab_spectra = jnp.stack(
        row_transform(
            (lax.all_to_all(sky_maps, "rows", split_axis=2, concat_axis=1, tiled=True), None), -1.0
        )
    )
    sky_spectra = to_frequency(slab_spectra)
    row_ids = lax.axis_index(("rows", "fields")) * local_rows + jnp.arange(
        local_rows, dtype=jnp.int32
    )
    freq_rows = jnp.where(row_ids < total_rows // 2, row_ids, row_ids - total_rows)[:, None]
    column_ids = jnp.arange(NC, dtype=jnp.int32)
    freq_cols = jnp.where(column_ids < NC // 2, column_ids, column_ids - NC)[None, :]
    scaled_rows = row_ratio * freq_rows
    radius_sq = freq_cols * freq_cols + scaled_rows * scaled_rows

    def band_mask(lower_cut, upper_cut):
        inside = (radius_sq >= lower_cut * lower_cut) & (radius_sq <= upper_cut * upper_cut)
        return inside.astype(jnp.float32)

    mask_temp = band_mask(band_cuts[0], band_cuts[1])
    mask_pol = band_mask(band_cuts[2], band_cuts[3])
    mask_out = band_mask(band_cuts[4], band_cuts[5])
    radius_floor = jnp.maximum(radius_sq, 1).astype(jnp.float32)
    cos_two = (freq_cols * freq_cols - scaled_rows * scaled_rows).astype(jnp.float32) / radius_floor
    sin_two = (2 * freq_cols * scaled_rows).astype(jnp.float32) / radius_floor
    along_x = (2 * freq_cols).astype(jnp.float32) / NC
    along_y = (2 * freq_rows).astype(jnp.float32) / total_rows
    raising = (-along_y + 0.0 * along_x, along_x + 0.0 * along_y)
    lowering = (along_y + 0.0 * along_x, along_x + 0.0 * along_y)
    rotation = (cos_two, sin_two)
    temp_modes = (sky_spectra[0, 0], sky_spectra[1, 0])
    stokes_q = (sky_spectra[0, 1], sky_spectra[1, 1])
    stokes_u = (sky_spectra[0, 2], sky_spectra[1, 2])
    e_modes = (
        -(cos_two * stokes_q[0] + sin_two * stokes_u[0]),
        -(cos_two * stokes_q[1] + sin_two * stokes_u[1]),
    )
    b_modes = (
        sin_two * stokes_q[0] - cos_two * stokes_u[0],
        sin_two * stokes_q[1] - cos_two * stokes_u[1],
    )
    temp_weight = mask_temp * filters[0]
    e_weight = mask_pol * filters[1]
    b_weight = mask_pol * filters[2]
    temp_bar = (temp_weight * temp_modes[0], temp_weight * temp_modes[1])
    e_bar = (e_weight * e_modes[0], e_weight * e_modes[1])
    b_bar = (b_weight * b_modes[0], b_weight * b_modes[1])
    grad_temp = complex_mul(raising, (wiener[0] * temp_bar[0], wiener[0] * temp_bar[1]))
    pol_sum = complex_mul((e_bar[0] - b_bar[1], e_bar[1] + b_bar[0]), rotation)
    pol_bar = (-pol_sum[0], -pol_sum[1])
    pol_rot = complex_mul((wiener[1] * e_bar[0], wiener[1] * e_bar[1]), rotation)
    pol_wiener = (-pol_rot[0], -pol_rot[1])
    spin_three = complex_mul(raising, pol_wiener)
    spin_one = complex_mul(lowering, pol_wiener)
    leg_spectra = jnp.stack(
        [
            jnp.stack([temp_bar[0], grad_temp[0], pol_bar[0], spin_three[0], spin_one[0]]),
            jnp.stack([temp_bar[1], grad_temp[1], pol_bar[1], spin_three[1], spin_one[1]]),
        ]
    )
    leg_maps = to_space(inverse_columns(leg_spectra))
    temp_leg = (leg_maps[0, 0], leg_maps[1, 0])
    grad_leg = (leg_maps[0, 1], leg_maps[1, 1])
    pol_leg = (leg_maps[0, 2], leg_maps[1, 2])
    three_leg = (leg_maps[0, 3], leg_maps[1, 3])
    one_leg = (leg_maps[0, 4], leg_maps[1, 4])
    temp_term = complex_mul(temp_leg, grad_leg)
    raise_term = conj_mul(pol_leg, three_leg)
    lower_term = conj_mul(one_leg, pol_leg)
    current = (
        temp_term[0] + 0.5 * (raise_term[0] + lower_term[0]),
        temp_term[1] + 0.5 * (raise_term[1] + lower_term[1]),
    )
    current_rows = jnp.stack(row_transform((current[0][None], current[1][None]), -1.0))
    current_modes = to_frequency(current_rows)
    out_weight = mask_out * response
    estimate_modes = complex_mul(
        lowering, (out_weight * current_modes[0, 0], out_weight * current_modes[1, 0])
    )
    estimate_stack = jnp.stack([estimate_modes[0][None], estimate_modes[1][None]])
    estimate_maps = to_space(inverse_columns(estimate_stack))
    slab_result = estimate_maps[:, 0]
    return lax.all_to_all(slab_result, "rows", split_axis=1, concat_axis=2, tiled=True)


SIDE = 128
TILE = (8, 128)
LEG_GROUPS = ((0, 2), (2, 2), (4, 1))
WEIGHT_GROUPS = ((0, 3), (1, 4), (2,), (5,))
MESH = pl.DeviceIdType.MESH


def add_pair(a, b):
    imag = a[1] if b[1] is None else b[1] if a[1] is None else a[1] + b[1]
    return (a[0] + b[0], imag)


def sub_pair(a, b):
    imag = a[1] if b[1] is None else -b[1] if a[1] is None else a[1] - b[1]
    return (a[0] - b[0], imag)


def turn_pair(value, step, length, direction):
    real, imag = value
    if step == 0:
        return value
    if 4 * step == length:
        if imag is None:
            return (jnp.zeros_like(real), real if direction > 0 else -real)
        return (-imag, real) if direction > 0 else (imag, -real)
    angle = 2.0 * math.pi * step / length
    c, s = math.cos(angle), direction * math.sin(angle)
    if imag is None:
        return (real * c, real * s)
    if 8 * step == length:
        if direction > 0:
            return ((real - imag) * c, (real + imag) * c)
        return ((real + imag) * c, (imag - real) * c)
    if 8 * step == 3 * length:
        if direction > 0:
            return ((real + imag) * c, (imag - real) * c)
        return ((real - imag) * c, (real + imag) * c)
    return (real * c - imag * s, real * s + imag * c)


def short_transform(values, direction):
    length = len(values)
    if length == 1:
        return values
    even = short_transform(values[0::2], direction)
    odd = short_transform(values[1::2], direction)
    low, high = [], []
    for step in range(length // 2):
        turned = turn_pair(odd[step], step, length, direction)
        low.append(add_pair(even[step], turned))
        high.append(sub_pair(even[step], turned))
    return low + high


def split_number(x):
    top = x.astype(jnp.bfloat16)
    return top, (x - top.astype(jnp.float32)).astype(jnp.bfloat16)


def dot32(a, b):
    return jnp.dot(a, b, preferred_element_type=jnp.float32)


def matrix_left(table_ref, which, x):
    top, rest = split_number(x)
    m_top, m_rest = table_ref[which, 0], table_ref[which, 1]
    return dot32(m_top, top) + (dot32(m_top, rest) + dot32(m_rest, top))


def matrix_right(table_ref, which, x):
    top, rest = split_number(x)
    m_top, m_rest = table_ref[which, 0], table_ref[which, 1]
    return dot32(top, m_top) + (dot32(top, m_rest) + dot32(rest, m_top))


BITS = (0, 1)
OFFSETS = [
    (c, a1, e, a0) for a0 in BITS for c, a1, e in
    ((1, 1, 1), (1, 0, 0), (0, 1, 0), (0, 0, 1), (1, 1, 0), (0, 1, 1), (1, 0, 1), (0, 0, 0))
]
PEERS = [offset for offset in OFFSETS if any(offset)]
WEIGHT_ORDER = (0, 3, 1, 4, 2, 5)


def lens_kernel(
    cuts_ref, sky_hbm, filters_hbm, wiener_hbm, response_hbm, table_hbm, twiddle_hbm, out_ref,
    table_ref, twiddle_ref, sky_ref, raw, weight_ref, slab_out, slab_in, relay_buf, spec_out, spec_in, weights, legs_out, legs_in,
    maps, current, cur_out, cur_in, est_out, est_in, fin_out, fin_in,
    slab_sem, relay_sem, spec_sem, weight_sem, legs_sem, cur_sem, est_sem, fin_sem, send_sem, load_sem,
):
    rows_count, fields_count, local_rows = 4, 4, 2
    groups = rows_count * fields_count
    total_rows = groups * local_rows
    in_rows = total_rows // rows_count
    row_ratio = NC // total_rows
    my_x, my_r, my_z = (lax.axis_index(name) for name in ("sims", "rows", "fields"))
    my_y, my_c, my_h, my_l = my_r // 2, my_r % 2, my_z // 2, my_z % 2
    x_at, y_at, c_at, h_at, l_at = ((bit, 1 - bit) for bit in (my_x, my_y, my_c, my_h, my_l))
    me = my_r * fields_count + 2 * my_x + my_l
    my_block = (2 * my_x + my_l) * rows_count + my_r
    stays = my_x == my_h

    def row_of(offset):
        return 2 * y_at[offset[1]] + c_at[offset[3]]

    def peer_of(offset):
        return row_of(offset) * fields_count + 2 * x_at[offset[0]] + l_at[offset[2]]

    def peer_block(offset):
        return (2 * x_at[offset[0]] + l_at[offset[2]]) * rows_count + row_of(offset)

    def remote(src, dst, sems, x, r, z):
        return pltpu.make_async_remote_copy(
            src_ref=src, dst_ref=dst, send_sem=sems[0], recv_sem=sems[1],
            device_id={"sims": x, "rows": r, "fields": z}, device_id_type=MESH,
        )

    def send(offset, src, dst, sems):
        return remote(src, dst, sems, x_at[offset[0]], row_of(offset), 2 * my_h + l_at[offset[2]])

    def send_home(offset, src, dst, sems):
        return remote(src, dst, sems, my_h, row_of(offset), 2 * x_at[offset[0]] + l_at[offset[2]])

    def each_peer(body):
        for offset in PEERS:
            body(offset)

    def wait_all(ref, sem):
        pltpu.make_async_copy(ref, ref, sem).wait()

    for src, dst, n in (
        (sky_hbm, sky_ref, 0),
        (filters_hbm, raw.at[0:3], 1),
        (wiener_hbm, raw.at[3:5], 1),
        (response_hbm, raw.at[5], 1),
        (table_hbm, table_ref, 2),
        (twiddle_hbm, twiddle_ref, 3),
    ):
        pltpu.make_async_copy(src, dst, load_sem.at[n]).start()

    (
        slab_left, relay_left, forward_left, spec_left, weight_left, legs_left, cur_left, est_left, fin_left,
    ) = (send_sem.at[n] for n in range(9))

    barrier = pltpu.get_barrier_semaphore()
    for h in BITS:
        for c, a1, e, a0 in OFFSETS:
            if h or c or a1 or e or a0:
                pl.semaphore_signal(
                    barrier, inc=1, device_id_type=MESH,
                    device_id={"sims": x_at[c], "rows": 2 * y_at[a1] + c_at[a0], "fields": 2 * h_at[h] + l_at[e]},
                )
    wait_all(sky_ref, load_sem.at[0])
    tiles = sky_ref.shape[2] // SIDE
    for field in range(3):
        for t in range(tiles):
            slab_out[t // 8, field, :, t % 8, :] = sky_ref[field, :, t * SIDE:(t + 1) * SIDE]
    pl.semaphore_wait(barrier, 2 * groups - 1)

    ROW_OFFSETS = [(0, a1, 0, a0) for a1 in BITS for a0 in BITS]

    def slab_copy(field, offset):
        r = row_of(offset)
        return send_home(
            offset, slab_out.at[r, field], slab_in.at[my_r, field],
            (slab_left, slab_sem.at[field]),
        )

    def own_slab(field):
        return pltpu.make_async_copy(slab_out.at[my_r, field], slab_in.at[my_r, field], slab_sem.at[field])

    def relay_copy(field):
        return remote(
            slab_out.at[pl.ds(2 * y_at[1], 2), field], relay_buf.at[field],
            (relay_left, relay_sem.at[field]), x_at[1], my_r, my_z,
        )

    def forward_copy(field, core):
        a0 = core
        return remote(
            relay_buf.at[field, c_at[a0]], slab_in.at[my_r, field],
            (forward_left, slab_sem.at[field]),
            my_x, 2 * y_at[1] + c_at[a0], 2 * h_at[1] + my_l,
        )

    @pl.when(stays)
    def _():
        for field in range(3):
            own_slab(field).start()
            for offset in ROW_OFFSETS[1:]:
                slab_copy(field, offset).start()

    @pl.when(jnp.logical_not(stays))
    def _():
        for field in range(3):
            relay_copy(field).start()
            for offset in ROW_OFFSETS[:2]:
                slab_copy(field, offset).start()

    low_index = lax.broadcasted_iota(jnp.int32, (SIDE, SIDE), 0)
    high_index = lax.broadcasted_iota(jnp.int32, (SIDE, SIDE), 1)
    column_ids = low_index + SIDE * high_index
    freq_cols = jnp.where(column_ids < NC // 2, column_ids, column_ids - NC)

    def row_frequency(row):
        row_id = in_rows * my_r + 4 * (my_h + row - 2 * my_h * row) + 2 * my_l + my_x
        return jnp.where(row_id < total_rows // 2, row_id, row_id - total_rows)

    wait_all(raw, load_sem.at[1])

    def spread(n, carry):
        for j in range(8):
            start = pl.multiple_of((n * 8 + j) * SIDE, SIDE)
            weight_ref[:, :, n * 8 + j, :] = raw[:, :, pl.ds(start, SIDE)]
        return carry

    lax.fori_loop(0, SIDE // 8, spread, 0)
    scaled_home = row_ratio * row_frequency(0)
    radius_home = freq_cols * freq_cols + scaled_home * scaled_home

    def mask(n):
        low, high = cuts_ref[2 * n], cuts_ref[2 * n + 1]
        inside = (radius_home >= low * low) & (radius_home <= high * high)
        return inside.astype(jnp.float32)

    def weight_copy(n):
        group = [n in members for members in WEIGHT_GROUPS].index(True)
        return remote(
            weights.at[n, 0], weights.at[n, 1], (weight_left, weight_sem.at[group]),
            my_x, my_r, 2 * h_at[1] + my_l,
        )

    pol = mask(1)
    weights[0, 0] = mask(0) * weight_ref[0, my_x].T
    weights[1, 0] = pol * weight_ref[1, my_x].T
    weights[2, 0] = pol * weight_ref[2, my_x].T
    weights[3, 0] = weight_ref[3, my_x].T
    weights[4, 0] = weight_ref[4, my_x].T
    weights[5, 0] = mask(2) * weight_ref[5, my_x].T
    weight_copy(WEIGHT_ORDER[0]).start()

    @pl.when(jnp.logical_not(stays))
    def _():
        for n in WEIGHT_ORDER[1:]:
            weight_copy(n).start()

    def owner(k):
        return k // 8 * fields_count + 2 * (k % 2) + k // 2 % 2

    def local_row(k, half):
        return 1 - half if k // 4 % 2 else half

    def spec_copy(field, row, offset):
        return send(
            offset, spec_out.at[field, row, peer_of(offset)], spec_in.at[field, row, :, my_block],
            (spec_left, spec_sem.at[row]),
        )

    def own_spec(field, row):
        return pltpu.make_async_copy(
            spec_out.at[field, row, me], spec_in.at[field, row, :, my_block],
            spec_sem.at[row],
        )

    def spec_start(field, row):
        each_peer(lambda offset: spec_copy(field, row, offset).start())
        own_spec(field, row).start()

    def row_step(field, carry):
        @pl.when(stays)
        def _():
            wait_all(relay_buf.at[field], relay_sem.at[field])
            for core in BITS:
                forward_copy(field, core).start()

        wait_all(slab_in.at[:, field], slab_sem.at[field])
        values = [
            (slab_in[y // in_rows, field, y % in_rows], None) for y in range(total_rows)
        ]
        for k, (real, imag) in enumerate(short_transform(values, -1)):
            spec_out[field, local_row(k, my_h), owner(k), 0] = real
            spec_out[field, local_row(k, my_h), owner(k), 1] = (
                jnp.zeros_like(real) if imag is None else imag
            )
        spec_start(field, 0)
        return carry

    lax.fori_loop(0, 3, row_step, 0)

    @pl.when(stays)
    def _():
        for n in WEIGHT_ORDER[1:]:
            weight_copy(n).start()

    def later_rows(field, carry):
        spec_start(field, 1)
        return carry

    lax.fori_loop(0, 3, later_rows, 0)

    cos_f, sin_f, cos_b, sin_b = 0, 1, 2, 3

    def side_by_side(pieces, axis):
        return pieces[0] if len(pieces) == 1 else jnp.concatenate(pieces, axis=axis)

    def long_forward(pieces):
        y = matrix_left(table_ref, 0, side_by_side(pieces, 1))
        c, s = twiddle_ref[cos_f], twiddle_ref[sin_f]
        turned = []
        for n in range(len(pieces)):
            yr, yi = y[:SIDE, n * SIDE:(n + 1) * SIDE], y[SIDE:, n * SIDE:(n + 1) * SIDE]
            turned.append(jnp.concatenate([yr * c - yi * s, yr * s + yi * c], axis=1))
        z = matrix_right(table_ref, 1, side_by_side(turned, 0))
        return [
            (z[n * SIDE:(n + 1) * SIDE, :SIDE], z[n * SIDE:(n + 1) * SIDE, SIDE:])
            for n in range(len(pieces))
        ]

    def long_inverse(pairs):
        stacks = [jnp.concatenate([pair[0], pair[1]], axis=1) for pair in pairs]
        u = matrix_right(table_ref, 0, side_by_side(stacks, 0))
        c, s = twiddle_ref[cos_b], twiddle_ref[sin_b]
        turned = []
        for n in range(len(pairs)):
            ur, ui = u[n * SIDE:(n + 1) * SIDE, :SIDE], u[n * SIDE:(n + 1) * SIDE, SIDE:]
            turned.append(jnp.concatenate([ur * c - ui * s, ur * s + ui * c], axis=0))
        x = matrix_left(table_ref, 1, side_by_side(turned, 1))
        return [
            x[:, n * SIDE:(n + 1) * SIDE].reshape((2, groups) + TILE)
            for n in range(len(pairs))
        ]

    def legs_copy(row, g, offset):
        first, count = LEG_GROUPS[g]
        return send(
            offset, legs_out.at[row, first:first + count, :, peer_block(offset)],
            legs_in.at[row, me, first:first + count],
            (legs_left, legs_sem.at[g]),
        )

    def own_legs(row, g):
        first, count = LEG_GROUPS[g]
        return pltpu.make_async_copy(
            legs_out.at[row, first:first + count, :, my_block],
            legs_in.at[row, me, first:first + count],
            legs_sem.at[g],
        )

    def wait_weights(group):
        members = WEIGHT_GROUPS[group]
        wait_all(weights.at[0:len(members), 1], weight_sem.at[group])

    def slopes(row):
        along_x = (2 * freq_cols).astype(jnp.float32) / NC
        along_y = (2 * row_frequency(row)).astype(jnp.float32) / total_rows
        return along_x, along_y

    def leg_step(row, carry):
        wait_all(spec_in.at[:, row], spec_sem.at[row])
        temp, stokes_q, stokes_u = long_forward(
            [spec_in[field, row].reshape(2 * SIDE, SIDE) for field in range(3)]
        )
        scaled = row_ratio * row_frequency(row)
        radius_sq = freq_cols * freq_cols + scaled * scaled
        floor = jnp.maximum(radius_sq, 1).astype(jnp.float32)
        cos2 = (freq_cols * freq_cols - scaled * scaled).astype(jnp.float32) / floor
        sin2 = (2 * freq_cols * scaled).astype(jnp.float32) / floor
        along_x, along_y = slopes(row)
        raising, lowering = (-along_y, along_x), (along_y, along_x)
        rot = (cos2, sin2)

        def temp_legs():
            t_bar = (weights[0, row] * temp[0], weights[0, row] * temp[1])
            return t_bar, complex_mul((weights[3, row] * t_bar[0], weights[3, row] * t_bar[1]), raising)

        def e_modes():
            return tuple(-weights[1, row] * (cos2 * a + sin2 * b) for a, b in zip(stokes_q, stokes_u))

        def spin_legs():
            e_bar = e_modes()
            w = complex_mul((-weights[4, row] * e_bar[0], -weights[4, row] * e_bar[1]), rot)
            return complex_mul(w, raising), complex_mul(w, lowering)

        def pol_leg():
            e_bar = e_modes()
            b_bar = tuple(weights[2, row] * (sin2 * a - cos2 * b) for a, b in zip(stokes_q, stokes_u))
            return (complex_mul((b_bar[1] - e_bar[0], -(e_bar[1] + b_bar[0])), rot),)

        for n, make in enumerate((temp_legs, spin_legs, pol_leg)):
            @pl.when(row == 1)
            def _():
                wait_weights(n)

            for k, leg_map in enumerate(long_inverse(make())):
                legs_out[row, LEG_GROUPS[n][0] + k] = leg_map
            each_peer(lambda offset: legs_copy(row, n, offset).start())
            own_legs(row, n).start()
        return carry

    wait_all(table_ref, load_sem.at[2])
    wait_all(twiddle_ref, load_sem.at[3])
    lax.fori_loop(0, local_rows, leg_step, 0)

    def map_step(n, carry):
        values = [
            (legs_in[local_row(k, my_h), owner(k), n, 0], legs_in[local_row(k, my_h), owner(k), n, 1])
            for k in range(total_rows)
        ]
        for y, (real, imag) in enumerate(short_transform(values, 1)):
            maps[n, 0, y] = real
            maps[n, 1, y] = imag
        return carry

    for g, (first, count) in enumerate(LEG_GROUPS):
        wait_all(legs_in.at[:, :, first:first + count], legs_sem.at[g])
        lax.fori_loop(first, first + count, map_step, 0)

    def product_step(y, carry):
        a, g, h3, h1, p = [(maps[n, 0, y], maps[n, 1, y]) for n in range(5)]
        ag, ph, hp = complex_mul(a, g), conj_mul(p, h3), conj_mul(h1, p)
        current[0, y] = ag[0] + 0.5 * (ph[0] + hp[0])
        current[1, y] = ag[1] + 0.5 * (ph[1] + hp[1])
        return carry

    lax.fori_loop(0, total_rows, product_step, 0)

    values = [(current[0, y], current[1, y]) for y in range(total_rows)]
    for k, (real, imag) in enumerate(short_transform(values, -1)):
        cur_out[local_row(k, my_h), owner(k), 0] = real
        cur_out[local_row(k, my_h), owner(k), 1] = imag

    def cur_copy(row, offset):
        return send(
            offset, cur_out.at[row, peer_of(offset)], cur_in.at[row, :, my_block],
            (cur_left, cur_sem.at[row]),
        )

    def own_cur(row):
        return pltpu.make_async_copy(
            cur_out.at[row, me], cur_in.at[row, :, my_block], cur_sem.at[row]
        )

    def cur_start(row, carry):
        each_peer(lambda offset: cur_copy(row, offset).start())
        own_cur(row).start()
        return carry

    lax.fori_loop(0, local_rows, cur_start, 0)

    def est_copy(row, offset):
        return send_home(
            offset, est_out.at[row, :, peer_block(offset)], est_in.at[row, me],
            (est_left, est_sem.at[0]),
        )

    ORIGIN = (0, 0, 0, 0)

    def own_est(row):
        return pltpu.make_async_copy(
            est_out.at[row, :, my_block], est_in.at[row, me], est_sem.at[0]
        )

    def estimate_step(row, carry):
        wait_all(cur_in.at[row], cur_sem.at[row])

        @pl.when(row == 1)
        def _():
            wait_weights(3)

        (modes,) = long_forward([cur_in[row].reshape(2 * SIDE, SIDE)])
        along_x, along_y = slopes(row)
        w = weights[5, row]
        estimate = complex_mul((w * modes[0], w * modes[1]), (along_y, along_x))
        (est_out[row],) = long_inverse([estimate])
        each_peer(lambda offset: est_copy(row, offset).start())

        @pl.when(stays)
        def _():
            own_est(row).start()

        @pl.when(jnp.logical_not(stays))
        def _():
            est_copy(row, ORIGIN).start()

        return carry

    lax.fori_loop(0, local_rows, estimate_step, 0)

    wait_all(est_in, est_sem.at[0])
    values = [
        (est_in[local_row(k, my_x), owner(k), 0], est_in[local_row(k, my_x), owner(k), 1])
        for k in range(total_rows)
    ]
    for y, (real, imag) in enumerate(short_transform(values, 1)):
        fin_out[y // in_rows, 0, y % in_rows] = real
        fin_out[y // in_rows, 1, y % in_rows] = imag

    def fin_copy(offset):
        r = row_of(offset)
        return remote(
            fin_out.at[r], fin_in.at[my_r], (fin_left, fin_sem.at[0]), my_x, r, my_z
        )

    for offset in ROW_OFFSETS[1:]:
        fin_copy(offset).start()
    own_fin = pltpu.make_async_copy(
        fin_out.at[my_r], fin_in.at[my_r], fin_sem.at[0]
    )
    own_fin.start()

    others = groups - 1

    @pl.when(stays)
    def _():
        wait_all(slab_out.at[0:3], slab_left)
        wait_all(relay_buf, forward_left)
        wait_all(est_out.at[:, :, 0:others], est_left)

    @pl.when(jnp.logical_not(stays))
    def _():
        wait_all(slab_out.at[0:2], slab_left)
        wait_all(relay_buf, relay_left)
        wait_all(est_out, est_left)

    wait_all(weights.at[:, 0], weight_left)
    wait_all(spec_out.at[:, :, 0:others], spec_left)
    wait_all(legs_out.at[:, :, :, 0:others], legs_left)
    wait_all(cur_out.at[:, 0:others], cur_left)
    wait_all(fin_in, fin_sem.at[0])
    for part in range(2):
        for t in range(tiles):
            out_ref[part, :, t * SIDE:(t + 1) * SIDE] = fin_in[t // 8, part, :, t % 8, :]

    wait_all(fin_out.at[0:3], fin_left)


def long_tables(total_rows):
    index = np.arange(SIDE)
    angle = 2.0 * np.pi * (index[:, None] * index[None, :] % SIDE) / SIDE
    c, s = np.cos(angle), np.sin(angle)
    forward = np.block([[c, s], [-s, c]]).astype(np.float32)
    tables = np.stack([forward, forward.T])
    top = tables.astype(jnp.bfloat16)
    rest = (tables - top.astype(np.float32)).astype(jnp.bfloat16)
    turn = 2.0 * np.pi * (index[:, None] * index[None, :]) / NC
    scale = 1.0 / (NC * total_rows)
    twiddle = np.stack(
        [np.cos(turn), -np.sin(turn), scale * np.cos(turn), scale * np.sin(turn)]
    ).astype(np.float32)
    return np.stack([top, rest], axis=1), twiddle


def fused_body(rows_count, fields_count, sky_maps, band_cuts, filters, wiener, response):
    groups = rows_count * fields_count
    local_rows = response.shape[0]
    total_rows = local_rows * groups
    in_rows = total_rows // rows_count
    table, twiddle = long_tables(total_rows)
    vmem = pl.BlockSpec(memory_space=pltpu.VMEM)
    f32 = jnp.float32
    dma = pltpu.SemaphoreType.DMA
    slab = pltpu.VMEM((rows_count, 3, in_rows) + TILE, f32)
    chunk = pltpu.VMEM((local_rows, groups, 2) + TILE, f32)
    lines = pltpu.VMEM((local_rows, 2, groups) + TILE, f32)
    final = pltpu.VMEM((rows_count, 2, in_rows) + TILE, f32)
    return pl.pallas_call(
        lens_kernel,
        out_shape=jax.ShapeDtypeStruct((2,) + sky_maps.shape[1:], f32),
        in_specs=[pl.BlockSpec(memory_space=pltpu.SMEM)] + [pl.BlockSpec(memory_space=pl.ANY)] * 6,
        out_specs=vmem,
        scratch_shapes=[
            pltpu.VMEM(table.shape, table.dtype), pltpu.VMEM(twiddle.shape, f32),
            pltpu.VMEM(sky_maps.shape, f32),
            pltpu.VMEM((6, local_rows, NC), f32),
            pltpu.VMEM((6, local_rows, SIDE, SIDE), f32),
            slab, slab,
            pltpu.VMEM((3, 2, in_rows) + TILE, f32),
            pltpu.VMEM((3, local_rows, groups, 2) + TILE, f32),
            pltpu.VMEM((3, local_rows, 2, groups) + TILE, f32),
            pltpu.VMEM((6, local_rows, SIDE, SIDE), f32),
            pltpu.VMEM((local_rows, 5, 2, groups) + TILE, f32),
            pltpu.VMEM((local_rows, groups, 5, 2) + TILE, f32),
            pltpu.VMEM((5, 2, total_rows) + TILE, f32),
            pltpu.VMEM((2, total_rows) + TILE, f32),
            chunk, lines, lines, chunk, final, final,
            dma((3,)), dma((3,)), dma((local_rows,)), dma((len(WEIGHT_GROUPS),)), dma((len(LEG_GROUPS),)),
            dma((local_rows,)), dma((1,)), dma((1,)), dma((9,)), dma((4,)),
        ],
        compiler_params=pltpu.CompilerParams(
            collective_id=0, has_side_effects=True, vmem_limit_bytes=60 * 1024 * 1024
        ),
        name="lens",
    )(band_cuts, sky_maps, filters, wiener, response, jnp.asarray(table), jnp.asarray(twiddle))


def solution(mesh):
    placed = (
        P("sims", "rows", "fields"),
        P(),
        P(None, ("rows", "fields"), None),
        P(None, ("rows", "fields"), None),
        P(("rows", "fields"), None),
    )
    rows_count, fields_count = mesh.shape["rows"], mesh.shape["fields"]
    groups = rows_count * fields_count

    def choose(sky_maps, *rest):
        fits = (
            NC == SIDE * SIDE
            and (mesh.shape["sims"], rows_count, fields_count) == (2, 4, 4)
            and NC // groups == TILE[0] * TILE[1]
            and sky_maps.shape[0] == 3
            and sky_maps.shape[1] * rows_count == 32
        )
        if fits:
            return fused_body(rows_count, fields_count, sky_maps, *rest)
        return body(sky_maps, *rest)

    return jax.shard_map(
        choose, mesh=mesh, in_specs=placed, out_specs=P("sims", "rows", "fields"), check_vma=False
    )
```

```python
import functools
import math

import jax
import jax.numpy as jnp
import numpy as np
from jax import lax
from jax.experimental import pallas as pl
from jax.experimental.pallas import tpu as pltpu
from jax.sharding import PartitionSpec as P

NC = 16384


exact_mode = lax.Precision.HIGHEST


def split_factor(length):
    best_first = 1
    for divisor in range(1, math.isqrt(length) + 1):
        if length % divisor == 0:
            best_first = divisor
    return (best_first, length // best_first)


def phase_table(left_index, right_index, period, direction):
    product = left_index[:, None] * right_index[None, :] % period
    angles = direction * 2.0 * math.pi / period * product.astype(jnp.float32)
    return (jnp.cos(angles), jnp.sin(angles))


def complex_einsum(formula, data_pair, table_pair):
    data_real, data_imag = data_pair
    table_real, table_imag = table_pair
    real_out = jnp.einsum(formula, data_real, table_real, precision=exact_mode)
    imag_out = jnp.einsum(formula, data_real, table_imag, precision=exact_mode)
    if data_imag is not None:
        real_out = real_out - jnp.einsum(formula, data_imag, table_imag, precision=exact_mode)
        imag_out = imag_out + jnp.einsum(formula, data_imag, table_real, precision=exact_mode)
    return (real_out, imag_out)


def complex_mul(left_pair, right_pair):
    return (
        left_pair[0] * right_pair[0] - left_pair[1] * right_pair[1],
        left_pair[0] * right_pair[1] + left_pair[1] * right_pair[0],
    )


def conj_mul(left_pair, right_pair):
    return (
        left_pair[0] * right_pair[0] + left_pair[1] * right_pair[1],
        left_pair[0] * right_pair[1] - left_pair[1] * right_pair[0],
    )


def row_transform(data_pair, direction):
    batch_len, length, block_width = data_pair[0].shape
    outer_len, inner_len = split_factor(length)
    outer_ids = jnp.arange(outer_len, dtype=jnp.int32)
    inner_ids = jnp.arange(inner_len, dtype=jnp.int32)
    real_in = data_pair[0].reshape(batch_len, outer_len, inner_len, block_width)
    imag_in = None
    if data_pair[1] is not None:
        imag_in = data_pair[1].reshape(batch_len, outer_len, inner_len, block_width)
    middle = complex_einsum(
        "bjmc,jk->bkmc", (real_in, imag_in), phase_table(outer_ids, outer_ids, outer_len, direction)
    )
    twiddle = phase_table(outer_ids, inner_ids, length, direction)
    middle = complex_mul(middle, (twiddle[0][None, :, :, None], twiddle[1][None, :, :, None]))
    result = complex_einsum(
        "bkmc,mq->bqkc", middle, phase_table(inner_ids, inner_ids, inner_len, direction)
    )
    norm_factor = 1.0 if direction < 0 else 1.0 / length
    return (
        result[0].reshape(batch_len, length, block_width) * norm_factor,
        result[1].reshape(batch_len, length, block_width) * norm_factor,
    )


def block_order(groups, fields_count):
    positions = jnp.arange(groups, dtype=jnp.int32)
    blocks = positions % fields_count * (groups // fields_count) + positions // fields_count
    return (positions, blocks)


def column_forward(data_pair, groups, fields_count):
    batch_len, local_rows, total_len = data_pair[0].shape
    block_width = total_len // groups
    positions, blocks = block_order(groups, fields_count)
    column_ids = jnp.arange(block_width, dtype=jnp.int32)
    shaped = (
        data_pair[0].reshape(batch_len, local_rows, groups, block_width),
        data_pair[1].reshape(batch_len, local_rows, groups, block_width),
    )
    middle = complex_einsum("brpc,pk->brkc", shaped, phase_table(blocks, positions, groups, -1.0))
    twiddle = phase_table(positions, column_ids, total_len, -1.0)
    middle = complex_mul(middle, (twiddle[0][None, None], twiddle[1][None, None]))
    result = complex_einsum(
        "brkc,cq->brqk", middle, phase_table(column_ids, column_ids, block_width, -1.0)
    )
    return (
        result[0].reshape(batch_len, local_rows, total_len),
        result[1].reshape(batch_len, local_rows, total_len),
    )


def column_inverse(data_pair, groups, fields_count):
    batch_len, local_rows, total_len = data_pair[0].shape
    block_width = total_len // groups
    positions, blocks = block_order(groups, fields_count)
    column_ids = jnp.arange(block_width, dtype=jnp.int32)
    shaped = (
        data_pair[0].reshape(batch_len, local_rows, block_width, groups),
        data_pair[1].reshape(batch_len, local_rows, block_width, groups),
    )
    middle = complex_einsum(
        "brqk,qc->brkc", shaped, phase_table(column_ids, column_ids, block_width, 1.0)
    )
    twiddle = phase_table(positions, column_ids, total_len, 1.0)
    middle = complex_mul(middle, (twiddle[0][None, None], twiddle[1][None, None]))
    result = complex_einsum("brkc,kp->brpc", middle, phase_table(positions, blocks, groups, 1.0))
    norm_factor = 1.0 / total_len
    return (
        result[0].reshape(batch_len, local_rows, total_len) * norm_factor,
        result[1].reshape(batch_len, local_rows, total_len) * norm_factor,
    )


def body(sky_maps, band_cuts, filters, wiener, response):
    rows_count = lax.axis_size("rows")
    fields_count = lax.axis_size("fields")
    groups = rows_count * fields_count
    local_rows = filters.shape[1]
    total_rows = local_rows * groups
    row_ratio = NC // total_rows

    def forward_columns(stacked):
        return jnp.stack(column_forward((stacked[0], stacked[1]), groups, fields_count))

    def inverse_rows(stacked):
        return jnp.stack(row_transform((stacked[0], stacked[1]), 1.0))

    def inverse_columns(stacked):
        return jnp.stack(column_inverse((stacked[0], stacked[1]), groups, fields_count))

    def to_frequency(stacked):
        batch_len = stacked.shape[1]
        block_width = stacked.shape[3]
        shaped = stacked.reshape(
            2, batch_len, rows_count, fields_count, local_rows, 1, 1, block_width
        )
        arrived = lax.all_to_all(
            lax.all_to_all(shaped, "rows", split_axis=2, concat_axis=5, tiled=True),
            "fields",
            split_axis=3,
            concat_axis=6,
            tiled=True,
        )
        result = forward_columns(arrived.reshape(2, batch_len, local_rows, groups * block_width))
        return result

    def to_space(stacked):
        batch_len = stacked.shape[1]
        block_width = stacked.shape[3] // groups
        shaped = stacked.reshape(
            2, batch_len, 1, 1, local_rows, rows_count, fields_count, block_width
        )
        arrived = lax.all_to_all(
            lax.all_to_all(shaped, "rows", split_axis=5, concat_axis=2, tiled=True),
            "fields",
            split_axis=6,
            concat_axis=3,
            tiled=True,
        )
        result = inverse_rows(arrived.reshape(2, batch_len, total_rows, block_width))
        return result

    slab_spectra = jnp.stack(
        row_transform(
            (lax.all_to_all(sky_maps, "rows", split_axis=2, concat_axis=1, tiled=True), None), -1.0
        )
    )
    sky_spectra = to_frequency(slab_spectra)
    row_ids = lax.axis_index(("rows", "fields")) * local_rows + jnp.arange(
        local_rows, dtype=jnp.int32
    )
    freq_rows = jnp.where(row_ids < total_rows // 2, row_ids, row_ids - total_rows)[:, None]
    column_ids = jnp.arange(NC, dtype=jnp.int32)
    freq_cols = jnp.where(column_ids < NC // 2, column_ids, column_ids - NC)[None, :]
    scaled_rows = row_ratio * freq_rows
    radius_sq = freq_cols * freq_cols + scaled_rows * scaled_rows

    def band_mask(lower_cut, upper_cut):
        inside = (radius_sq >= lower_cut * lower_cut) & (radius_sq <= upper_cut * upper_cut)
        return inside.astype(jnp.float32)

    mask_temp = band_mask(band_cuts[0], band_cuts[1])
    mask_pol = band_mask(band_cuts[2], band_cuts[3])
    mask_out = band_mask(band_cuts[4], band_cuts[5])
    radius_floor = jnp.maximum(radius_sq, 1).astype(jnp.float32)
    cos_two = (freq_cols * freq_cols - scaled_rows * scaled_rows).astype(jnp.float32) / radius_floor
    sin_two = (2 * freq_cols * scaled_rows).astype(jnp.float32) / radius_floor
    along_x = (2 * freq_cols).astype(jnp.float32) / NC
    along_y = (2 * freq_rows).astype(jnp.float32) / total_rows
    raising = (-along_y + 0.0 * along_x, along_x + 0.0 * along_y)
    lowering = (along_y + 0.0 * along_x, along_x + 0.0 * along_y)
    rotation = (cos_two, sin_two)
    temp_modes = (sky_spectra[0, 0], sky_spectra[1, 0])
    stokes_q = (sky_spectra[0, 1], sky_spectra[1, 1])
    stokes_u = (sky_spectra[0, 2], sky_spectra[1, 2])
    e_modes = (
        -(cos_two * stokes_q[0] + sin_two * stokes_u[0]),
        -(cos_two * stokes_q[1] + sin_two * stokes_u[1]),
    )
    b_modes = (
        sin_two * stokes_q[0] - cos_two * stokes_u[0],
        sin_two * stokes_q[1] - cos_two * stokes_u[1],
    )
    temp_weight = mask_temp * filters[0]
    e_weight = mask_pol * filters[1]
    b_weight = mask_pol * filters[2]
    temp_bar = (temp_weight * temp_modes[0], temp_weight * temp_modes[1])
    e_bar = (e_weight * e_modes[0], e_weight * e_modes[1])
    b_bar = (b_weight * b_modes[0], b_weight * b_modes[1])
    grad_temp = complex_mul(raising, (wiener[0] * temp_bar[0], wiener[0] * temp_bar[1]))
    pol_sum = complex_mul((e_bar[0] - b_bar[1], e_bar[1] + b_bar[0]), rotation)
    pol_bar = (-pol_sum[0], -pol_sum[1])
    pol_rot = complex_mul((wiener[1] * e_bar[0], wiener[1] * e_bar[1]), rotation)
    pol_wiener = (-pol_rot[0], -pol_rot[1])
    spin_three = complex_mul(raising, pol_wiener)
    spin_one = complex_mul(lowering, pol_wiener)
    leg_spectra = jnp.stack(
        [
            jnp.stack([temp_bar[0], grad_temp[0], pol_bar[0], spin_three[0], spin_one[0]]),
            jnp.stack([temp_bar[1], grad_temp[1], pol_bar[1], spin_three[1], spin_one[1]]),
        ]
    )
    leg_maps = to_space(inverse_columns(leg_spectra))
    temp_leg = (leg_maps[0, 0], leg_maps[1, 0])
    grad_leg = (leg_maps[0, 1], leg_maps[1, 1])
    pol_leg = (leg_maps[0, 2], leg_maps[1, 2])
    three_leg = (leg_maps[0, 3], leg_maps[1, 3])
    one_leg = (leg_maps[0, 4], leg_maps[1, 4])
    temp_term = complex_mul(temp_leg, grad_leg)
    raise_term = conj_mul(pol_leg, three_leg)
    lower_term = conj_mul(one_leg, pol_leg)
    current = (
        temp_term[0] + 0.5 * (raise_term[0] + lower_term[0]),
        temp_term[1] + 0.5 * (raise_term[1] + lower_term[1]),
    )
    current_rows = jnp.stack(row_transform((current[0][None], current[1][None]), -1.0))
    current_modes = to_frequency(current_rows)
    out_weight = mask_out * response
    estimate_modes = complex_mul(
        lowering, (out_weight * current_modes[0, 0], out_weight * current_modes[1, 0])
    )
    estimate_stack = jnp.stack([estimate_modes[0][None], estimate_modes[1][None]])
    estimate_maps = to_space(inverse_columns(estimate_stack))
    slab_result = estimate_maps[:, 0]
    return lax.all_to_all(slab_result, "rows", split_axis=1, concat_axis=2, tiled=True)


SIDE = 128
TILE = (8, 128)
LEG_GROUPS = ((0, 2), (2, 2), (4, 1))
WEIGHT_GROUPS = ((0, 3), (1, 4), (2,), (5,))
MESH = pl.DeviceIdType.MESH


def add_pair(a, b):
    imag = a[1] if b[1] is None else b[1] if a[1] is None else a[1] + b[1]
    return (a[0] + b[0], imag)


def sub_pair(a, b):
    imag = a[1] if b[1] is None else -b[1] if a[1] is None else a[1] - b[1]
    return (a[0] - b[0], imag)


def turn_pair(value, step, length, direction):
    real, imag = value
    if step == 0:
        return value
    if 4 * step == length:
        if imag is None:
            return (jnp.zeros_like(real), real if direction > 0 else -real)
        return (-imag, real) if direction > 0 else (imag, -real)
    angle = 2.0 * math.pi * step / length
    c, s = math.cos(angle), direction * math.sin(angle)
    if imag is None:
        return (real * c, real * s)
    if 8 * step == length:
        if direction > 0:
            return ((real - imag) * c, (real + imag) * c)
        return ((real + imag) * c, (imag - real) * c)
    if 8 * step == 3 * length:
        if direction > 0:
            return ((real + imag) * c, (imag - real) * c)
        return ((real - imag) * c, (real + imag) * c)
    return (real * c - imag * s, real * s + imag * c)


def short_transform(values, direction):
    length = len(values)
    if length == 1:
        return values
    even = short_transform(values[0::2], direction)
    odd = short_transform(values[1::2], direction)
    low, high = [], []
    for step in range(length // 2):
        turned = turn_pair(odd[step], step, length, direction)
        low.append(add_pair(even[step], turned))
        high.append(sub_pair(even[step], turned))
    return low + high


def split_number(x):
    top = x.astype(jnp.bfloat16)
    return top, (x - top.astype(jnp.float32)).astype(jnp.bfloat16)


def dot32(a, b):
    return jnp.dot(a, b, preferred_element_type=jnp.float32)


def matrix_left(table_ref, which, x):
    top, rest = split_number(x)
    m_top, m_rest = table_ref[which, 0], table_ref[which, 1]
    return dot32(m_top, top) + (dot32(m_top, rest) + dot32(m_rest, top))


def matrix_right(table_ref, which, x):
    top, rest = split_number(x)
    m_top, m_rest = table_ref[which, 0], table_ref[which, 1]
    return dot32(top, m_top) + (dot32(top, m_rest) + dot32(rest, m_top))


BITS = (0, 1)
OFFSETS = [
    (c, a1, e, a0) for a0 in BITS for c, a1, e in
    ((1, 1, 1), (1, 0, 0), (0, 1, 0), (0, 0, 1), (1, 1, 0), (0, 1, 1), (1, 0, 1), (0, 0, 0))
]
PEERS = [offset for offset in OFFSETS if any(offset)]
WEIGHT_ORDER = (0, 3, 1, 4, 2, 5)


def lens_kernel(
    cuts_ref, sky_hbm, filters_hbm, wiener_hbm, response_hbm, table_hbm, twiddle_hbm, out_ref,
    table_ref, twiddle_ref, sky_ref, raw, weight_ref, slab_out, slab_in, relay_buf, spec_out, spec_in, weights, modes, legs_out, legs_in,
    maps, current, cur_out, cur_in, est_out, est_in, fin_out, fin_in,
    slab_sem, relay_sem, spec_sem, weight_sem, legs_sem, cur_sem, est_sem, fin_sem, send_sem, load_sem,
):
    rows_count, fields_count, local_rows = 4, 4, 2
    groups = rows_count * fields_count
    total_rows = groups * local_rows
    in_rows = total_rows // rows_count
    row_ratio = NC // total_rows
    my_x, my_r, my_z = (lax.axis_index(name) for name in ("sims", "rows", "fields"))
    my_y, my_c, my_h, my_l = my_r // 2, my_r % 2, my_z // 2, my_z % 2
    x_at, y_at, c_at, h_at, l_at = ((bit, 1 - bit) for bit in (my_x, my_y, my_c, my_h, my_l))
    me = my_r * fields_count + 2 * my_x + my_l
    my_block = (2 * my_x + my_l) * rows_count + my_r
    stays = my_x == my_h

    half_rows = total_rows // 2
    corner = my_x + my_l == 0
    far = jnp.logical_and(corner, my_y == 1)
    near = jnp.logical_and(corner, my_y == 0)
    home_row = in_rows * my_r + 4 * my_h + 2 * my_l + my_x
    first_row = jnp.where(corner, in_rows * my_c + 4 * (my_h + my_y - 2 * my_h * my_y), home_row)

    def signed(row):
        return jnp.where(row < half_rows, row, row - total_rows)

    def row_of(offset):
        return 2 * y_at[offset[1]] + c_at[offset[3]]

    def peer_of(offset):
        return row_of(offset) * fields_count + 2 * x_at[offset[0]] + l_at[offset[2]]

    def peer_block(offset):
        return (2 * x_at[offset[0]] + l_at[offset[2]]) * rows_count + row_of(offset)

    def remote(src, dst, sems, x, r, z):
        return pltpu.make_async_remote_copy(
            src_ref=src, dst_ref=dst, send_sem=sems[0], recv_sem=sems[1],
            device_id={"sims": x, "rows": r, "fields": z}, device_id_type=MESH,
        )

    def send(offset, src, dst, sems):
        return remote(src, dst, sems, x_at[offset[0]], row_of(offset), 2 * my_h + l_at[offset[2]])

    def send_home(offset, src, dst, sems):
        return remote(src, dst, sems, my_h, row_of(offset), 2 * x_at[offset[0]] + l_at[offset[2]])

    def each_peer(body):
        for offset in PEERS:
            body(offset)

    def wait_all(ref, sem):
        pltpu.make_async_copy(ref, ref, sem).wait()

    for src, dst, n in (
        (sky_hbm, sky_ref, 0),
        (filters_hbm, raw.at[0:3], 1),
        (wiener_hbm, raw.at[3:5], 1),
        (response_hbm, raw.at[5], 1),
        (table_hbm, table_ref, 2),
        (twiddle_hbm, twiddle_ref, 3),
    ):
        pltpu.make_async_copy(src, dst, load_sem.at[n]).start()

    (
        slab_left, relay_left, forward_left, spec_left, weight_left, legs_left, cur_left, est_left, fin_left,
        extra_left,
    ) = (send_sem.at[n] for n in range(10))

    barrier = pltpu.get_barrier_semaphore()
    for h in BITS:
        for c, a1, e, a0 in OFFSETS:
            if h or c or a1 or e or a0:
                pl.semaphore_signal(
                    barrier, inc=1, device_id_type=MESH,
                    device_id={"sims": x_at[c], "rows": 2 * y_at[a1] + c_at[a0], "fields": 2 * h_at[h] + l_at[e]},
                )
    wait_all(sky_ref, load_sem.at[0])
    tiles = sky_ref.shape[2] // SIDE
    for field in range(3):
        for t in range(tiles):
            slab_out[t // 8, field, :, t % 8, :] = sky_ref[field, :, t * SIDE:(t + 1) * SIDE]
    pl.semaphore_wait(barrier, 2 * groups - 1)

    ROW_OFFSETS = [(0, a1, 0, a0) for a1 in BITS for a0 in BITS]

    def slab_copy(field, offset):
        r = row_of(offset)
        return send_home(
            offset, slab_out.at[r, field], slab_in.at[my_r, field],
            (slab_left, slab_sem.at[field]),
        )

    def own_slab(field):
        return pltpu.make_async_copy(slab_out.at[my_r, field], slab_in.at[my_r, field], slab_sem.at[field])

    def relay_copy(field):
        return remote(
            slab_out.at[pl.ds(2 * y_at[1], 2), field], relay_buf.at[field],
            (relay_left, relay_sem.at[field]), x_at[1], my_r, my_z,
        )

    def forward_copy(field, core):
        a0 = core
        return remote(
            relay_buf.at[field, c_at[a0]], slab_in.at[my_r, field],
            (forward_left, slab_sem.at[field]),
            my_x, 2 * y_at[1] + c_at[a0], 2 * h_at[1] + my_l,
        )

    @pl.when(stays)
    def _():
        for field in range(3):
            own_slab(field).start()
            for offset in ROW_OFFSETS[1:]:
                slab_copy(field, offset).start()

    @pl.when(jnp.logical_not(stays))
    def _():
        for field in range(3):
            relay_copy(field).start()
            for offset in ROW_OFFSETS[:2]:
                slab_copy(field, offset).start()

    low_index = lax.broadcasted_iota(jnp.int32, (SIDE, SIDE), 0)
    high_index = lax.broadcasted_iota(jnp.int32, (SIDE, SIDE), 1)
    column_ids = low_index + SIDE * high_index
    freq_cols = jnp.where(column_ids < NC // 2, column_ids, column_ids - NC)

    def row_frequency(row):
        return jnp.where(first_row == 0, -half_rows * row, signed(first_row) * (1 - 2 * row))

    wait_all(raw, load_sem.at[1])

    def spread(n, carry):
        for j in range(8):
            start = pl.multiple_of((n * 8 + j) * SIDE, SIDE)
            weight_ref[:, :, n * 8 + j, :] = raw[:, :, pl.ds(start, SIDE)]
        return carry

    lax.fori_loop(0, SIDE // 8, spread, 0)
    scaled_home = row_ratio * signed(home_row)
    radius_home = freq_cols * freq_cols + scaled_home * scaled_home

    def mask(n):
        low, high = cuts_ref[2 * n], cuts_ref[2 * n + 1]
        inside = (radius_home >= low * low) & (radius_home <= high * high)
        return inside.astype(jnp.float32)

    home_slot = jnp.where(far, 2, 0)
    slot = jnp.where(near, 0, 1)
    other_r = jnp.where(near, my_r + 2, jnp.where(far, jnp.where(my_h == 0, my_r, 5 - my_r), 3 - my_r))

    def weight_copy(n):
        group = [n in members for members in WEIGHT_GROUPS].index(True)
        return remote(
            weights.at[n, home_slot], weights.at[n, slot], (weight_left, weight_sem.at[slot, group]),
            my_x, other_r, 2 * h_at[1] + jnp.where(my_x == 1, 1 - my_l, my_l),
        )

    def extra_copy(n):
        group = [n in members for members in WEIGHT_GROUPS].index(True)
        return remote(
            weights.at[n, home_slot], weights.at[n, 1], (extra_left, weight_sem.at[1, group]),
            my_x, jnp.where(my_h == 0, my_r - 2, 3 - my_r), my_z,
        )

    def weight_start(n):
        weight_copy(n).start()

        @pl.when(far)
        def _():
            extra_copy(n).start()

    pol = mask(1)
    weights[0, home_slot] = mask(0) * weight_ref[0, my_x].T
    weights[1, home_slot] = pol * weight_ref[1, my_x].T
    weights[2, home_slot] = pol * weight_ref[2, my_x].T
    weights[3, home_slot] = weight_ref[3, my_x].T
    weights[4, home_slot] = weight_ref[4, my_x].T
    weights[5, home_slot] = mask(2) * weight_ref[5, my_x].T
    weight_start(WEIGHT_ORDER[0])

    @pl.when(jnp.logical_not(stays))
    def _():
        for n in WEIGHT_ORDER[1:5]:
            weight_start(n)

    def owner(k):
        return k // 8 * fields_count + 2 * (k % 2) + k // 2 % 2

    def place(k, half):
        if k % 4 == 0:
            base = k % half_rows if k <= half_rows else total_rows - k
            upper = half if base % 8 == 0 else 1 - half
            return int(k >= half_rows), (base // in_rows + 2 * upper) * fields_count
        away = 1 - half if k // 4 % 2 else half
        return away, owner(k) + away * (owner(total_rows - k) - owner(k))

    def spec_copy(field, offset):
        return send(
            offset, spec_out.at[field, 0, peer_of(offset)], spec_in.at[field, :, my_block],
            (spec_left, spec_sem.at[field]),
        )

    def own_spec(field):
        return pltpu.make_async_copy(
            spec_out.at[field, 0, me], spec_in.at[field, :, my_block], spec_sem.at[field]
        )

    def spec_start(field):
        each_peer(lambda offset: spec_copy(field, offset).start())
        own_spec(field).start()

    def row_step(field, carry):
        @pl.when(stays)
        def _():
            wait_all(relay_buf.at[field], relay_sem.at[field])
            for core in BITS:
                forward_copy(field, core).start()

        wait_all(slab_in.at[:, field], slab_sem.at[field])
        values = [
            (slab_in[y // in_rows, field, y % in_rows], None) for y in range(total_rows)
        ]
        lines = short_transform(values, -1)
        lines[0] = (lines[0][0], lines[half_rows][0])
        for k, (real, imag) in enumerate(lines):
            if k % 4 == 0 and k >= half_rows:
                continue
            local, device = place(k, my_h)
            spec_out[field, local, device, 0] = real
            spec_out[field, local, device, 1] = imag
        spec_start(field)
        return carry

    lax.fori_loop(0, 3, row_step, 0)

    @pl.when(stays)
    def _():
        for n in WEIGHT_ORDER[1:5]:
            weight_start(n)

    cos_f, sin_f, cos_b, sin_b = 0, 1, 2, 3

    def side_by_side(pieces, axis):
        return pieces[0] if len(pieces) == 1 else jnp.concatenate(pieces, axis=axis)

    def long_forward(pieces):
        y = matrix_left(table_ref, 0, side_by_side(pieces, 1))
        c, s = twiddle_ref[cos_f], twiddle_ref[sin_f]
        turned = []
        for n in range(len(pieces)):
            yr, yi = y[:SIDE, n * SIDE:(n + 1) * SIDE], y[SIDE:, n * SIDE:(n + 1) * SIDE]
            turned.append(jnp.concatenate([yr * c - yi * s, yr * s + yi * c], axis=1))
        z = matrix_right(table_ref, 1, side_by_side(turned, 0))
        return [
            (z[n * SIDE:(n + 1) * SIDE, :SIDE], z[n * SIDE:(n + 1) * SIDE, SIDE:])
            for n in range(len(pieces))
        ]

    def long_inverse(pairs):
        stacks = [jnp.concatenate([pair[0], pair[1]], axis=1) for pair in pairs]
        u = matrix_right(table_ref, 0, side_by_side(stacks, 0))
        c, s = twiddle_ref[cos_b], twiddle_ref[sin_b]
        turned = []
        for n in range(len(pairs)):
            ur, ui = u[n * SIDE:(n + 1) * SIDE, :SIDE], u[n * SIDE:(n + 1) * SIDE, SIDE:]
            turned.append(jnp.concatenate([ur * c - ui * s, ur * s + ui * c], axis=0))
        x = matrix_left(table_ref, 1, side_by_side(turned, 1))
        return [
            x[:, n * SIDE:(n + 1) * SIDE].reshape((2, groups) + TILE)
            for n in range(len(pairs))
        ]

    def legs_copy(row, g, offset):
        first, count = LEG_GROUPS[g]
        return send(
            offset, legs_out.at[row, first:first + count, :, peer_block(offset)],
            legs_in.at[row, me, first:first + count],
            (legs_left, legs_sem.at[g]),
        )

    def own_legs(row, g):
        first, count = LEG_GROUPS[g]
        return pltpu.make_async_copy(
            legs_out.at[row, first:first + count, :, my_block],
            legs_in.at[row, me, first:first + count],
            legs_sem.at[g],
        )

    def wait_weights(group, row):
        members = WEIGHT_GROUPS[group]

        @pl.when(jnp.logical_or(row == 1, far))
        def _():
            wait_all(weights.at[0:len(members), row], weight_sem.at[row, group])

    def slopes(row):
        along_x = (2 * freq_cols).astype(jnp.float32) / NC
        along_y = (2 * row_frequency(row)).astype(jnp.float32) / total_rows
        return along_x, along_y

    packed = jnp.where(first_row == 0, 0.5, 0.0)

    def both_rows(field):
        wait_all(spec_in.at[field], spec_sem.at[field])
        line = spec_in[field].reshape(2 * SIDE, SIDE)
        (ar, ai), (br, bi) = long_forward([line, jnp.concatenate([line[:SIDE], -line[SIDE:]], axis=0)])
        modes[field, 0, 0] = (1.0 - packed) * ar + packed * br
        modes[field, 0, 1] = (1.0 - packed) * ai + packed * bi
        modes[field, 1, 0] = (1.0 - 2.0 * packed) * br + packed * (ai - bi)
        modes[field, 1, 1] = (1.0 - 2.0 * packed) * bi + packed * (br - ar)

    def leg_step(row, carry):
        scaled = row_ratio * row_frequency(row)
        radius_sq = freq_cols * freq_cols + scaled * scaled
        floor = jnp.maximum(radius_sq, 1).astype(jnp.float32)
        cos2 = (freq_cols * freq_cols - scaled * scaled).astype(jnp.float32) / floor
        sin2 = (2 * freq_cols * scaled).astype(jnp.float32) / floor
        along_x, along_y = slopes(row)
        raising, lowering = (-along_y, along_x), (along_y, along_x)
        rot = (cos2, sin2)

        def temp_legs():
            t_bar = (weights[0, row] * modes[0, row, 0], weights[0, row] * modes[0, row, 1])
            return t_bar, complex_mul((weights[3, row] * t_bar[0], weights[3, row] * t_bar[1]), raising)

        def e_modes():
            return tuple(
                -weights[1, row] * (cos2 * modes[1, row, n] + sin2 * modes[2, row, n]) for n in range(2)
            )

        def spin_legs():
            e_bar = e_modes()
            w = complex_mul((-weights[4, row] * e_bar[0], -weights[4, row] * e_bar[1]), rot)
            return complex_mul(w, raising), complex_mul(w, lowering)

        def pol_leg():
            e_bar = e_modes()
            b_bar = tuple(
                weights[2, row] * (sin2 * modes[1, row, n] - cos2 * modes[2, row, n]) for n in range(2)
            )
            return (complex_mul((b_bar[1] - e_bar[0], -(e_bar[1] + b_bar[0])), rot),)

        for n, make in enumerate((temp_legs, spin_legs, pol_leg)):
            if n == 1:
                @pl.when(row == 0)
                def _():
                    both_rows(1)
                    both_rows(2)

            wait_weights(n, row)
            for k, leg_map in enumerate(long_inverse(make())):
                legs_out[row, LEG_GROUPS[n][0] + k] = leg_map
            each_peer(lambda offset: legs_copy(row, n, offset).start())
            own_legs(row, n).start()
        return carry

    wait_all(table_ref, load_sem.at[2])
    wait_all(twiddle_ref, load_sem.at[3])
    both_rows(0)
    lax.fori_loop(0, local_rows, leg_step, 0)
    weight_start(5)

    def map_step(n, carry):
        values = [
            (legs_in[place(k, my_h) + (n, 0)], legs_in[place(k, my_h) + (n, 1)])
            for k in range(total_rows)
        ]
        for y, (real, imag) in enumerate(short_transform(values, 1)):
            maps[n, 0, y] = real
            maps[n, 1, y] = imag
        return carry

    for g, (first, count) in enumerate(LEG_GROUPS):
        wait_all(legs_in.at[:, :, first:first + count], legs_sem.at[g])
        lax.fori_loop(first, first + count, map_step, 0)

    def product_step(y, carry):
        a, g, h3, h1, p = [(maps[n, 0, y], maps[n, 1, y]) for n in range(5)]
        ag, ph, hp = complex_mul(a, g), conj_mul(p, h3), conj_mul(h1, p)
        current[0, y] = ag[0] + 0.5 * (ph[0] + hp[0])
        current[1, y] = ag[1] + 0.5 * (ph[1] + hp[1])
        return carry

    lax.fori_loop(0, total_rows, product_step, 0)

    values = [(current[0, y], current[1, y]) for y in range(total_rows)]
    for k, (real, imag) in enumerate(short_transform(values, -1)):
        cur_out[place(k, my_h) + (0,)] = real
        cur_out[place(k, my_h) + (1,)] = imag

    def cur_copy(row, offset):
        return send(
            offset, cur_out.at[row, peer_of(offset)], cur_in.at[row, :, my_block],
            (cur_left, cur_sem.at[row]),
        )

    def own_cur(row):
        return pltpu.make_async_copy(
            cur_out.at[row, me], cur_in.at[row, :, my_block], cur_sem.at[row]
        )

    def cur_start(row, carry):
        each_peer(lambda offset: cur_copy(row, offset).start())
        own_cur(row).start()
        return carry

    lax.fori_loop(0, local_rows, cur_start, 0)

    def est_copy(row, offset):
        return send_home(
            offset, est_out.at[row, :, peer_block(offset)], est_in.at[row, me],
            (est_left, est_sem.at[0]),
        )

    ORIGIN = (0, 0, 0, 0)

    def own_est(row):
        return pltpu.make_async_copy(
            est_out.at[row, :, my_block], est_in.at[row, me], est_sem.at[0]
        )

    def estimate_step(row, carry):
        wait_all(cur_in.at[row], cur_sem.at[row])
        wait_weights(3, row)

        (modes,) = long_forward([cur_in[row].reshape(2 * SIDE, SIDE)])
        along_x, along_y = slopes(row)
        w = weights[5, row]
        estimate = complex_mul((w * modes[0], w * modes[1]), (along_y, along_x))
        (est_out[row],) = long_inverse([estimate])
        each_peer(lambda offset: est_copy(row, offset).start())

        @pl.when(stays)
        def _():
            own_est(row).start()

        @pl.when(jnp.logical_not(stays))
        def _():
            est_copy(row, ORIGIN).start()

        return carry

    lax.fori_loop(0, local_rows, estimate_step, 0)

    wait_all(est_in, est_sem.at[0])
    values = [
        (est_in[place(k, my_x) + (0,)], est_in[place(k, my_x) + (1,)])
        for k in range(total_rows)
    ]
    for y, (real, imag) in enumerate(short_transform(values, 1)):
        fin_out[y // in_rows, 0, y % in_rows] = real
        fin_out[y // in_rows, 1, y % in_rows] = imag

    def fin_copy(offset):
        r = row_of(offset)
        return remote(
            fin_out.at[r], fin_in.at[my_r], (fin_left, fin_sem.at[0]), my_x, r, my_z
        )

    for offset in ROW_OFFSETS[1:]:
        fin_copy(offset).start()
    own_fin = pltpu.make_async_copy(
        fin_out.at[my_r], fin_in.at[my_r], fin_sem.at[0]
    )
    own_fin.start()

    others = groups - 1

    @pl.when(stays)
    def _():
        wait_all(slab_out.at[0:3], slab_left)
        wait_all(relay_buf, forward_left)
        wait_all(est_out.at[:, :, 0:others], est_left)

    @pl.when(jnp.logical_not(stays))
    def _():
        wait_all(slab_out.at[0:2], slab_left)
        wait_all(relay_buf, relay_left)
        wait_all(est_out, est_left)

    @pl.when(far)
    def _():
        wait_all(weights.at[:, 0], extra_left)

    wait_all(weights.at[:, 0], weight_left)
    wait_all(spec_out.at[:, 0, 0:others], spec_left)
    wait_all(legs_out.at[:, :, :, 0:others], legs_left)
    wait_all(cur_out.at[:, 0:others], cur_left)
    wait_all(fin_in, fin_sem.at[0])
    for part in range(2):
        for t in range(tiles):
            out_ref[part, :, t * SIDE:(t + 1) * SIDE] = fin_in[t // 8, part, :, t % 8, :]

    wait_all(fin_out.at[0:3], fin_left)


def long_tables(total_rows):
    index = np.arange(SIDE)
    angle = 2.0 * np.pi * (index[:, None] * index[None, :] % SIDE) / SIDE
    c, s = np.cos(angle), np.sin(angle)
    forward = np.block([[c, s], [-s, c]]).astype(np.float32)
    tables = np.stack([forward, forward.T])
    top = tables.astype(jnp.bfloat16)
    rest = (tables - top.astype(np.float32)).astype(jnp.bfloat16)
    turn = 2.0 * np.pi * (index[:, None] * index[None, :]) / NC
    scale = 1.0 / (NC * total_rows)
    twiddle = np.stack(
        [np.cos(turn), -np.sin(turn), scale * np.cos(turn), scale * np.sin(turn)]
    ).astype(np.float32)
    return np.stack([top, rest], axis=1), twiddle


def fused_body(rows_count, fields_count, sky_maps, band_cuts, filters, wiener, response):
    groups = rows_count * fields_count
    local_rows = response.shape[0]
    total_rows = local_rows * groups
    in_rows = total_rows // rows_count
    table, twiddle = long_tables(total_rows)
    vmem = pl.BlockSpec(memory_space=pltpu.VMEM)
    f32 = jnp.float32
    dma = pltpu.SemaphoreType.DMA
    slab = pltpu.VMEM((rows_count, 3, in_rows) + TILE, f32)
    chunk = pltpu.VMEM((local_rows, groups, 2) + TILE, f32)
    lines = pltpu.VMEM((local_rows, 2, groups) + TILE, f32)
    final = pltpu.VMEM((rows_count, 2, in_rows) + TILE, f32)
    return pl.pallas_call(
        lens_kernel,
        out_shape=jax.ShapeDtypeStruct((2,) + sky_maps.shape[1:], f32),
        in_specs=[pl.BlockSpec(memory_space=pltpu.SMEM)] + [pl.BlockSpec(memory_space=pl.ANY)] * 6,
        out_specs=vmem,
        scratch_shapes=[
            pltpu.VMEM(table.shape, table.dtype), pltpu.VMEM(twiddle.shape, f32),
            pltpu.VMEM(sky_maps.shape, f32),
            pltpu.VMEM((6, local_rows, NC), f32),
            pltpu.VMEM((6, local_rows, SIDE, SIDE), f32),
            slab, slab,
            pltpu.VMEM((3, 2, in_rows) + TILE, f32),
            pltpu.VMEM((3, local_rows, groups, 2) + TILE, f32),
            pltpu.VMEM((3, 2, groups) + TILE, f32),
            pltpu.VMEM((6, 3, SIDE, SIDE), f32),
            pltpu.VMEM((3, local_rows, 2, SIDE, SIDE), f32),
            pltpu.VMEM((local_rows, 5, 2, groups) + TILE, f32),
            pltpu.VMEM((local_rows, groups, 5, 2) + TILE, f32),
            pltpu.VMEM((5, 2, total_rows) + TILE, f32),
            pltpu.VMEM((2, total_rows) + TILE, f32),
            chunk, lines, lines, chunk, final, final,
            dma((3,)), dma((3,)), dma((3,)), dma((local_rows, len(WEIGHT_GROUPS))), dma((len(LEG_GROUPS),)),
            dma((local_rows,)), dma((1,)), dma((1,)), dma((10,)), dma((4,)),
        ],
        compiler_params=pltpu.CompilerParams(
            collective_id=0, has_side_effects=True, vmem_limit_bytes=60 * 1024 * 1024
        ),
        name="lens",
    )(band_cuts, sky_maps, filters, wiener, response, jnp.asarray(table), jnp.asarray(twiddle))


def solution(mesh):
    placed = (
        P("sims", "rows", "fields"),
        P(),
        P(None, ("rows", "fields"), None),
        P(None, ("rows", "fields"), None),
        P(("rows", "fields"), None),
    )
    rows_count, fields_count = mesh.shape["rows"], mesh.shape["fields"]
    groups = rows_count * fields_count

    def choose(sky_maps, *rest):
        fits = (
            NC == SIDE * SIDE
            and (mesh.shape["sims"], rows_count, fields_count) == (2, 4, 4)
            and NC // groups == TILE[0] * TILE[1]
            and sky_maps.shape[0] == 3
            and sky_maps.shape[1] * rows_count == 32
        )
        if fits:
            return fused_body(rows_count, fields_count, sky_maps, *rest)
        return body(sky_maps, *rest)

    return jax.shard_map(
        choose, mesh=mesh, in_specs=placed, out_specs=P("sims", "rows", "fields"), check_vma=False
    )
```

```python
import functools
import math

import jax
import jax.numpy as jnp
import numpy as np
from jax import lax
from jax.experimental import pallas as pl
from jax.experimental.pallas import tpu as pltpu
from jax.sharding import PartitionSpec as P

NC = 16384


exact_mode = lax.Precision.HIGHEST


def split_factor(length):
    best_first = 1
    for divisor in range(1, math.isqrt(length) + 1):
        if length % divisor == 0:
            best_first = divisor
    return (best_first, length // best_first)


def phase_table(left_index, right_index, period, direction):
    product = left_index[:, None] * right_index[None, :] % period
    angles = direction * 2.0 * math.pi / period * product.astype(jnp.float32)
    return (jnp.cos(angles), jnp.sin(angles))


def complex_einsum(formula, data_pair, table_pair):
    data_real, data_imag = data_pair
    table_real, table_imag = table_pair
    real_out = jnp.einsum(formula, data_real, table_real, precision=exact_mode)
    imag_out = jnp.einsum(formula, data_real, table_imag, precision=exact_mode)
    if data_imag is not None:
        real_out = real_out - jnp.einsum(formula, data_imag, table_imag, precision=exact_mode)
        imag_out = imag_out + jnp.einsum(formula, data_imag, table_real, precision=exact_mode)
    return (real_out, imag_out)


def complex_mul(left_pair, right_pair):
    return (
        left_pair[0] * right_pair[0] - left_pair[1] * right_pair[1],
        left_pair[0] * right_pair[1] + left_pair[1] * right_pair[0],
    )


def conj_mul(left_pair, right_pair):
    return (
        left_pair[0] * right_pair[0] + left_pair[1] * right_pair[1],
        left_pair[0] * right_pair[1] - left_pair[1] * right_pair[0],
    )


def row_transform(data_pair, direction):
    batch_len, length, block_width = data_pair[0].shape
    outer_len, inner_len = split_factor(length)
    outer_ids = jnp.arange(outer_len, dtype=jnp.int32)
    inner_ids = jnp.arange(inner_len, dtype=jnp.int32)
    real_in = data_pair[0].reshape(batch_len, outer_len, inner_len, block_width)
    imag_in = None
    if data_pair[1] is not None:
        imag_in = data_pair[1].reshape(batch_len, outer_len, inner_len, block_width)
    middle = complex_einsum(
        "bjmc,jk->bkmc", (real_in, imag_in), phase_table(outer_ids, outer_ids, outer_len, direction)
    )
    twiddle = phase_table(outer_ids, inner_ids, length, direction)
    middle = complex_mul(middle, (twiddle[0][None, :, :, None], twiddle[1][None, :, :, None]))
    result = complex_einsum(
        "bkmc,mq->bqkc", middle, phase_table(inner_ids, inner_ids, inner_len, direction)
    )
    norm_factor = 1.0 if direction < 0 else 1.0 / length
    return (
        result[0].reshape(batch_len, length, block_width) * norm_factor,
        result[1].reshape(batch_len, length, block_width) * norm_factor,
    )


def block_order(groups, fields_count):
    positions = jnp.arange(groups, dtype=jnp.int32)
    blocks = positions % fields_count * (groups // fields_count) + positions // fields_count
    return (positions, blocks)


def column_forward(data_pair, groups, fields_count):
    batch_len, local_rows, total_len = data_pair[0].shape
    block_width = total_len // groups
    positions, blocks = block_order(groups, fields_count)
    column_ids = jnp.arange(block_width, dtype=jnp.int32)
    shaped = (
        data_pair[0].reshape(batch_len, local_rows, groups, block_width),
        data_pair[1].reshape(batch_len, local_rows, groups, block_width),
    )
    middle = complex_einsum("brpc,pk->brkc", shaped, phase_table(blocks, positions, groups, -1.0))
    twiddle = phase_table(positions, column_ids, total_len, -1.0)
    middle = complex_mul(middle, (twiddle[0][None, None], twiddle[1][None, None]))
    result = complex_einsum(
        "brkc,cq->brqk", middle, phase_table(column_ids, column_ids, block_width, -1.0)
    )
    return (
        result[0].reshape(batch_len, local_rows, total_len),
        result[1].reshape(batch_len, local_rows, total_len),
    )


def column_inverse(data_pair, groups, fields_count):
    batch_len, local_rows, total_len = data_pair[0].shape
    block_width = total_len // groups
    positions, blocks = block_order(groups, fields_count)
    column_ids = jnp.arange(block_width, dtype=jnp.int32)
    shaped = (
        data_pair[0].reshape(batch_len, local_rows, block_width, groups),
        data_pair[1].reshape(batch_len, local_rows, block_width, groups),
    )
    middle = complex_einsum(
        "brqk,qc->brkc", shaped, phase_table(column_ids, column_ids, block_width, 1.0)
    )
    twiddle = phase_table(positions, column_ids, total_len, 1.0)
    middle = complex_mul(middle, (twiddle[0][None, None], twiddle[1][None, None]))
    result = complex_einsum("brkc,kp->brpc", middle, phase_table(positions, blocks, groups, 1.0))
    norm_factor = 1.0 / total_len
    return (
        result[0].reshape(batch_len, local_rows, total_len) * norm_factor,
        result[1].reshape(batch_len, local_rows, total_len) * norm_factor,
    )


def body(sky_maps, band_cuts, filters, wiener, response):
    rows_count = lax.axis_size("rows")
    fields_count = lax.axis_size("fields")
    groups = rows_count * fields_count
    local_rows = filters.shape[1]
    total_rows = local_rows * groups
    row_ratio = NC // total_rows

    def forward_columns(stacked):
        return jnp.stack(column_forward((stacked[0], stacked[1]), groups, fields_count))

    def inverse_rows(stacked):
        return jnp.stack(row_transform((stacked[0], stacked[1]), 1.0))

    def inverse_columns(stacked):
        return jnp.stack(column_inverse((stacked[0], stacked[1]), groups, fields_count))

    def to_frequency(stacked):
        batch_len = stacked.shape[1]
        block_width = stacked.shape[3]
        shaped = stacked.reshape(
            2, batch_len, rows_count, fields_count, local_rows, 1, 1, block_width
        )
        arrived = lax.all_to_all(
            lax.all_to_all(shaped, "rows", split_axis=2, concat_axis=5, tiled=True),
            "fields",
            split_axis=3,
            concat_axis=6,
            tiled=True,
        )
        result = forward_columns(arrived.reshape(2, batch_len, local_rows, groups * block_width))
        return result

    def to_space(stacked):
        batch_len = stacked.shape[1]
        block_width = stacked.shape[3] // groups
        shaped = stacked.reshape(
            2, batch_len, 1, 1, local_rows, rows_count, fields_count, block_width
        )
        arrived = lax.all_to_all(
            lax.all_to_all(shaped, "rows", split_axis=5, concat_axis=2, tiled=True),
            "fields",
            split_axis=6,
            concat_axis=3,
            tiled=True,
        )
        result = inverse_rows(arrived.reshape(2, batch_len, total_rows, block_width))
        return result

    slab_spectra = jnp.stack(
        row_transform(
            (lax.all_to_all(sky_maps, "rows", split_axis=2, concat_axis=1, tiled=True), None), -1.0
        )
    )
    sky_spectra = to_frequency(slab_spectra)
    row_ids = lax.axis_index(("rows", "fields")) * local_rows + jnp.arange(
        local_rows, dtype=jnp.int32
    )
    freq_rows = jnp.where(row_ids < total_rows // 2, row_ids, row_ids - total_rows)[:, None]
    column_ids = jnp.arange(NC, dtype=jnp.int32)
    freq_cols = jnp.where(column_ids < NC // 2, column_ids, column_ids - NC)[None, :]
    scaled_rows = row_ratio * freq_rows
    radius_sq = freq_cols * freq_cols + scaled_rows * scaled_rows

    def band_mask(lower_cut, upper_cut):
        inside = (radius_sq >= lower_cut * lower_cut) & (radius_sq <= upper_cut * upper_cut)
        return inside.astype(jnp.float32)

    mask_temp = band_mask(band_cuts[0], band_cuts[1])
    mask_pol = band_mask(band_cuts[2], band_cuts[3])
    mask_out = band_mask(band_cuts[4], band_cuts[5])
    radius_floor = jnp.maximum(radius_sq, 1).astype(jnp.float32)
    cos_two = (freq_cols * freq_cols - scaled_rows * scaled_rows).astype(jnp.float32) / radius_floor
    sin_two = (2 * freq_cols * scaled_rows).astype(jnp.float32) / radius_floor
    along_x = (2 * freq_cols).astype(jnp.float32) / NC
    along_y = (2 * freq_rows).astype(jnp.float32) / total_rows
    raising = (-along_y + 0.0 * along_x, along_x + 0.0 * along_y)
    lowering = (along_y + 0.0 * along_x, along_x + 0.0 * along_y)
    rotation = (cos_two, sin_two)
    temp_modes = (sky_spectra[0, 0], sky_spectra[1, 0])
    stokes_q = (sky_spectra[0, 1], sky_spectra[1, 1])
    stokes_u = (sky_spectra[0, 2], sky_spectra[1, 2])
    e_modes = (
        -(cos_two * stokes_q[0] + sin_two * stokes_u[0]),
        -(cos_two * stokes_q[1] + sin_two * stokes_u[1]),
    )
    b_modes = (
        sin_two * stokes_q[0] - cos_two * stokes_u[0],
        sin_two * stokes_q[1] - cos_two * stokes_u[1],
    )
    temp_weight = mask_temp * filters[0]
    e_weight = mask_pol * filters[1]
    b_weight = mask_pol * filters[2]
    temp_bar = (temp_weight * temp_modes[0], temp_weight * temp_modes[1])
    e_bar = (e_weight * e_modes[0], e_weight * e_modes[1])
    b_bar = (b_weight * b_modes[0], b_weight * b_modes[1])
    grad_temp = complex_mul(raising, (wiener[0] * temp_bar[0], wiener[0] * temp_bar[1]))
    pol_sum = complex_mul((e_bar[0] - b_bar[1], e_bar[1] + b_bar[0]), rotation)
    pol_bar = (-pol_sum[0], -pol_sum[1])
    pol_rot = complex_mul((wiener[1] * e_bar[0], wiener[1] * e_bar[1]), rotation)
    pol_wiener = (-pol_rot[0], -pol_rot[1])
    spin_three = complex_mul(raising, pol_wiener)
    spin_one = complex_mul(lowering, pol_wiener)
    leg_spectra = jnp.stack(
        [
            jnp.stack([temp_bar[0], grad_temp[0], pol_bar[0], spin_three[0], spin_one[0]]),
            jnp.stack([temp_bar[1], grad_temp[1], pol_bar[1], spin_three[1], spin_one[1]]),
        ]
    )
    leg_maps = to_space(inverse_columns(leg_spectra))
    temp_leg = (leg_maps[0, 0], leg_maps[1, 0])
    grad_leg = (leg_maps[0, 1], leg_maps[1, 1])
    pol_leg = (leg_maps[0, 2], leg_maps[1, 2])
    three_leg = (leg_maps[0, 3], leg_maps[1, 3])
    one_leg = (leg_maps[0, 4], leg_maps[1, 4])
    temp_term = complex_mul(temp_leg, grad_leg)
    raise_term = conj_mul(pol_leg, three_leg)
    lower_term = conj_mul(one_leg, pol_leg)
    current = (
        temp_term[0] + 0.5 * (raise_term[0] + lower_term[0]),
        temp_term[1] + 0.5 * (raise_term[1] + lower_term[1]),
    )
    current_rows = jnp.stack(row_transform((current[0][None], current[1][None]), -1.0))
    current_modes = to_frequency(current_rows)
    out_weight = mask_out * response
    estimate_modes = complex_mul(
        lowering, (out_weight * current_modes[0, 0], out_weight * current_modes[1, 0])
    )
    estimate_stack = jnp.stack([estimate_modes[0][None], estimate_modes[1][None]])
    estimate_maps = to_space(inverse_columns(estimate_stack))
    slab_result = estimate_maps[:, 0]
    return lax.all_to_all(slab_result, "rows", split_axis=1, concat_axis=2, tiled=True)


SIDE = 128
TILE = (8, 128)
LEG_GROUPS = ((0, 2), (2, 2), (4, 1))
WEIGHT_GROUPS = ((0, 3), (1, 4), (2,), (5,))
MESH = pl.DeviceIdType.MESH


def add_pair(a, b):
    imag = a[1] if b[1] is None else b[1] if a[1] is None else a[1] + b[1]
    return (a[0] + b[0], imag)


def sub_pair(a, b):
    imag = a[1] if b[1] is None else -b[1] if a[1] is None else a[1] - b[1]
    return (a[0] - b[0], imag)


def turn_pair(value, step, length, direction):
    real, imag = value
    if step == 0:
        return value
    if 4 * step == length:
        if imag is None:
            return (jnp.zeros_like(real), real if direction > 0 else -real)
        return (-imag, real) if direction > 0 else (imag, -real)
    angle = 2.0 * math.pi * step / length
    c, s = math.cos(angle), direction * math.sin(angle)
    if imag is None:
        return (real * c, real * s)
    if 8 * step == length:
        if direction > 0:
            return ((real - imag) * c, (real + imag) * c)
        return ((real + imag) * c, (imag - real) * c)
    if 8 * step == 3 * length:
        if direction > 0:
            return ((real + imag) * c, (imag - real) * c)
        return ((real - imag) * c, (real + imag) * c)
    return (real * c - imag * s, real * s + imag * c)


def short_transform(values, direction):
    length = len(values)
    if length == 1:
        return values
    even = short_transform(values[0::2], direction)
    odd = short_transform(values[1::2], direction)
    low, high = [], []
    for step in range(length // 2):
        turned = turn_pair(odd[step], step, length, direction)
        low.append(add_pair(even[step], turned))
        high.append(sub_pair(even[step], turned))
    return low + high


def split_number(x):
    top = x.astype(jnp.bfloat16)
    return top, (x - top.astype(jnp.float32)).astype(jnp.bfloat16)


def dot32(a, b):
    return jnp.dot(a, b, preferred_element_type=jnp.float32)


def matrix_left(table_ref, which, x):
    top, rest = split_number(x)
    m_top, m_rest = table_ref[which, 0], table_ref[which, 1]
    return dot32(m_top, top) + (dot32(m_top, rest) + dot32(m_rest, top))


def matrix_right(table_ref, which, x):
    top, rest = split_number(x)
    m_top, m_rest = table_ref[which, 0], table_ref[which, 1]
    return dot32(top, m_top) + (dot32(top, m_rest) + dot32(rest, m_top))


BITS = (0, 1)
OFFSETS = [
    (c, a1, e, a0) for a0 in BITS for c, a1, e in
    ((1, 1, 1), (1, 0, 0), (0, 1, 0), (0, 0, 1), (1, 1, 0), (0, 1, 1), (1, 0, 1), (0, 0, 0))
]
PEERS = [offset for offset in OFFSETS if any(offset)]
WEIGHT_ORDER = (0, 3, 1, 4, 2, 5)


def lens_kernel(
    cuts_ref, sky_hbm, filters_hbm, wiener_hbm, response_hbm, table_hbm, twiddle_hbm, out_ref,
    table_ref, twiddle_ref, sky_ref, raw, weight_ref, slab_out, slab_in, relay_buf, relay_weights, spec_out, spec_in, weights, modes, legs_out, legs_in,
    maps, current, cur_out, cur_in, est_out, est_in, fin_out, fin_in,
    slab_sem, relay_sem, spec_sem, weight_sem, hand_sem, legs_sem, cur_sem, est_sem, fin_sem, send_sem, load_sem,
):
    rows_count, fields_count, local_rows = 4, 4, 2
    groups = rows_count * fields_count
    total_rows = groups * local_rows
    in_rows = total_rows // rows_count
    row_ratio = NC // total_rows
    my_x, my_r, my_z = (lax.axis_index(name) for name in ("sims", "rows", "fields"))
    my_y, my_c, my_h, my_l = my_r // 2, my_r % 2, my_z // 2, my_z % 2
    x_at, y_at, c_at, h_at, l_at = ((bit, 1 - bit) for bit in (my_x, my_y, my_c, my_h, my_l))
    me = my_r * fields_count + 2 * my_x + my_l
    my_block = (2 * my_x + my_l) * rows_count + my_r
    stays = my_x == my_h

    half_rows = total_rows // 2
    corner = my_x + my_l == 0
    far = jnp.logical_and(corner, my_y == 1)
    near = jnp.logical_and(corner, my_y == 0)
    home_row = in_rows * my_r + 4 * my_h + 2 * my_l + my_x
    first_row = jnp.where(corner, in_rows * my_c + 4 * (my_h + my_y - 2 * my_h * my_y), home_row)

    def signed(row):
        return jnp.where(row < half_rows, row, row - total_rows)

    def row_of(offset):
        return 2 * y_at[offset[1]] + c_at[offset[3]]

    def peer_of(offset):
        return row_of(offset) * fields_count + 2 * x_at[offset[0]] + l_at[offset[2]]

    def peer_block(offset):
        return (2 * x_at[offset[0]] + l_at[offset[2]]) * rows_count + row_of(offset)

    def remote(src, dst, sems, x, r, z):
        return pltpu.make_async_remote_copy(
            src_ref=src, dst_ref=dst, send_sem=sems[0], recv_sem=sems[1],
            device_id={"sims": x, "rows": r, "fields": z}, device_id_type=MESH,
        )

    def send(offset, src, dst, sems):
        return remote(src, dst, sems, x_at[offset[0]], row_of(offset), 2 * my_h + l_at[offset[2]])

    def send_home(offset, src, dst, sems):
        return remote(src, dst, sems, my_h, row_of(offset), 2 * x_at[offset[0]] + l_at[offset[2]])

    def each_peer(body):
        for offset in PEERS:
            body(offset)

    def wait_all(ref, sem):
        pltpu.make_async_copy(ref, ref, sem).wait()

    for src, dst, n in (
        (sky_hbm, sky_ref, 0),
        (filters_hbm, raw.at[0:3], 1),
        (wiener_hbm, raw.at[3:5], 1),
        (response_hbm, raw.at[5], 1),
        (table_hbm, table_ref, 2),
        (twiddle_hbm, twiddle_ref, 3),
    ):
        pltpu.make_async_copy(src, dst, load_sem.at[n]).start()

    (
        slab_left, relay_left, forward_left, spec_left, weight_left, legs_left, cur_left, est_left, fin_left,
        extra_left, pass_left,
    ) = (send_sem.at[n] for n in range(11))

    barrier = pltpu.get_barrier_semaphore()
    for h in BITS:
        for c, a1, e, a0 in OFFSETS:
            if h or c or a1 or e or a0:
                pl.semaphore_signal(
                    barrier, inc=1, device_id_type=MESH,
                    device_id={"sims": x_at[c], "rows": 2 * y_at[a1] + c_at[a0], "fields": 2 * h_at[h] + l_at[e]},
                )
    wait_all(sky_ref, load_sem.at[0])
    tiles = sky_ref.shape[2] // SIDE
    for field in range(3):
        for t in range(tiles):
            slab_out[t // 8, field, :, t % 8, :] = sky_ref[field, :, t * SIDE:(t + 1) * SIDE]
    pl.semaphore_wait(barrier, 2 * groups - 1)

    ROW_OFFSETS = [(0, a1, 0, a0) for a1 in BITS for a0 in BITS]

    def slab_copy(field, offset):
        r = row_of(offset)
        return send_home(
            offset, slab_out.at[r, field], slab_in.at[my_r, field],
            (slab_left, slab_sem.at[field]),
        )

    def own_slab(field):
        return pltpu.make_async_copy(slab_out.at[my_r, field], slab_in.at[my_r, field], slab_sem.at[field])

    def relay_copy(field):
        return remote(
            slab_out.at[pl.ds(2 * y_at[1], 2), field], relay_buf.at[field],
            (relay_left, relay_sem.at[field]), x_at[1], my_r, my_z,
        )

    def forward_copy(field, core):
        a0 = core
        return remote(
            relay_buf.at[field, c_at[a0]], slab_in.at[my_r, field],
            (forward_left, slab_sem.at[field]),
            my_x, 2 * y_at[1] + c_at[a0], 2 * h_at[1] + my_l,
        )

    @pl.when(stays)
    def _():
        for field in range(3):
            own_slab(field).start()
            for offset in ROW_OFFSETS[1:]:
                slab_copy(field, offset).start()

    def slab_start(field):
        relay_copy(field).start()
        for offset in ROW_OFFSETS[:2]:
            slab_copy(field, offset).start()

    @pl.when(jnp.logical_not(stays))
    def _():
        slab_start(0)

    low_index = lax.broadcasted_iota(jnp.int32, (SIDE, SIDE), 0)
    high_index = lax.broadcasted_iota(jnp.int32, (SIDE, SIDE), 1)
    column_ids = low_index + SIDE * high_index
    freq_cols = jnp.where(column_ids < NC // 2, column_ids, column_ids - NC)

    def row_frequency(row):
        return jnp.where(first_row == 0, -half_rows * row, signed(first_row) * (1 - 2 * row))

    wait_all(raw, load_sem.at[1])

    def spread(n, carry):
        for j in range(8):
            start = pl.multiple_of((n * 8 + j) * SIDE, SIDE)
            weight_ref[:, :, n * 8 + j, :] = raw[:, :, pl.ds(start, SIDE)]
        return carry

    lax.fori_loop(0, SIDE // 8, spread, 0)
    scaled_home = row_ratio * signed(home_row)
    radius_home = freq_cols * freq_cols + scaled_home * scaled_home

    def mask(n):
        low, high = cuts_ref[2 * n], cuts_ref[2 * n + 1]
        inside = (radius_home >= low * low) & (radius_home <= high * high)
        return inside.astype(jnp.float32)

    home_slot = jnp.where(far, 2, 0)
    outer = my_l == my_h
    inner = my_l != my_h

    def group_of(n):
        return [n in members for members in WEIGHT_GROUPS].index(True)

    def weight_copy(n, source, low, sem):
        cornered = my_x + low == 0
        upper, lower = jnp.logical_and(cornered, my_y == 0), jnp.logical_and(cornered, my_y == 1)
        other_r = jnp.where(upper, my_r + 2, jnp.where(lower, jnp.where(my_h == 0, my_r, 5 - my_r), 3 - my_r))
        slot = jnp.where(upper, 0, 1)
        return remote(
            source, weights.at[n, slot], (sem, weight_sem.at[slot, group_of(n)]),
            my_x, other_r, 2 * h_at[1] + jnp.where(my_x == 1, 1 - low, low),
        )

    def own_weight(n):
        return weight_copy(n, weights.at[n, home_slot], my_l, weight_left)

    def hand_copy(n):
        return remote(
            weights.at[n, home_slot], relay_weights.at[n], (weight_left, hand_sem.at[n]),
            my_x, my_r, 2 * my_h + l_at[1],
        )

    def extra_copy(n):
        return remote(
            weights.at[n, home_slot], weights.at[n, 1], (extra_left, weight_sem.at[1, group_of(n)]),
            my_x, jnp.where(my_h == 0, my_r - 2, 3 - my_r), my_z,
        )

    def weight_start(members):
        @pl.when(outer)
        def _():
            for n in members:
                hand_copy(n).start()

        @pl.when(inner)
        def _():
            for n in members:
                own_weight(n).start()

        @pl.when(far)
        def _():
            for n in members:
                extra_copy(n).start()

    def weight_pass_on(members):
        @pl.when(inner)
        def _():
            for n in members:
                wait_all(relay_weights.at[n], hand_sem.at[n])
                weight_copy(n, relay_weights.at[n], l_at[1], pass_left).start()

    pol = mask(1)
    weights[0, home_slot] = mask(0) * weight_ref[0, my_x].T
    weights[1, home_slot] = pol * weight_ref[1, my_x].T
    weights[2, home_slot] = pol * weight_ref[2, my_x].T
    weights[3, home_slot] = weight_ref[3, my_x].T
    weights[4, home_slot] = weight_ref[4, my_x].T
    weights[5, home_slot] = mask(2) * weight_ref[5, my_x].T
    @pl.when(jnp.logical_and(inner, jnp.logical_not(stays)))
    def _():
        slab_start(1)
        slab_start(2)
        for n in WEIGHT_ORDER[:5]:
            own_weight(n).start()

    @pl.when(jnp.logical_and(outer, jnp.logical_not(stays)))
    def _():
        hand_copy(0).start()
        slab_start(1)
        hand_copy(3).start()
        slab_start(2)
        hand_copy(1).start()

    @pl.when(jnp.logical_and(inner, stays))
    def _():
        own_weight(0).start()

    @pl.when(jnp.logical_and(outer, stays))
    def _():
        hand_copy(0).start()
        hand_copy(3).start()

    def owner(k):
        return k // 8 * fields_count + 2 * (k % 2) + k // 2 % 2

    def place(k, half):
        if k % 4 == 0:
            base = k % half_rows if k <= half_rows else total_rows - k
            upper = half if base % 8 == 0 else 1 - half
            return int(k >= half_rows), (base // in_rows + 2 * upper) * fields_count
        away = 1 - half if k // 4 % 2 else half
        return away, owner(k) + away * (owner(total_rows - k) - owner(k))

    def spec_copy(field, offset):
        return send(
            offset, spec_out.at[field, 0, peer_of(offset)], spec_in.at[field, :, my_block],
            (spec_left, spec_sem.at[field]),
        )

    def own_spec(field):
        return pltpu.make_async_copy(
            spec_out.at[field, 0, me], spec_in.at[field, :, my_block], spec_sem.at[field]
        )

    def spec_start(field):
        each_peer(lambda offset: spec_copy(field, offset).start())
        own_spec(field).start()

    def row_step(field):
        @pl.when(stays)
        def _():
            wait_all(relay_buf.at[field], relay_sem.at[field])
            for core in BITS:
                forward_copy(field, core).start()

        if field == 1:
            @pl.when(jnp.logical_and(outer, stays))
            def _():
                hand_copy(1).start()

        if field == 2:
            @pl.when(jnp.logical_and(inner, stays))
            def _():
                for n in WEIGHT_ORDER[1:5]:
                    own_weight(n).start()

        wait_all(slab_in.at[:, field], slab_sem.at[field])
        values = [
            (slab_in[y // in_rows, field, y % in_rows], None) for y in range(total_rows)
        ]
        lines = short_transform(values, -1)
        lines[0] = (lines[0][0], lines[half_rows][0])
        for k, (real, imag) in enumerate(lines):
            if k % 4 == 0 and k >= half_rows:
                continue
            local, device = place(k, my_h)
            spec_out[field, local, device, 0] = real
            spec_out[field, local, device, 1] = imag
        spec_start(field)

    for field in range(3):
        row_step(field)

    @pl.when(outer)
    def _():
        hand_copy(4).start()
        hand_copy(2).start()

    @pl.when(far)
    def _():
        for n in WEIGHT_ORDER[:5]:
            extra_copy(n).start()

    weight_pass_on((0, 3, 1))

    cos_f, sin_f, cos_b, sin_b = 0, 1, 2, 3

    def side_by_side(pieces, axis):
        return pieces[0] if len(pieces) == 1 else jnp.concatenate(pieces, axis=axis)

    def long_forward(pieces):
        y = matrix_left(table_ref, 0, side_by_side(pieces, 1))
        c, s = twiddle_ref[cos_f], twiddle_ref[sin_f]
        turned = []
        for n in range(len(pieces)):
            yr, yi = y[:SIDE, n * SIDE:(n + 1) * SIDE], y[SIDE:, n * SIDE:(n + 1) * SIDE]
            turned.append(jnp.concatenate([yr * c - yi * s, yr * s + yi * c], axis=1))
        z = matrix_right(table_ref, 1, side_by_side(turned, 0))
        return [
            (z[n * SIDE:(n + 1) * SIDE, :SIDE], z[n * SIDE:(n + 1) * SIDE, SIDE:])
            for n in range(len(pieces))
        ]

    def long_inverse(pairs):
        stacks = [jnp.concatenate([pair[0], pair[1]], axis=1) for pair in pairs]
        u = matrix_right(table_ref, 0, side_by_side(stacks, 0))
        c, s = twiddle_ref[cos_b], twiddle_ref[sin_b]
        turned = []
        for n in range(len(pairs)):
            ur, ui = u[n * SIDE:(n + 1) * SIDE, :SIDE], u[n * SIDE:(n + 1) * SIDE, SIDE:]
            turned.append(jnp.concatenate([ur * c - ui * s, ur * s + ui * c], axis=0))
        x = matrix_left(table_ref, 1, side_by_side(turned, 1))
        return [
            x[:, n * SIDE:(n + 1) * SIDE].reshape((2, groups) + TILE)
            for n in range(len(pairs))
        ]

    def legs_copy(row, g, offset):
        first, count = LEG_GROUPS[g]
        return send(
            offset, legs_out.at[row, first:first + count, :, peer_block(offset)],
            legs_in.at[row, me, first:first + count],
            (legs_left, legs_sem.at[g]),
        )

    def own_legs(row, g):
        first, count = LEG_GROUPS[g]
        return pltpu.make_async_copy(
            legs_out.at[row, first:first + count, :, my_block],
            legs_in.at[row, me, first:first + count],
            legs_sem.at[g],
        )

    def wait_weights(group, row):
        members = WEIGHT_GROUPS[group]

        @pl.when(jnp.logical_or(row == 1, far))
        def _():
            wait_all(weights.at[0:len(members), row], weight_sem.at[row, group])

    def slopes(row):
        along_x = (2 * freq_cols).astype(jnp.float32) / NC
        along_y = (2 * row_frequency(row)).astype(jnp.float32) / total_rows
        return along_x, along_y

    packed = jnp.where(first_row == 0, 0.5, 0.0)

    def both_rows(field):
        wait_all(spec_in.at[field], spec_sem.at[field])
        line = spec_in[field].reshape(2 * SIDE, SIDE)
        (ar, ai), (br, bi) = long_forward([line, jnp.concatenate([line[:SIDE], -line[SIDE:]], axis=0)])
        modes[field, 0, 0] = (1.0 - packed) * ar + packed * br
        modes[field, 0, 1] = (1.0 - packed) * ai + packed * bi
        modes[field, 1, 0] = (1.0 - 2.0 * packed) * br + packed * (ai - bi)
        modes[field, 1, 1] = (1.0 - 2.0 * packed) * bi + packed * (br - ar)

    def leg_step(n, row):
        scaled = row_ratio * row_frequency(row)
        radius_sq = freq_cols * freq_cols + scaled * scaled
        floor = jnp.maximum(radius_sq, 1).astype(jnp.float32)
        cos2 = (freq_cols * freq_cols - scaled * scaled).astype(jnp.float32) / floor
        sin2 = (2 * freq_cols * scaled).astype(jnp.float32) / floor
        along_x, along_y = slopes(row)
        raising, lowering = (-along_y, along_x), (along_y, along_x)
        rot = (cos2, sin2)

        def temp_legs():
            t_bar = (weights[0, row] * modes[0, row, 0], weights[0, row] * modes[0, row, 1])
            return t_bar, complex_mul((weights[3, row] * t_bar[0], weights[3, row] * t_bar[1]), raising)

        def e_modes():
            return tuple(
                -weights[1, row] * (cos2 * modes[1, row, n] + sin2 * modes[2, row, n]) for n in range(2)
            )

        def spin_legs():
            e_bar = e_modes()
            w = complex_mul((-weights[4, row] * e_bar[0], -weights[4, row] * e_bar[1]), rot)
            return complex_mul(w, raising), complex_mul(w, lowering)

        def pol_leg():
            e_bar = e_modes()
            b_bar = tuple(
                weights[2, row] * (sin2 * modes[1, row, n] - cos2 * modes[2, row, n]) for n in range(2)
            )
            return (complex_mul((b_bar[1] - e_bar[0], -(e_bar[1] + b_bar[0])), rot),)

        wait_weights(n, row)
        for k, leg_map in enumerate(long_inverse((temp_legs, spin_legs, pol_leg)[n]())):
            legs_out[row, LEG_GROUPS[n][0] + k] = leg_map
        each_peer(lambda offset: legs_copy(row, n, offset).start())
        own_legs(row, n).start()

    wait_all(table_ref, load_sem.at[2])
    wait_all(twiddle_ref, load_sem.at[3])
    both_rows(0)

    @pl.when(jnp.logical_not(far))
    def _():
        leg_step(0, 0)

    both_rows(1)
    both_rows(2)
    weight_pass_on((4, 2))

    @pl.when(far)
    def _():
        for n in range(len(LEG_GROUPS)):
            def group_steps(row, carry):
                leg_step(n, row)
                return carry

            lax.fori_loop(0, local_rows, group_steps, 0)

    @pl.when(jnp.logical_not(far))
    def _():
        leg_step(1, 0)
        leg_step(2, 0)
        for n in range(len(LEG_GROUPS)):
            leg_step(n, 1)

    weight_start((5,))

    def map_step(n, carry):
        values = [
            (legs_in[place(k, my_h) + (n, 0)], legs_in[place(k, my_h) + (n, 1)])
            for k in range(total_rows)
        ]
        for y, (real, imag) in enumerate(short_transform(values, 1)):
            maps[n, 0, y] = real
            maps[n, 1, y] = imag
        return carry

    for g, (first, count) in enumerate(LEG_GROUPS):
        wait_all(legs_in.at[:, :, first:first + count], legs_sem.at[g])
        lax.fori_loop(first, first + count, map_step, 0)

    def product_step(y, carry):
        a, g, h3, h1, p = [(maps[n, 0, y], maps[n, 1, y]) for n in range(5)]
        ag, ph, hp = complex_mul(a, g), conj_mul(p, h3), conj_mul(h1, p)
        current[0, y] = ag[0] + 0.5 * (ph[0] + hp[0])
        current[1, y] = ag[1] + 0.5 * (ph[1] + hp[1])
        return carry

    lax.fori_loop(0, total_rows, product_step, 0)

    values = [(current[0, y], current[1, y]) for y in range(total_rows)]
    for k, (real, imag) in enumerate(short_transform(values, -1)):
        cur_out[place(k, my_h) + (0,)] = real
        cur_out[place(k, my_h) + (1,)] = imag

    def cur_copy(row, offset):
        return send(
            offset, cur_out.at[row, peer_of(offset)], cur_in.at[row, :, my_block],
            (cur_left, cur_sem.at[row]),
        )

    def own_cur(row):
        return pltpu.make_async_copy(
            cur_out.at[row, me], cur_in.at[row, :, my_block], cur_sem.at[row]
        )

    def cur_start(row, carry):
        each_peer(lambda offset: cur_copy(row, offset).start())
        own_cur(row).start()
        return carry

    lax.fori_loop(0, local_rows, cur_start, 0)
    weight_pass_on((5,))

    def est_copy(row, offset):
        return send_home(
            offset, est_out.at[row, :, peer_block(offset)], est_in.at[row, me],
            (est_left, est_sem.at[0]),
        )

    ORIGIN = (0, 0, 0, 0)

    def own_est(row):
        return pltpu.make_async_copy(
            est_out.at[row, :, my_block], est_in.at[row, me], est_sem.at[0]
        )

    def estimate_step(row, carry):
        wait_all(cur_in.at[row], cur_sem.at[row])
        wait_weights(3, row)

        (modes,) = long_forward([cur_in[row].reshape(2 * SIDE, SIDE)])
        along_x, along_y = slopes(row)
        w = weights[5, row]
        estimate = complex_mul((w * modes[0], w * modes[1]), (along_y, along_x))
        (est_out[row],) = long_inverse([estimate])
        each_peer(lambda offset: est_copy(row, offset).start())

        @pl.when(stays)
        def _():
            own_est(row).start()

        @pl.when(jnp.logical_not(stays))
        def _():
            est_copy(row, ORIGIN).start()

        return carry

    lax.fori_loop(0, local_rows, estimate_step, 0)

    wait_all(est_in, est_sem.at[0])
    values = [
        (est_in[place(k, my_x) + (0,)], est_in[place(k, my_x) + (1,)])
        for k in range(total_rows)
    ]
    for y, (real, imag) in enumerate(short_transform(values, 1)):
        fin_out[y // in_rows, 0, y % in_rows] = real
        fin_out[y // in_rows, 1, y % in_rows] = imag

    def fin_copy(offset):
        r = row_of(offset)
        return remote(
            fin_out.at[r], fin_in.at[my_r], (fin_left, fin_sem.at[0]), my_x, r, my_z
        )

    for offset in ROW_OFFSETS[1:]:
        fin_copy(offset).start()
    own_fin = pltpu.make_async_copy(
        fin_out.at[my_r], fin_in.at[my_r], fin_sem.at[0]
    )
    own_fin.start()

    others = groups - 1

    @pl.when(stays)
    def _():
        wait_all(slab_out.at[0:3], slab_left)
        wait_all(relay_buf, forward_left)
        wait_all(est_out.at[:, :, 0:others], est_left)

    @pl.when(jnp.logical_not(stays))
    def _():
        wait_all(slab_out.at[0:2], slab_left)
        wait_all(relay_buf, relay_left)
        wait_all(est_out, est_left)

    @pl.when(far)
    def _():
        wait_all(weights.at[:, 0], extra_left)

    @pl.when(inner)
    def _():
        wait_all(relay_weights, pass_left)

    wait_all(weights.at[:, 0], weight_left)
    wait_all(spec_out.at[:, 0, 0:others], spec_left)
    wait_all(legs_out.at[:, :, :, 0:others], legs_left)
    wait_all(cur_out.at[:, 0:others], cur_left)
    wait_all(fin_in, fin_sem.at[0])
    for part in range(2):
        for t in range(tiles):
            out_ref[part, :, t * SIDE:(t + 1) * SIDE] = fin_in[t // 8, part, :, t % 8, :]

    wait_all(fin_out.at[0:3], fin_left)


def long_tables(total_rows):
    index = np.arange(SIDE)
    angle = 2.0 * np.pi * (index[:, None] * index[None, :] % SIDE) / SIDE
    c, s = np.cos(angle), np.sin(angle)
    forward = np.block([[c, s], [-s, c]]).astype(np.float32)
    tables = np.stack([forward, forward.T])
    top = tables.astype(jnp.bfloat16)
    rest = (tables - top.astype(np.float32)).astype(jnp.bfloat16)
    turn = 2.0 * np.pi * (index[:, None] * index[None, :]) / NC
    scale = 1.0 / (NC * total_rows)
    twiddle = np.stack(
        [np.cos(turn), -np.sin(turn), scale * np.cos(turn), scale * np.sin(turn)]
    ).astype(np.float32)
    return np.stack([top, rest], axis=1), twiddle


def fused_body(rows_count, fields_count, sky_maps, band_cuts, filters, wiener, response):
    groups = rows_count * fields_count
    local_rows = response.shape[0]
    total_rows = local_rows * groups
    in_rows = total_rows // rows_count
    table, twiddle = long_tables(total_rows)
    vmem = pl.BlockSpec(memory_space=pltpu.VMEM)
    f32 = jnp.float32
    dma = pltpu.SemaphoreType.DMA
    slab = pltpu.VMEM((rows_count, 3, in_rows) + TILE, f32)
    chunk = pltpu.VMEM((local_rows, groups, 2) + TILE, f32)
    lines = pltpu.VMEM((local_rows, 2, groups) + TILE, f32)
    final = pltpu.VMEM((rows_count, 2, in_rows) + TILE, f32)
    return pl.pallas_call(
        lens_kernel,
        out_shape=jax.ShapeDtypeStruct((2,) + sky_maps.shape[1:], f32),
        in_specs=[pl.BlockSpec(memory_space=pltpu.SMEM)] + [pl.BlockSpec(memory_space=pl.ANY)] * 6,
        out_specs=vmem,
        scratch_shapes=[
            pltpu.VMEM(table.shape, table.dtype), pltpu.VMEM(twiddle.shape, f32),
            pltpu.VMEM(sky_maps.shape, f32),
            pltpu.VMEM((6, local_rows, NC), f32),
            pltpu.VMEM((6, local_rows, SIDE, SIDE), f32),
            slab, slab,
            pltpu.VMEM((3, 2, in_rows) + TILE, f32),
            pltpu.VMEM((6, SIDE, SIDE), f32),
            pltpu.VMEM((3, local_rows, groups, 2) + TILE, f32),
            pltpu.VMEM((3, 2, groups) + TILE, f32),
            pltpu.VMEM((6, 3, SIDE, SIDE), f32),
            pltpu.VMEM((3, local_rows, 2, SIDE, SIDE), f32),
            pltpu.VMEM((local_rows, 5, 2, groups) + TILE, f32),
            pltpu.VMEM((local_rows, groups, 5, 2) + TILE, f32),
            pltpu.VMEM((5, 2, total_rows) + TILE, f32),
            pltpu.VMEM((2, total_rows) + TILE, f32),
            chunk, lines, lines, chunk, final, final,
            dma((3,)), dma((3,)), dma((3,)), dma((local_rows, len(WEIGHT_GROUPS))), dma((6,)), dma((len(LEG_GROUPS),)),
            dma((local_rows,)), dma((1,)), dma((1,)), dma((11,)), dma((4,)),
        ],
        compiler_params=pltpu.CompilerParams(
            collective_id=0, has_side_effects=True, vmem_limit_bytes=60 * 1024 * 1024
        ),
        name="lens",
    )(band_cuts, sky_maps, filters, wiener, response, jnp.asarray(table), jnp.asarray(twiddle))


def solution(mesh):
    placed = (
        P("sims", "rows", "fields"),
        P(),
        P(None, ("rows", "fields"), None),
        P(None, ("rows", "fields"), None),
        P(("rows", "fields"), None),
    )
    rows_count, fields_count = mesh.shape["rows"], mesh.shape["fields"]
    groups = rows_count * fields_count

    def choose(sky_maps, *rest):
        fits = (
            NC == SIDE * SIDE
            and (mesh.shape["sims"], rows_count, fields_count) == (2, 4, 4)
            and NC // groups == TILE[0] * TILE[1]
            and sky_maps.shape[0] == 3
            and sky_maps.shape[1] * rows_count == 32
        )
        if fits:
            return fused_body(rows_count, fields_count, sky_maps, *rest)
        return body(sky_maps, *rest)

    return jax.shard_map(
        choose, mesh=mesh, in_specs=placed, out_specs=P("sims", "rows", "fields"), check_vma=False
    )
```

```python
import functools
import math

import jax
import jax.numpy as jnp
import numpy as np
from jax import lax
from jax.experimental import pallas as pl
from jax.experimental.pallas import tpu as pltpu
from jax.sharding import PartitionSpec as P

NC = 16384


exact_mode = lax.Precision.HIGHEST


def split_factor(length):
    best_first = 1
    for divisor in range(1, math.isqrt(length) + 1):
        if length % divisor == 0:
            best_first = divisor
    return (best_first, length // best_first)


def phase_table(left_index, right_index, period, direction):
    product = left_index[:, None] * right_index[None, :] % period
    angles = direction * 2.0 * math.pi / period * product.astype(jnp.float32)
    return (jnp.cos(angles), jnp.sin(angles))


def complex_einsum(formula, data_pair, table_pair):
    data_real, data_imag = data_pair
    table_real, table_imag = table_pair
    real_out = jnp.einsum(formula, data_real, table_real, precision=exact_mode)
    imag_out = jnp.einsum(formula, data_real, table_imag, precision=exact_mode)
    if data_imag is not None:
        real_out = real_out - jnp.einsum(formula, data_imag, table_imag, precision=exact_mode)
        imag_out = imag_out + jnp.einsum(formula, data_imag, table_real, precision=exact_mode)
    return (real_out, imag_out)


def complex_mul(left_pair, right_pair):
    return (
        left_pair[0] * right_pair[0] - left_pair[1] * right_pair[1],
        left_pair[0] * right_pair[1] + left_pair[1] * right_pair[0],
    )


def conj_mul(left_pair, right_pair):
    return (
        left_pair[0] * right_pair[0] + left_pair[1] * right_pair[1],
        left_pair[0] * right_pair[1] - left_pair[1] * right_pair[0],
    )


def row_transform(data_pair, direction):
    batch_len, length, block_width = data_pair[0].shape
    outer_len, inner_len = split_factor(length)
    outer_ids = jnp.arange(outer_len, dtype=jnp.int32)
    inner_ids = jnp.arange(inner_len, dtype=jnp.int32)
    real_in = data_pair[0].reshape(batch_len, outer_len, inner_len, block_width)
    imag_in = None
    if data_pair[1] is not None:
        imag_in = data_pair[1].reshape(batch_len, outer_len, inner_len, block_width)
    middle = complex_einsum(
        "bjmc,jk->bkmc", (real_in, imag_in), phase_table(outer_ids, outer_ids, outer_len, direction)
    )
    twiddle = phase_table(outer_ids, inner_ids, length, direction)
    middle = complex_mul(middle, (twiddle[0][None, :, :, None], twiddle[1][None, :, :, None]))
    result = complex_einsum(
        "bkmc,mq->bqkc", middle, phase_table(inner_ids, inner_ids, inner_len, direction)
    )
    norm_factor = 1.0 if direction < 0 else 1.0 / length
    return (
        result[0].reshape(batch_len, length, block_width) * norm_factor,
        result[1].reshape(batch_len, length, block_width) * norm_factor,
    )


def block_order(groups, fields_count):
    positions = jnp.arange(groups, dtype=jnp.int32)
    blocks = positions % fields_count * (groups // fields_count) + positions // fields_count
    return (positions, blocks)


def column_forward(data_pair, groups, fields_count):
    batch_len, local_rows, total_len = data_pair[0].shape
    block_width = total_len // groups
    positions, blocks = block_order(groups, fields_count)
    column_ids = jnp.arange(block_width, dtype=jnp.int32)
    shaped = (
        data_pair[0].reshape(batch_len, local_rows, groups, block_width),
        data_pair[1].reshape(batch_len, local_rows, groups, block_width),
    )
    middle = complex_einsum("brpc,pk->brkc", shaped, phase_table(blocks, positions, groups, -1.0))
    twiddle = phase_table(positions, column_ids, total_len, -1.0)
    middle = complex_mul(middle, (twiddle[0][None, None], twiddle[1][None, None]))
    result = complex_einsum(
        "brkc,cq->brqk", middle, phase_table(column_ids, column_ids, block_width, -1.0)
    )
    return (
        result[0].reshape(batch_len, local_rows, total_len),
        result[1].reshape(batch_len, local_rows, total_len),
    )


def column_inverse(data_pair, groups, fields_count):
    batch_len, local_rows, total_len = data_pair[0].shape
    block_width = total_len // groups
    positions, blocks = block_order(groups, fields_count)
    column_ids = jnp.arange(block_width, dtype=jnp.int32)
    shaped = (
        data_pair[0].reshape(batch_len, local_rows, block_width, groups),
        data_pair[1].reshape(batch_len, local_rows, block_width, groups),
    )
    middle = complex_einsum(
        "brqk,qc->brkc", shaped, phase_table(column_ids, column_ids, block_width, 1.0)
    )
    twiddle = phase_table(positions, column_ids, total_len, 1.0)
    middle = complex_mul(middle, (twiddle[0][None, None], twiddle[1][None, None]))
    result = complex_einsum("brkc,kp->brpc", middle, phase_table(positions, blocks, groups, 1.0))
    norm_factor = 1.0 / total_len
    return (
        result[0].reshape(batch_len, local_rows, total_len) * norm_factor,
        result[1].reshape(batch_len, local_rows, total_len) * norm_factor,
    )


def body(sky_maps, band_cuts, filters, wiener, response):
    rows_count = lax.axis_size("rows")
    fields_count = lax.axis_size("fields")
    groups = rows_count * fields_count
    local_rows = filters.shape[1]
    total_rows = local_rows * groups
    row_ratio = NC // total_rows

    def forward_columns(stacked):
        return jnp.stack(column_forward((stacked[0], stacked[1]), groups, fields_count))

    def inverse_rows(stacked):
        return jnp.stack(row_transform((stacked[0], stacked[1]), 1.0))

    def inverse_columns(stacked):
        return jnp.stack(column_inverse((stacked[0], stacked[1]), groups, fields_count))

    def to_frequency(stacked):
        batch_len = stacked.shape[1]
        block_width = stacked.shape[3]
        shaped = stacked.reshape(
            2, batch_len, rows_count, fields_count, local_rows, 1, 1, block_width
        )
        arrived = lax.all_to_all(
            lax.all_to_all(shaped, "rows", split_axis=2, concat_axis=5, tiled=True),
            "fields",
            split_axis=3,
            concat_axis=6,
            tiled=True,
        )
        result = forward_columns(arrived.reshape(2, batch_len, local_rows, groups * block_width))
        return result

    def to_space(stacked):
        batch_len = stacked.shape[1]
        block_width = stacked.shape[3] // groups
        shaped = stacked.reshape(
            2, batch_len, 1, 1, local_rows, rows_count, fields_count, block_width
        )
        arrived = lax.all_to_all(
            lax.all_to_all(shaped, "rows", split_axis=5, concat_axis=2, tiled=True),
            "fields",
            split_axis=6,
            concat_axis=3,
            tiled=True,
        )
        result = inverse_rows(arrived.reshape(2, batch_len, total_rows, block_width))
        return result

    slab_spectra = jnp.stack(
        row_transform(
            (lax.all_to_all(sky_maps, "rows", split_axis=2, concat_axis=1, tiled=True), None), -1.0
        )
    )
    sky_spectra = to_frequency(slab_spectra)
    row_ids = lax.axis_index(("rows", "fields")) * local_rows + jnp.arange(
        local_rows, dtype=jnp.int32
    )
    freq_rows = jnp.where(row_ids < total_rows // 2, row_ids, row_ids - total_rows)[:, None]
    column_ids = jnp.arange(NC, dtype=jnp.int32)
    freq_cols = jnp.where(column_ids < NC // 2, column_ids, column_ids - NC)[None, :]
    scaled_rows = row_ratio * freq_rows
    radius_sq = freq_cols * freq_cols + scaled_rows * scaled_rows

    def band_mask(lower_cut, upper_cut):
        inside = (radius_sq >= lower_cut * lower_cut) & (radius_sq <= upper_cut * upper_cut)
        return inside.astype(jnp.float32)

    mask_temp = band_mask(band_cuts[0], band_cuts[1])
    mask_pol = band_mask(band_cuts[2], band_cuts[3])
    mask_out = band_mask(band_cuts[4], band_cuts[5])
    radius_floor = jnp.maximum(radius_sq, 1).astype(jnp.float32)
    cos_two = (freq_cols * freq_cols - scaled_rows * scaled_rows).astype(jnp.float32) / radius_floor
    sin_two = (2 * freq_cols * scaled_rows).astype(jnp.float32) / radius_floor
    along_x = (2 * freq_cols).astype(jnp.float32) / NC
    along_y = (2 * freq_rows).astype(jnp.float32) / total_rows
    raising = (-along_y + 0.0 * along_x, along_x + 0.0 * along_y)
    lowering = (along_y + 0.0 * along_x, along_x + 0.0 * along_y)
    rotation = (cos_two, sin_two)
    temp_modes = (sky_spectra[0, 0], sky_spectra[1, 0])
    stokes_q = (sky_spectra[0, 1], sky_spectra[1, 1])
    stokes_u = (sky_spectra[0, 2], sky_spectra[1, 2])
    e_modes = (
        -(cos_two * stokes_q[0] + sin_two * stokes_u[0]),
        -(cos_two * stokes_q[1] + sin_two * stokes_u[1]),
    )
    b_modes = (
        sin_two * stokes_q[0] - cos_two * stokes_u[0],
        sin_two * stokes_q[1] - cos_two * stokes_u[1],
    )
    temp_weight = mask_temp * filters[0]
    e_weight = mask_pol * filters[1]
    b_weight = mask_pol * filters[2]
    temp_bar = (temp_weight * temp_modes[0], temp_weight * temp_modes[1])
    e_bar = (e_weight * e_modes[0], e_weight * e_modes[1])
    b_bar = (b_weight * b_modes[0], b_weight * b_modes[1])
    grad_temp = complex_mul(raising, (wiener[0] * temp_bar[0], wiener[0] * temp_bar[1]))
    pol_sum = complex_mul((e_bar[0] - b_bar[1], e_bar[1] + b_bar[0]), rotation)
    pol_bar = (-pol_sum[0], -pol_sum[1])
    pol_rot = complex_mul((wiener[1] * e_bar[0], wiener[1] * e_bar[1]), rotation)
    pol_wiener = (-pol_rot[0], -pol_rot[1])
    spin_three = complex_mul(raising, pol_wiener)
    spin_one = complex_mul(lowering, pol_wiener)
    leg_spectra = jnp.stack(
        [
            jnp.stack([temp_bar[0], grad_temp[0], pol_bar[0], spin_three[0], spin_one[0]]),
            jnp.stack([temp_bar[1], grad_temp[1], pol_bar[1], spin_three[1], spin_one[1]]),
        ]
    )
    leg_maps = to_space(inverse_columns(leg_spectra))
    temp_leg = (leg_maps[0, 0], leg_maps[1, 0])
    grad_leg = (leg_maps[0, 1], leg_maps[1, 1])
    pol_leg = (leg_maps[0, 2], leg_maps[1, 2])
    three_leg = (leg_maps[0, 3], leg_maps[1, 3])
    one_leg = (leg_maps[0, 4], leg_maps[1, 4])
    temp_term = complex_mul(temp_leg, grad_leg)
    raise_term = conj_mul(pol_leg, three_leg)
    lower_term = conj_mul(one_leg, pol_leg)
    current = (
        temp_term[0] + 0.5 * (raise_term[0] + lower_term[0]),
        temp_term[1] + 0.5 * (raise_term[1] + lower_term[1]),
    )
    current_rows = jnp.stack(row_transform((current[0][None], current[1][None]), -1.0))
    current_modes = to_frequency(current_rows)
    out_weight = mask_out * response
    estimate_modes = complex_mul(
        lowering, (out_weight * current_modes[0, 0], out_weight * current_modes[1, 0])
    )
    estimate_stack = jnp.stack([estimate_modes[0][None], estimate_modes[1][None]])
    estimate_maps = to_space(inverse_columns(estimate_stack))
    slab_result = estimate_maps[:, 0]
    return lax.all_to_all(slab_result, "rows", split_axis=1, concat_axis=2, tiled=True)


SIDE = 128
TILE = (8, 128)
LEG_GROUPS = ((0, 2), (2, 2), (4, 1))
WEIGHT_GROUPS = ((0, 3), (1, 4), (2,), (5,))
MESH = pl.DeviceIdType.MESH


def add_pair(a, b):
    imag = a[1] if b[1] is None else b[1] if a[1] is None else a[1] + b[1]
    return (a[0] + b[0], imag)


def sub_pair(a, b):
    imag = a[1] if b[1] is None else -b[1] if a[1] is None else a[1] - b[1]
    return (a[0] - b[0], imag)


def turn_pair(value, step, length, direction):
    real, imag = value
    if step == 0:
        return value
    if 4 * step == length:
        if imag is None:
            return (jnp.zeros_like(real), real if direction > 0 else -real)
        return (-imag, real) if direction > 0 else (imag, -real)
    angle = 2.0 * math.pi * step / length
    c, s = math.cos(angle), direction * math.sin(angle)
    if imag is None:
        return (real * c, real * s)
    if 8 * step == length:
        if direction > 0:
            return ((real - imag) * c, (real + imag) * c)
        return ((real + imag) * c, (imag - real) * c)
    if 8 * step == 3 * length:
        if direction > 0:
            return ((real + imag) * c, (imag - real) * c)
        return ((real - imag) * c, (real + imag) * c)
    return (real * c - imag * s, real * s + imag * c)


def short_transform(values, direction):
    length = len(values)
    if length == 1:
        return values
    even = short_transform(values[0::2], direction)
    odd = short_transform(values[1::2], direction)
    low, high = [], []
    for step in range(length // 2):
        turned = turn_pair(odd[step], step, length, direction)
        low.append(add_pair(even[step], turned))
        high.append(sub_pair(even[step], turned))
    return low + high


def split_number(x):
    top = x.astype(jnp.bfloat16)
    return top, (x - top.astype(jnp.float32)).astype(jnp.bfloat16)


def dot32(a, b):
    return jnp.dot(a, b, preferred_element_type=jnp.float32)


def matrix_left(table_ref, which, x):
    top, rest = split_number(x)
    m_top, m_rest = table_ref[which, 0], table_ref[which, 1]
    return dot32(m_top, top) + (dot32(m_top, rest) + dot32(m_rest, top))


def matrix_right(table_ref, which, x):
    top, rest = split_number(x)
    m_top, m_rest = table_ref[which, 0], table_ref[which, 1]
    return dot32(top, m_top) + (dot32(top, m_rest) + dot32(rest, m_top))


BITS = (0, 1)
OFFSETS = [
    (c, a1, e, a0) for a0 in BITS for c, a1, e in
    ((1, 1, 1), (1, 0, 0), (0, 1, 0), (0, 0, 1), (1, 1, 0), (0, 1, 1), (1, 0, 1), (0, 0, 0))
]
PEERS = [offset for offset in OFFSETS if any(offset)]
WEIGHT_ORDER = (0, 3, 1, 4, 2, 5)


def lens_kernel(
    cuts_ref, sky_hbm, filters_hbm, wiener_hbm, response_hbm, table_hbm, twiddle_hbm, out_ref,
    table_ref, twiddle_ref, sky_ref, raw, weight_ref, slab_out, slab_in, relay_buf, relay_weights, spec_out, spec_in, weights, modes, legs_out, legs_in,
    maps, current, cur_out, cur_in, est_out, est_in, fin_out, fin_in,
    slab_sem, relay_sem, spec_sem, weight_sem, hand_sem, legs_sem, cur_sem, est_sem, fin_sem, send_sem, load_sem,
):
    rows_count, fields_count, local_rows = 4, 4, 2
    groups = rows_count * fields_count
    total_rows = groups * local_rows
    in_rows = total_rows // rows_count
    row_ratio = NC // total_rows
    my_x, my_r, my_z = (lax.axis_index(name) for name in ("sims", "rows", "fields"))
    my_y, my_c, my_h, my_l = my_r // 2, my_r % 2, my_z // 2, my_z % 2
    x_at, y_at, c_at, h_at, l_at = ((bit, 1 - bit) for bit in (my_x, my_y, my_c, my_h, my_l))
    me = my_r * fields_count + 2 * my_x + my_l
    my_block = (2 * my_x + my_l) * rows_count + my_r
    stays = my_x == my_h

    outer = my_l == my_h
    inner = my_l != my_h
    home_row = in_rows * my_r + 4 * my_h + 2 * my_l + my_x

    def signed(row):
        return jnp.where(row < total_rows // 2, row, row - total_rows)

    def row_of(offset):
        return 2 * y_at[offset[1]] + c_at[offset[3]]

    def peer_of(offset):
        return row_of(offset) * fields_count + 2 * x_at[offset[0]] + l_at[offset[2]]

    def peer_block(offset):
        return (2 * x_at[offset[0]] + l_at[offset[2]]) * rows_count + row_of(offset)

    def remote(src, dst, sems, x, r, z):
        return pltpu.make_async_remote_copy(
            src_ref=src, dst_ref=dst, send_sem=sems[0], recv_sem=sems[1],
            device_id={"sims": x, "rows": r, "fields": z}, device_id_type=MESH,
        )

    def send(offset, src, dst, sems):
        return remote(src, dst, sems, x_at[offset[0]], row_of(offset), 2 * my_h + l_at[offset[2]])

    def send_home(offset, src, dst, sems):
        return remote(src, dst, sems, my_h, row_of(offset), 2 * x_at[offset[0]] + l_at[offset[2]])

    def each_peer(body):
        for offset in PEERS:
            body(offset)

    def wait_all(ref, sem):
        pltpu.make_async_copy(ref, ref, sem).wait()

    for src, dst, n in (
        (sky_hbm, sky_ref, 0),
        (filters_hbm, raw.at[0:3], 1),
        (wiener_hbm, raw.at[3:5], 1),
        (response_hbm, raw.at[5], 1),
        (table_hbm, table_ref, 2),
        (twiddle_hbm, twiddle_ref, 3),
    ):
        pltpu.make_async_copy(src, dst, load_sem.at[n]).start()

    (
        slab_left, relay_left, forward_left, spec_left, weight_left, legs_left, cur_left, est_left, fin_left,
        extra_left, pass_left,
    ) = (send_sem.at[n] for n in range(11))

    barrier = pltpu.get_barrier_semaphore()
    for h in BITS:
        for c, a1, e, a0 in OFFSETS:
            if h or c or a1 or e or a0:
                pl.semaphore_signal(
                    barrier, inc=1, device_id_type=MESH,
                    device_id={"sims": x_at[c], "rows": 2 * y_at[a1] + c_at[a0], "fields": 2 * h_at[h] + l_at[e]},
                )
    wait_all(sky_ref, load_sem.at[0])
    tiles = sky_ref.shape[2] // SIDE
    for field in range(3):
        for t in range(tiles):
            slab_out[t // 8, field, :, t % 8, :] = sky_ref[field, :, t * SIDE:(t + 1) * SIDE]
    pl.semaphore_wait(barrier, 2 * groups - 1)

    ROW_OFFSETS = [(0, a1, 0, a0) for a1 in BITS for a0 in BITS]

    def slab_copy(field, offset):
        r = row_of(offset)
        return send_home(
            offset, slab_out.at[r, field], slab_in.at[my_r, field],
            (slab_left, slab_sem.at[field]),
        )

    def own_slab(field):
        return pltpu.make_async_copy(slab_out.at[my_r, field], slab_in.at[my_r, field], slab_sem.at[field])

    def relay_copy(field):
        return remote(
            slab_out.at[pl.ds(2 * y_at[1], 2), field], relay_buf.at[field],
            (relay_left, relay_sem.at[field]), x_at[1], my_r, my_z,
        )

    def forward_copy(field, core):
        a0 = core
        return remote(
            relay_buf.at[field, c_at[a0]], slab_in.at[my_r, field],
            (forward_left, slab_sem.at[field]),
            my_x, 2 * y_at[1] + c_at[a0], 2 * h_at[1] + my_l,
        )

    @pl.when(stays)
    def _():
        for field in range(3):
            own_slab(field).start()
            for offset in ROW_OFFSETS[1:]:
                slab_copy(field, offset).start()

    def slab_start(field):
        relay_copy(field).start()
        for offset in ROW_OFFSETS[:2]:
            slab_copy(field, offset).start()

    @pl.when(jnp.logical_not(stays))
    def _():
        slab_start(0)

    low_index = lax.broadcasted_iota(jnp.int32, (SIDE, SIDE), 0)
    high_index = lax.broadcasted_iota(jnp.int32, (SIDE, SIDE), 1)
    column_ids = low_index + SIDE * high_index
    freq_cols = jnp.where(column_ids < NC // 2, column_ids, column_ids - NC)

    def row_frequency(row):
        return signed(in_rows * my_r + 4 * my_l + 2 * (my_h + row - 2 * my_h * row) + my_x)

    wait_all(raw, load_sem.at[1])

    def spread(n, carry):
        for j in range(8):
            start = pl.multiple_of((n * 8 + j) * SIDE, SIDE)
            weight_ref[:, :, n * 8 + j, :] = raw[:, :, pl.ds(start, SIDE)]
        return carry

    lax.fori_loop(0, SIDE // 8, spread, 0)
    scaled_home = row_ratio * signed(home_row)
    radius_home = freq_cols * freq_cols + scaled_home * scaled_home

    def mask(n):
        low, high = cuts_ref[2 * n], cuts_ref[2 * n + 1]
        inside = (radius_home >= low * low) & (radius_home <= high * high)
        return inside.astype(jnp.float32)

    home_slot = jnp.where(inner, 2, 0)

    def group_of(n):
        return [n in members for members in WEIGHT_GROUPS].index(True)

    def across(n, source, slot, left):
        return remote(
            source, weights.at[n, slot], (left, weight_sem.at[slot, group_of(n)]),
            my_x, my_r, 2 * h_at[1] + my_h,
        )

    def own_weight(n):
        return across(n, weights.at[n, home_slot], 0, weight_left)

    def near_copy(n):
        return remote(
            weights.at[n, home_slot], weights.at[n, 1], (extra_left, weight_sem.at[1, group_of(n)]),
            my_x, my_r, 2 * my_h + l_at[1],
        )

    def hand_copy(n):
        return remote(
            weights.at[n, home_slot], relay_weights.at[n], (weight_left, hand_sem.at[n]),
            my_x, my_r, 2 * my_h + l_at[1],
        )

    def weight_pass_on(members):
        @pl.when(inner)
        def _():
            for n in members:
                wait_all(relay_weights.at[n], hand_sem.at[n])
                across(n, relay_weights.at[n], 1, pass_left).start()

    pol = mask(1)
    weights[0, home_slot] = mask(0) * weight_ref[0, my_x].T
    weights[1, home_slot] = pol * weight_ref[1, my_x].T
    weights[2, home_slot] = pol * weight_ref[2, my_x].T
    weights[3, home_slot] = weight_ref[3, my_x].T
    weights[4, home_slot] = weight_ref[4, my_x].T
    weights[5, home_slot] = mask(2) * weight_ref[5, my_x].T
    @pl.when(jnp.logical_and(inner, jnp.logical_not(stays)))
    def _():
        slab_start(1)
        slab_start(2)
        for n in WEIGHT_ORDER[:5]:
            near_copy(n).start()
            own_weight(n).start()

    @pl.when(jnp.logical_and(outer, jnp.logical_not(stays)))
    def _():
        hand_copy(0).start()
        slab_start(1)
        hand_copy(3).start()
        slab_start(2)
        hand_copy(1).start()

    @pl.when(jnp.logical_and(inner, stays))
    def _():
        own_weight(0).start()
        for n in WEIGHT_ORDER[:5]:
            near_copy(n).start()

    @pl.when(jnp.logical_and(outer, stays))
    def _():
        hand_copy(0).start()
        hand_copy(3).start()

    def place(k, half):
        return 1 - half if k // 2 % 2 else half, k // in_rows * fields_count + 2 * (k % 2) + k // 4 % 2

    def spec_copy(field, row, offset):
        return send(
            offset, spec_out.at[field, row, peer_of(offset)], spec_in.at[field, row, :, my_block],
            (spec_left, spec_sem.at[field]),
        )

    def own_spec(field, row):
        return pltpu.make_async_copy(
            spec_out.at[field, row, me], spec_in.at[field, row, :, my_block], spec_sem.at[field]
        )

    def spec_start(field):
        for row in range(local_rows):
            each_peer(lambda offset: spec_copy(field, row, offset).start())
            own_spec(field, row).start()

    def row_step(field):
        @pl.when(stays)
        def _():
            wait_all(relay_buf.at[field], relay_sem.at[field])
            for core in BITS:
                forward_copy(field, core).start()

        if field == 1:
            @pl.when(jnp.logical_and(outer, stays))
            def _():
                hand_copy(1).start()

        if field == 2:
            @pl.when(jnp.logical_and(inner, stays))
            def _():
                for n in WEIGHT_ORDER[1:5]:
                    own_weight(n).start()

        wait_all(slab_in.at[:, field], slab_sem.at[field])
        values = [
            (slab_in[y // in_rows, field, y % in_rows], None) for y in range(total_rows)
        ]
        for k, (real, imag) in enumerate(short_transform(values, -1)):
            local, device = place(k, my_h)
            spec_out[field, local, device, 0] = real
            spec_out[field, local, device, 1] = jnp.zeros_like(real) if imag is None else imag
        spec_start(field)

    for field in range(3):
        row_step(field)

    @pl.when(outer)
    def _():
        hand_copy(4).start()
        hand_copy(2).start()

    weight_pass_on((0, 3, 1))

    cos_f, sin_f, cos_b, sin_b = 0, 1, 2, 3

    def side_by_side(pieces, axis):
        return pieces[0] if len(pieces) == 1 else jnp.concatenate(pieces, axis=axis)

    def long_forward(pieces):
        y = matrix_left(table_ref, 0, side_by_side(pieces, 1))
        c, s = twiddle_ref[cos_f], twiddle_ref[sin_f]
        turned = []
        for n in range(len(pieces)):
            yr, yi = y[:SIDE, n * SIDE:(n + 1) * SIDE], y[SIDE:, n * SIDE:(n + 1) * SIDE]
            turned.append(jnp.concatenate([yr * c - yi * s, yr * s + yi * c], axis=1))
        z = matrix_right(table_ref, 1, side_by_side(turned, 0))
        return [
            (z[n * SIDE:(n + 1) * SIDE, :SIDE], z[n * SIDE:(n + 1) * SIDE, SIDE:])
            for n in range(len(pieces))
        ]

    def long_inverse(pairs):
        stacks = [jnp.concatenate([pair[0], pair[1]], axis=1) for pair in pairs]
        u = matrix_right(table_ref, 0, side_by_side(stacks, 0))
        c, s = twiddle_ref[cos_b], twiddle_ref[sin_b]
        turned = []
        for n in range(len(pairs)):
            ur, ui = u[n * SIDE:(n + 1) * SIDE, :SIDE], u[n * SIDE:(n + 1) * SIDE, SIDE:]
            turned.append(jnp.concatenate([ur * c - ui * s, ur * s + ui * c], axis=0))
        x = matrix_left(table_ref, 1, side_by_side(turned, 1))
        return [
            x[:, n * SIDE:(n + 1) * SIDE].reshape((2, groups) + TILE)
            for n in range(len(pairs))
        ]

    def legs_copy(row, g, offset):
        first, count = LEG_GROUPS[g]
        return send(
            offset, legs_out.at[row, first:first + count, :, peer_block(offset)],
            legs_in.at[row, me, first:first + count],
            (legs_left, legs_sem.at[g]),
        )

    def own_legs(row, g):
        first, count = LEG_GROUPS[g]
        return pltpu.make_async_copy(
            legs_out.at[row, first:first + count, :, my_block],
            legs_in.at[row, me, first:first + count],
            legs_sem.at[g],
        )

    def wait_weights(group, row):
        members = WEIGHT_GROUPS[group]

        @pl.when(jnp.logical_or(row == 1, inner))
        def _():
            wait_all(weights.at[0:len(members), row], weight_sem.at[row, group])

    def slopes(row):
        along_x = (2 * freq_cols).astype(jnp.float32) / NC
        along_y = (2 * row_frequency(row)).astype(jnp.float32) / total_rows
        return along_x, along_y

    def both_rows(field):
        wait_all(spec_in.at[field], spec_sem.at[field])
        pairs = long_forward([spec_in[field, row].reshape(2 * SIDE, SIDE) for row in range(local_rows)])
        for row, pair in enumerate(pairs):
            modes[field, row, 0], modes[field, row, 1] = pair

    def leg_step(n, row):
        scaled = row_ratio * row_frequency(row)
        radius_sq = freq_cols * freq_cols + scaled * scaled
        floor = jnp.maximum(radius_sq, 1).astype(jnp.float32)
        cos2 = (freq_cols * freq_cols - scaled * scaled).astype(jnp.float32) / floor
        sin2 = (2 * freq_cols * scaled).astype(jnp.float32) / floor
        along_x, along_y = slopes(row)
        raising, lowering = (-along_y, along_x), (along_y, along_x)
        rot = (cos2, sin2)

        def temp_legs():
            t_bar = (weights[0, row] * modes[0, row, 0], weights[0, row] * modes[0, row, 1])
            return t_bar, complex_mul((weights[3, row] * t_bar[0], weights[3, row] * t_bar[1]), raising)

        def e_modes():
            return tuple(
                -weights[1, row] * (cos2 * modes[1, row, n] + sin2 * modes[2, row, n]) for n in range(2)
            )

        def spin_legs():
            e_bar = e_modes()
            w = complex_mul((-weights[4, row] * e_bar[0], -weights[4, row] * e_bar[1]), rot)
            return complex_mul(w, raising), complex_mul(w, lowering)

        def pol_leg():
            e_bar = e_modes()
            b_bar = tuple(
                weights[2, row] * (sin2 * modes[1, row, n] - cos2 * modes[2, row, n]) for n in range(2)
            )
            return (complex_mul((b_bar[1] - e_bar[0], -(e_bar[1] + b_bar[0])), rot),)

        wait_weights(n, row)
        for k, leg_map in enumerate(long_inverse((temp_legs, spin_legs, pol_leg)[n]())):
            legs_out[row, LEG_GROUPS[n][0] + k] = leg_map
        each_peer(lambda offset: legs_copy(row, n, offset).start())
        own_legs(row, n).start()

    wait_all(table_ref, load_sem.at[2])
    wait_all(twiddle_ref, load_sem.at[3])
    both_rows(0)

    @pl.when(outer)
    def _():
        leg_step(0, 0)
        leg_step(0, 1)

    both_rows(1)
    both_rows(2)
    weight_pass_on((4, 2))

    @pl.when(inner)
    def _():
        leg_step(0, 0)

    def later_steps(row, carry):
        @pl.when(jnp.logical_and(inner, row == 1))
        def _():
            leg_step(0, 1)

        leg_step(1, row)
        leg_step(2, row)
        return carry

    lax.fori_loop(0, local_rows, later_steps, 0)

    @pl.when(inner)
    def _():
        near_copy(5).start()
        own_weight(5).start()

    @pl.when(outer)
    def _():
        hand_copy(5).start()

    def map_step(n, carry):
        values = [
            (legs_in[place(k, my_h) + (n, 0)], legs_in[place(k, my_h) + (n, 1)])
            for k in range(total_rows)
        ]
        for y, (real, imag) in enumerate(short_transform(values, 1)):
            maps[n, 0, y] = real
            maps[n, 1, y] = imag
        return carry

    for g, (first, count) in enumerate(LEG_GROUPS):
        wait_all(legs_in.at[:, :, first:first + count], legs_sem.at[g])
        lax.fori_loop(first, first + count, map_step, 0)

    def product_step(y, carry):
        a, g, h3, h1, p = [(maps[n, 0, y], maps[n, 1, y]) for n in range(5)]
        ag, ph, hp = complex_mul(a, g), conj_mul(p, h3), conj_mul(h1, p)
        current[0, y] = ag[0] + 0.5 * (ph[0] + hp[0])
        current[1, y] = ag[1] + 0.5 * (ph[1] + hp[1])
        return carry

    lax.fori_loop(0, total_rows, product_step, 0)

    values = [(current[0, y], current[1, y]) for y in range(total_rows)]
    for k, (real, imag) in enumerate(short_transform(values, -1)):
        cur_out[place(k, my_h) + (0,)] = real
        cur_out[place(k, my_h) + (1,)] = imag

    def cur_copy(row, offset):
        return send(
            offset, cur_out.at[row, peer_of(offset)], cur_in.at[row, :, my_block],
            (cur_left, cur_sem.at[row]),
        )

    def own_cur(row):
        return pltpu.make_async_copy(
            cur_out.at[row, me], cur_in.at[row, :, my_block], cur_sem.at[row]
        )

    def cur_start(row, carry):
        each_peer(lambda offset: cur_copy(row, offset).start())
        own_cur(row).start()
        return carry

    lax.fori_loop(0, local_rows, cur_start, 0)
    weight_pass_on((5,))

    HOME_OFFSETS = sorted(PEERS, key=lambda offset: -offset[0])
    ORIGIN = (0, 0, 0, 0)

    def est_copy(row, offset):
        r, z = row_of(offset), 2 * h_at[offset[0]] + l_at[offset[2]]
        return remote(
            est_out.at[row, :, z * rows_count + r], est_in.at[row, me], (est_left, est_sem.at[0]), my_h, r, z
        )

    def own_est(row):
        return pltpu.make_async_copy(
            est_out.at[row, :, my_z * rows_count + my_r], est_in.at[row, me], est_sem.at[0]
        )

    def estimate_step(row, carry):
        wait_all(cur_in.at[row], cur_sem.at[row])
        wait_weights(3, row)

        (modes,) = long_forward([cur_in[row].reshape(2 * SIDE, SIDE)])
        along_x, along_y = slopes(row)
        w = weights[5, row]
        estimate = complex_mul((w * modes[0], w * modes[1]), (along_y, along_x))
        (est_out[row],) = long_inverse([estimate])
        for offset in HOME_OFFSETS:
            est_copy(row, offset).start()

        @pl.when(stays)
        def _():
            own_est(row).start()

        @pl.when(jnp.logical_not(stays))
        def _():
            est_copy(row, ORIGIN).start()

        return carry

    lax.fori_loop(0, local_rows, estimate_step, 0)

    wait_all(est_in, est_sem.at[0])
    values = [
        (est_in[place(k, my_x) + (0,)], est_in[place(k, my_x) + (1,)])
        for k in range(total_rows)
    ]
    for y, (real, imag) in enumerate(short_transform(values, 1)):
        fin_out[y // in_rows, 0, y % in_rows] = real
        fin_out[y // in_rows, 1, y % in_rows] = imag

    def fin_copy(offset):
        r = row_of(offset)
        return remote(
            fin_out.at[r], fin_in.at[my_r], (fin_left, fin_sem.at[0]), my_x, r, my_z
        )

    for offset in ROW_OFFSETS[1:]:
        fin_copy(offset).start()
    own_fin = pltpu.make_async_copy(
        fin_out.at[my_r], fin_in.at[my_r], fin_sem.at[0]
    )
    own_fin.start()

    others = groups - 1

    @pl.when(stays)
    def _():
        wait_all(slab_out.at[0:3], slab_left)
        wait_all(relay_buf, forward_left)
        wait_all(est_out.at[:, :, 0:others], est_left)

    @pl.when(jnp.logical_not(stays))
    def _():
        wait_all(slab_out.at[0:2], slab_left)
        wait_all(relay_buf, relay_left)
        wait_all(est_out, est_left)

    @pl.when(inner)
    def _():
        wait_all(relay_weights, pass_left)
        wait_all(relay_weights, extra_left)

    wait_all(weights.at[:, 0], weight_left)
    wait_all(spec_out.at[:, :, 0:others], spec_left)
    wait_all(legs_out.at[:, :, :, 0:others], legs_left)
    wait_all(cur_out.at[:, 0:others], cur_left)
    wait_all(fin_in, fin_sem.at[0])
    for part in range(2):
        for t in range(tiles):
            out_ref[part, :, t * SIDE:(t + 1) * SIDE] = fin_in[t // 8, part, :, t % 8, :]

    wait_all(fin_out.at[0:3], fin_left)


def long_tables(total_rows):
    index = np.arange(SIDE)
    angle = 2.0 * np.pi * (index[:, None] * index[None, :] % SIDE) / SIDE
    c, s = np.cos(angle), np.sin(angle)
    forward = np.block([[c, s], [-s, c]]).astype(np.float32)
    tables = np.stack([forward, forward.T])
    top = tables.astype(jnp.bfloat16)
    rest = (tables - top.astype(np.float32)).astype(jnp.bfloat16)
    turn = 2.0 * np.pi * (index[:, None] * index[None, :]) / NC
    scale = 1.0 / (NC * total_rows)
    twiddle = np.stack(
        [np.cos(turn), -np.sin(turn), scale * np.cos(turn), scale * np.sin(turn)]
    ).astype(np.float32)
    return np.stack([top, rest], axis=1), twiddle


def fused_body(rows_count, fields_count, sky_maps, band_cuts, filters, wiener, response):
    groups = rows_count * fields_count
    local_rows = response.shape[0]
    total_rows = local_rows * groups
    in_rows = total_rows // rows_count
    table, twiddle = long_tables(total_rows)
    vmem = pl.BlockSpec(memory_space=pltpu.VMEM)
    f32 = jnp.float32
    dma = pltpu.SemaphoreType.DMA
    slab = pltpu.VMEM((rows_count, 3, in_rows) + TILE, f32)
    chunk = pltpu.VMEM((local_rows, groups, 2) + TILE, f32)
    lines = pltpu.VMEM((local_rows, 2, groups) + TILE, f32)
    final = pltpu.VMEM((rows_count, 2, in_rows) + TILE, f32)
    return pl.pallas_call(
        lens_kernel,
        out_shape=jax.ShapeDtypeStruct((2,) + sky_maps.shape[1:], f32),
        in_specs=[pl.BlockSpec(memory_space=pltpu.SMEM)] + [pl.BlockSpec(memory_space=pl.ANY)] * 6,
        out_specs=vmem,
        scratch_shapes=[
            pltpu.VMEM(table.shape, table.dtype), pltpu.VMEM(twiddle.shape, f32),
            pltpu.VMEM(sky_maps.shape, f32),
            pltpu.VMEM((6, local_rows, NC), f32),
            pltpu.VMEM((6, local_rows, SIDE, SIDE), f32),
            slab, slab,
            pltpu.VMEM((3, 2, in_rows) + TILE, f32),
            pltpu.VMEM((6, SIDE, SIDE), f32),
            pltpu.VMEM((3, local_rows, groups, 2) + TILE, f32),
            pltpu.VMEM((3, local_rows, 2, groups) + TILE, f32),
            pltpu.VMEM((6, 3, SIDE, SIDE), f32),
            pltpu.VMEM((3, local_rows, 2, SIDE, SIDE), f32),
            pltpu.VMEM((local_rows, 5, 2, groups) + TILE, f32),
            pltpu.VMEM((local_rows, groups, 5, 2) + TILE, f32),
            pltpu.VMEM((5, 2, total_rows) + TILE, f32),
            pltpu.VMEM((2, total_rows) + TILE, f32),
            chunk, lines, lines, chunk, final, final,
            dma((3,)), dma((3,)), dma((3,)), dma((local_rows, len(WEIGHT_GROUPS))), dma((6,)), dma((len(LEG_GROUPS),)),
            dma((local_rows,)), dma((1,)), dma((1,)), dma((11,)), dma((4,)),
        ],
        compiler_params=pltpu.CompilerParams(
            collective_id=0, has_side_effects=True, vmem_limit_bytes=60 * 1024 * 1024
        ),
        name="lens",
    )(band_cuts, sky_maps, filters, wiener, response, jnp.asarray(table), jnp.asarray(twiddle))


def solution(mesh):
    placed = (
        P("sims", "rows", "fields"),
        P(),
        P(None, ("rows", "fields"), None),
        P(None, ("rows", "fields"), None),
        P(("rows", "fields"), None),
    )
    rows_count, fields_count = mesh.shape["rows"], mesh.shape["fields"]
    groups = rows_count * fields_count

    def choose(sky_maps, *rest):
        fits = (
            NC == SIDE * SIDE
            and (mesh.shape["sims"], rows_count, fields_count) == (2, 4, 4)
            and NC // groups == TILE[0] * TILE[1]
            and sky_maps.shape[0] == 3
            and sky_maps.shape[1] * rows_count == 32
        )
        if fits:
            return fused_body(rows_count, fields_count, sky_maps, *rest)
        return body(sky_maps, *rest)

    return jax.shard_map(
        choose, mesh=mesh, in_specs=placed, out_specs=P("sims", "rows", "fields"), check_vma=False
    )
```

```python
import functools
import math

import jax
import jax.numpy as jnp
import numpy as np
from jax import lax
from jax.experimental import pallas as pl
from jax.experimental.pallas import tpu as pltpu
from jax.sharding import PartitionSpec as P

NC = 16384


exact_mode = lax.Precision.HIGHEST


def split_factor(length):
    best_first = 1
    for divisor in range(1, math.isqrt(length) + 1):
        if length % divisor == 0:
            best_first = divisor
    return (best_first, length // best_first)


def phase_table(left_index, right_index, period, direction):
    product = left_index[:, None] * right_index[None, :] % period
    angles = direction * 2.0 * math.pi / period * product.astype(jnp.float32)
    return (jnp.cos(angles), jnp.sin(angles))


def complex_einsum(formula, data_pair, table_pair):
    data_real, data_imag = data_pair
    table_real, table_imag = table_pair
    real_out = jnp.einsum(formula, data_real, table_real, precision=exact_mode)
    imag_out = jnp.einsum(formula, data_real, table_imag, precision=exact_mode)
    if data_imag is not None:
        real_out = real_out - jnp.einsum(formula, data_imag, table_imag, precision=exact_mode)
        imag_out = imag_out + jnp.einsum(formula, data_imag, table_real, precision=exact_mode)
    return (real_out, imag_out)


def complex_mul(left_pair, right_pair):
    return (
        left_pair[0] * right_pair[0] - left_pair[1] * right_pair[1],
        left_pair[0] * right_pair[1] + left_pair[1] * right_pair[0],
    )


def conj_mul(left_pair, right_pair):
    return (
        left_pair[0] * right_pair[0] + left_pair[1] * right_pair[1],
        left_pair[0] * right_pair[1] - left_pair[1] * right_pair[0],
    )


def row_transform(data_pair, direction):
    batch_len, length, block_width = data_pair[0].shape
    outer_len, inner_len = split_factor(length)
    outer_ids = jnp.arange(outer_len, dtype=jnp.int32)
    inner_ids = jnp.arange(inner_len, dtype=jnp.int32)
    real_in = data_pair[0].reshape(batch_len, outer_len, inner_len, block_width)
    imag_in = None
    if data_pair[1] is not None:
        imag_in = data_pair[1].reshape(batch_len, outer_len, inner_len, block_width)
    middle = complex_einsum(
        "bjmc,jk->bkmc", (real_in, imag_in), phase_table(outer_ids, outer_ids, outer_len, direction)
    )
    twiddle = phase_table(outer_ids, inner_ids, length, direction)
    middle = complex_mul(middle, (twiddle[0][None, :, :, None], twiddle[1][None, :, :, None]))
    result = complex_einsum(
        "bkmc,mq->bqkc", middle, phase_table(inner_ids, inner_ids, inner_len, direction)
    )
    norm_factor = 1.0 if direction < 0 else 1.0 / length
    return (
        result[0].reshape(batch_len, length, block_width) * norm_factor,
        result[1].reshape(batch_len, length, block_width) * norm_factor,
    )


def block_order(groups, fields_count):
    positions = jnp.arange(groups, dtype=jnp.int32)
    blocks = positions % fields_count * (groups // fields_count) + positions // fields_count
    return (positions, blocks)


def column_forward(data_pair, groups, fields_count):
    batch_len, local_rows, total_len = data_pair[0].shape
    block_width = total_len // groups
    positions, blocks = block_order(groups, fields_count)
    column_ids = jnp.arange(block_width, dtype=jnp.int32)
    shaped = (
        data_pair[0].reshape(batch_len, local_rows, groups, block_width),
        data_pair[1].reshape(batch_len, local_rows, groups, block_width),
    )
    middle = complex_einsum("brpc,pk->brkc", shaped, phase_table(blocks, positions, groups, -1.0))
    twiddle = phase_table(positions, column_ids, total_len, -1.0)
    middle = complex_mul(middle, (twiddle[0][None, None], twiddle[1][None, None]))
    result = complex_einsum(
        "brkc,cq->brqk", middle, phase_table(column_ids, column_ids, block_width, -1.0)
    )
    return (
        result[0].reshape(batch_len, local_rows, total_len),
        result[1].reshape(batch_len, local_rows, total_len),
    )


def column_inverse(data_pair, groups, fields_count):
    batch_len, local_rows, total_len = data_pair[0].shape
    block_width = total_len // groups
    positions, blocks = block_order(groups, fields_count)
    column_ids = jnp.arange(block_width, dtype=jnp.int32)
    shaped = (
        data_pair[0].reshape(batch_len, local_rows, block_width, groups),
        data_pair[1].reshape(batch_len, local_rows, block_width, groups),
    )
    middle = complex_einsum(
        "brqk,qc->brkc", shaped, phase_table(column_ids, column_ids, block_width, 1.0)
    )
    twiddle = phase_table(positions, column_ids, total_len, 1.0)
    middle = complex_mul(middle, (twiddle[0][None, None], twiddle[1][None, None]))
    result = complex_einsum("brkc,kp->brpc", middle, phase_table(positions, blocks, groups, 1.0))
    norm_factor = 1.0 / total_len
    return (
        result[0].reshape(batch_len, local_rows, total_len) * norm_factor,
        result[1].reshape(batch_len, local_rows, total_len) * norm_factor,
    )


def body(sky_maps, band_cuts, filters, wiener, response):
    rows_count = lax.axis_size("rows")
    fields_count = lax.axis_size("fields")
    groups = rows_count * fields_count
    local_rows = filters.shape[1]
    total_rows = local_rows * groups
    row_ratio = NC // total_rows

    def forward_columns(stacked):
        return jnp.stack(column_forward((stacked[0], stacked[1]), groups, fields_count))

    def inverse_rows(stacked):
        return jnp.stack(row_transform((stacked[0], stacked[1]), 1.0))

    def inverse_columns(stacked):
        return jnp.stack(column_inverse((stacked[0], stacked[1]), groups, fields_count))

    def to_frequency(stacked):
        batch_len = stacked.shape[1]
        block_width = stacked.shape[3]
        shaped = stacked.reshape(
            2, batch_len, rows_count, fields_count, local_rows, 1, 1, block_width
        )
        arrived = lax.all_to_all(
            lax.all_to_all(shaped, "rows", split_axis=2, concat_axis=5, tiled=True),
            "fields",
            split_axis=3,
            concat_axis=6,
            tiled=True,
        )
        result = forward_columns(arrived.reshape(2, batch_len, local_rows, groups * block_width))
        return result

    def to_space(stacked):
        batch_len = stacked.shape[1]
        block_width = stacked.shape[3] // groups
        shaped = stacked.reshape(
            2, batch_len, 1, 1, local_rows, rows_count, fields_count, block_width
        )
        arrived = lax.all_to_all(
            lax.all_to_all(shaped, "rows", split_axis=5, concat_axis=2, tiled=True),
            "fields",
            split_axis=6,
            concat_axis=3,
            tiled=True,
        )
        result = inverse_rows(arrived.reshape(2, batch_len, total_rows, block_width))
        return result

    slab_spectra = jnp.stack(
        row_transform(
            (lax.all_to_all(sky_maps, "rows", split_axis=2, concat_axis=1, tiled=True), None), -1.0
        )
    )
    sky_spectra = to_frequency(slab_spectra)
    row_ids = lax.axis_index(("rows", "fields")) * local_rows + jnp.arange(
        local_rows, dtype=jnp.int32
    )
    freq_rows = jnp.where(row_ids < total_rows // 2, row_ids, row_ids - total_rows)[:, None]
    column_ids = jnp.arange(NC, dtype=jnp.int32)
    freq_cols = jnp.where(column_ids < NC // 2, column_ids, column_ids - NC)[None, :]
    scaled_rows = row_ratio * freq_rows
    radius_sq = freq_cols * freq_cols + scaled_rows * scaled_rows

    def band_mask(lower_cut, upper_cut):
        inside = (radius_sq >= lower_cut * lower_cut) & (radius_sq <= upper_cut * upper_cut)
        return inside.astype(jnp.float32)

    mask_temp = band_mask(band_cuts[0], band_cuts[1])
    mask_pol = band_mask(band_cuts[2], band_cuts[3])
    mask_out = band_mask(band_cuts[4], band_cuts[5])
    radius_floor = jnp.maximum(radius_sq, 1).astype(jnp.float32)
    cos_two = (freq_cols * freq_cols - scaled_rows * scaled_rows).astype(jnp.float32) / radius_floor
    sin_two = (2 * freq_cols * scaled_rows).astype(jnp.float32) / radius_floor
    along_x = (2 * freq_cols).astype(jnp.float32) / NC
    along_y = (2 * freq_rows).astype(jnp.float32) / total_rows
    raising = (-along_y + 0.0 * along_x, along_x + 0.0 * along_y)
    lowering = (along_y + 0.0 * along_x, along_x + 0.0 * along_y)
    rotation = (cos_two, sin_two)
    temp_modes = (sky_spectra[0, 0], sky_spectra[1, 0])
    stokes_q = (sky_spectra[0, 1], sky_spectra[1, 1])
    stokes_u = (sky_spectra[0, 2], sky_spectra[1, 2])
    e_modes = (
        -(cos_two * stokes_q[0] + sin_two * stokes_u[0]),
        -(cos_two * stokes_q[1] + sin_two * stokes_u[1]),
    )
    b_modes = (
        sin_two * stokes_q[0] - cos_two * stokes_u[0],
        sin_two * stokes_q[1] - cos_two * stokes_u[1],
    )
    temp_weight = mask_temp * filters[0]
    e_weight = mask_pol * filters[1]
    b_weight = mask_pol * filters[2]
    temp_bar = (temp_weight * temp_modes[0], temp_weight * temp_modes[1])
    e_bar = (e_weight * e_modes[0], e_weight * e_modes[1])
    b_bar = (b_weight * b_modes[0], b_weight * b_modes[1])
    grad_temp = complex_mul(raising, (wiener[0] * temp_bar[0], wiener[0] * temp_bar[1]))
    pol_sum = complex_mul((e_bar[0] - b_bar[1], e_bar[1] + b_bar[0]), rotation)
    pol_bar = (-pol_sum[0], -pol_sum[1])
    pol_rot = complex_mul((wiener[1] * e_bar[0], wiener[1] * e_bar[1]), rotation)
    pol_wiener = (-pol_rot[0], -pol_rot[1])
    spin_three = complex_mul(raising, pol_wiener)
    spin_one = complex_mul(lowering, pol_wiener)
    leg_spectra = jnp.stack(
        [
            jnp.stack([temp_bar[0], grad_temp[0], pol_bar[0], spin_three[0], spin_one[0]]),
            jnp.stack([temp_bar[1], grad_temp[1], pol_bar[1], spin_three[1], spin_one[1]]),
        ]
    )
    leg_maps = to_space(inverse_columns(leg_spectra))
    temp_leg = (leg_maps[0, 0], leg_maps[1, 0])
    grad_leg = (leg_maps[0, 1], leg_maps[1, 1])
    pol_leg = (leg_maps[0, 2], leg_maps[1, 2])
    three_leg = (leg_maps[0, 3], leg_maps[1, 3])
    one_leg = (leg_maps[0, 4], leg_maps[1, 4])
    temp_term = complex_mul(temp_leg, grad_leg)
    raise_term = conj_mul(pol_leg, three_leg)
    lower_term = conj_mul(one_leg, pol_leg)
    current = (
        temp_term[0] + 0.5 * (raise_term[0] + lower_term[0]),
        temp_term[1] + 0.5 * (raise_term[1] + lower_term[1]),
    )
    current_rows = jnp.stack(row_transform((current[0][None], current[1][None]), -1.0))
    current_modes = to_frequency(current_rows)
    out_weight = mask_out * response
    estimate_modes = complex_mul(
        lowering, (out_weight * current_modes[0, 0], out_weight * current_modes[1, 0])
    )
    estimate_stack = jnp.stack([estimate_modes[0][None], estimate_modes[1][None]])
    estimate_maps = to_space(inverse_columns(estimate_stack))
    slab_result = estimate_maps[:, 0]
    return lax.all_to_all(slab_result, "rows", split_axis=1, concat_axis=2, tiled=True)


SIDE = 128
TILE = (8, 128)
LEG_GROUPS = ((0, 2), (2, 2), (4, 1))
WEIGHT_GROUPS = ((0, 3), (1, 4), (2,), (5,))
MESH = pl.DeviceIdType.MESH


def add_pair(a, b):
    imag = a[1] if b[1] is None else b[1] if a[1] is None else a[1] + b[1]
    return (a[0] + b[0], imag)


def sub_pair(a, b):
    imag = a[1] if b[1] is None else -b[1] if a[1] is None else a[1] - b[1]
    return (a[0] - b[0], imag)


def turn_pair(value, step, length, direction):
    real, imag = value
    if step == 0:
        return value
    if 4 * step == length:
        if imag is None:
            return (jnp.zeros_like(real), real if direction > 0 else -real)
        return (-imag, real) if direction > 0 else (imag, -real)
    angle = 2.0 * math.pi * step / length
    c, s = math.cos(angle), direction * math.sin(angle)
    if imag is None:
        return (real * c, real * s)
    if 8 * step == length:
        if direction > 0:
            return ((real - imag) * c, (real + imag) * c)
        return ((real + imag) * c, (imag - real) * c)
    if 8 * step == 3 * length:
        if direction > 0:
            return ((real + imag) * c, (imag - real) * c)
        return ((real - imag) * c, (real + imag) * c)
    return (real * c - imag * s, real * s + imag * c)


def short_transform(values, direction):
    length = len(values)
    if length == 1:
        return values
    even = short_transform(values[0::2], direction)
    odd = short_transform(values[1::2], direction)
    low, high = [], []
    for step in range(length // 2):
        turned = turn_pair(odd[step], step, length, direction)
        low.append(add_pair(even[step], turned))
        high.append(sub_pair(even[step], turned))
    return low + high


def split_number(x):
    top = x.astype(jnp.bfloat16)
    return top, (x - top.astype(jnp.float32)).astype(jnp.bfloat16)


def dot32(a, b):
    return jnp.dot(a, b, preferred_element_type=jnp.float32)


def matrix_left(table_ref, which, x):
    top, rest = split_number(x)
    m_top, m_rest = table_ref[which, 0], table_ref[which, 1]
    return dot32(m_top, top) + (dot32(m_top, rest) + dot32(m_rest, top))


def matrix_right(table_ref, which, x):
    top, rest = split_number(x)
    m_top, m_rest = table_ref[which, 0], table_ref[which, 1]
    return dot32(top, m_top) + (dot32(top, m_rest) + dot32(rest, m_top))


BITS = (0, 1)
OFFSETS = [
    (c, a1, e, a0) for a0 in BITS for c, a1, e in
    ((1, 1, 1), (1, 0, 0), (0, 1, 0), (0, 0, 1), (1, 1, 0), (0, 1, 1), (1, 0, 1), (0, 0, 0))
]
PEERS = [offset for offset in OFFSETS if any(offset)]
WEIGHT_ORDER = (0, 3, 1, 4, 2, 5)


def lens_kernel(
    cuts_ref, sky_hbm, filters_hbm, wiener_hbm, response_hbm, table_hbm, twiddle_hbm, out_ref,
    table_ref, twiddle_ref, sky_ref, raw, weight_ref, slab_out, slab_in, relay_buf, relay_weights, spec_out, spec_in, weights, modes, legs_out, legs_in,
    maps, current, cur_out, cur_in, est_out, est_in, fin_out, fin_in,
    slab_sem, relay_sem, spec_sem, weight_sem, hand_sem, legs_sem, cur_sem, est_sem, fin_sem, send_sem, load_sem,
):
    rows_count, fields_count, local_rows = 4, 4, 2
    groups = rows_count * fields_count
    total_rows = groups * local_rows
    in_rows = total_rows // rows_count
    row_ratio = NC // total_rows
    my_x, my_r, my_z = (lax.axis_index(name) for name in ("sims", "rows", "fields"))
    my_y, my_c, my_h, my_l = my_r // 2, my_r % 2, my_z // 2, my_z % 2
    x_at, y_at, c_at, h_at, l_at = ((bit, 1 - bit) for bit in (my_x, my_y, my_c, my_h, my_l))
    me = my_r * fields_count + 2 * my_x + my_l
    my_block = (2 * my_x + my_l) * rows_count + my_r
    stays = my_x == my_h

    outer = my_l == my_h
    inner = my_l != my_h
    home_row = in_rows * my_r + 4 * my_h + 2 * my_l + my_x

    def signed(row):
        return jnp.where(row < total_rows // 2, row, row - total_rows)

    def row_of(offset):
        return 2 * y_at[offset[1]] + c_at[offset[3]]

    def peer_of(offset):
        return row_of(offset) * fields_count + 2 * x_at[offset[0]] + l_at[offset[2]]

    def peer_block(offset):
        return (2 * x_at[offset[0]] + l_at[offset[2]]) * rows_count + row_of(offset)

    def remote(src, dst, sems, x, r, z):
        return pltpu.make_async_remote_copy(
            src_ref=src, dst_ref=dst, send_sem=sems[0], recv_sem=sems[1],
            device_id={"sims": x, "rows": r, "fields": z}, device_id_type=MESH,
        )

    def send(offset, src, dst, sems):
        return remote(src, dst, sems, x_at[offset[0]], row_of(offset), 2 * my_h + l_at[offset[2]])

    def send_home(offset, src, dst, sems):
        return remote(src, dst, sems, my_h, row_of(offset), 2 * x_at[offset[0]] + l_at[offset[2]])

    def each_peer(body):
        for offset in PEERS:
            body(offset)

    def wait_all(ref, sem):
        pltpu.make_async_copy(ref, ref, sem).wait()

    for src, dst, n in (
        (sky_hbm, sky_ref, 0),
        (filters_hbm, raw.at[0:3], 1),
        (wiener_hbm, raw.at[3:5], 1),
        (response_hbm, raw.at[5], 1),
        (table_hbm, table_ref, 2),
        (twiddle_hbm, twiddle_ref, 3),
    ):
        pltpu.make_async_copy(src, dst, load_sem.at[n]).start()

    (
        slab_left, relay_left, forward_left, spec_left, weight_left, legs_left, cur_left, est_left, fin_left,
        extra_left, pass_left,
    ) = (send_sem.at[n] for n in range(11))

    barrier = pltpu.get_barrier_semaphore()
    for h in BITS:
        for c, a1, e, a0 in OFFSETS:
            if h or c or a1 or e or a0:
                pl.semaphore_signal(
                    barrier, inc=1, device_id_type=MESH,
                    device_id={"sims": x_at[c], "rows": 2 * y_at[a1] + c_at[a0], "fields": 2 * h_at[h] + l_at[e]},
                )
    wait_all(sky_ref, load_sem.at[0])
    tiles = sky_ref.shape[2] // SIDE
    for field in range(3):
        for t in range(tiles):
            slab_out[t // 8, field, :, t % 8, :] = sky_ref[field, :, t * SIDE:(t + 1) * SIDE]
    pl.semaphore_wait(barrier, 2 * groups - 1)

    ROW_OFFSETS = [(0, a1, 0, a0) for a1 in BITS for a0 in BITS]

    def slab_copy(field, offset):
        r = row_of(offset)
        return send_home(
            offset, slab_out.at[r, field], slab_in.at[my_r, field],
            (slab_left, slab_sem.at[field]),
        )

    def own_slab(field):
        return pltpu.make_async_copy(slab_out.at[my_r, field], slab_in.at[my_r, field], slab_sem.at[field])

    def relay_copy(field):
        return remote(
            slab_out.at[pl.ds(2 * y_at[1], 2), field], relay_buf.at[field],
            (relay_left, relay_sem.at[field]), x_at[1], my_r, my_z,
        )

    def forward_copy(field, core):
        a0 = core
        return remote(
            relay_buf.at[field, c_at[a0]], slab_in.at[my_r, field],
            (forward_left, slab_sem.at[field]),
            my_x, 2 * y_at[1] + c_at[a0], 2 * h_at[1] + my_l,
        )

    @pl.when(stays)
    def _():
        for field in range(3):
            own_slab(field).start()
            for offset in ROW_OFFSETS[1:]:
                slab_copy(field, offset).start()

    def slab_start(field):
        relay_copy(field).start()
        for offset in ROW_OFFSETS[:2]:
            slab_copy(field, offset).start()

    @pl.when(jnp.logical_not(stays))
    def _():
        slab_start(0)

    low_index = lax.broadcasted_iota(jnp.int32, (SIDE, SIDE), 0)
    high_index = lax.broadcasted_iota(jnp.int32, (SIDE, SIDE), 1)
    column_ids = low_index + SIDE * high_index
    freq_cols = jnp.where(column_ids < NC // 2, column_ids, column_ids - NC)

    def row_frequency(row):
        return signed(in_rows * my_r + 4 * my_l + 2 * (my_h + row - 2 * my_h * row) + my_x)

    wait_all(raw, load_sem.at[1])

    def spread(n, carry):
        for j in range(8):
            start = pl.multiple_of((n * 8 + j) * SIDE, SIDE)
            weight_ref[:, :, n * 8 + j, :] = raw[:, :, pl.ds(start, SIDE)]
        return carry

    lax.fori_loop(0, SIDE // 8, spread, 0)
    scaled_home = row_ratio * signed(home_row)
    radius_home = freq_cols * freq_cols + scaled_home * scaled_home

    def mask(n):
        low, high = cuts_ref[2 * n], cuts_ref[2 * n + 1]
        inside = (radius_home >= low * low) & (radius_home <= high * high)
        return inside.astype(jnp.float32)

    home_slot = jnp.where(inner, 2, 0)

    def group_of(n):
        return [n in members for members in WEIGHT_GROUPS].index(True)

    def across(n, source, slot, left):
        return remote(
            source, weights.at[n, slot], (left, weight_sem.at[slot, group_of(n)]),
            my_x, my_r, 2 * h_at[1] + my_h,
        )

    def own_weight(n):
        return across(n, weights.at[n, home_slot], 0, weight_left)

    def near_copy(n):
        return remote(
            weights.at[n, home_slot], weights.at[n, 1], (extra_left, weight_sem.at[1, group_of(n)]),
            my_x, my_r, 2 * my_h + l_at[1],
        )

    def hand_copy(n):
        return remote(
            weights.at[n, home_slot], relay_weights.at[n], (weight_left, hand_sem.at[n]),
            my_x, my_r, 2 * my_h + l_at[1],
        )

    def weight_pass_on(members):
        @pl.when(inner)
        def _():
            for n in members:
                wait_all(relay_weights.at[n], hand_sem.at[n])
                across(n, relay_weights.at[n], 1, pass_left).start()

    pol = mask(1)
    weights[0, home_slot] = mask(0) * weight_ref[0, my_x].T
    weights[1, home_slot] = pol * weight_ref[1, my_x].T
    weights[2, home_slot] = pol * weight_ref[2, my_x].T
    weights[3, home_slot] = weight_ref[3, my_x].T
    weights[4, home_slot] = weight_ref[4, my_x].T
    weights[5, home_slot] = mask(2) * weight_ref[5, my_x].T
    @pl.when(jnp.logical_and(inner, jnp.logical_not(stays)))
    def _():
        slab_start(1)
        slab_start(2)
        for n in WEIGHT_ORDER[:5]:
            near_copy(n).start()
            own_weight(n).start()

    @pl.when(jnp.logical_and(outer, jnp.logical_not(stays)))
    def _():
        hand_copy(0).start()
        slab_start(1)
        hand_copy(3).start()
        slab_start(2)
        hand_copy(1).start()

    @pl.when(jnp.logical_and(inner, stays))
    def _():
        own_weight(0).start()
        for n in WEIGHT_ORDER[:5]:
            near_copy(n).start()

    @pl.when(jnp.logical_and(outer, stays))
    def _():
        hand_copy(0).start()
        hand_copy(3).start()

    def place(k, half):
        return 1 - half if k // 2 % 2 else half, k // in_rows * fields_count + 2 * (k % 2) + k // 4 % 2

    def spec_copy(field, row, offset):
        return send(
            offset, spec_out.at[field, row, peer_of(offset)], spec_in.at[field, row, :, my_block],
            (spec_left, spec_sem.at[field]),
        )

    def own_spec(field, row):
        return pltpu.make_async_copy(
            spec_out.at[field, row, me], spec_in.at[field, row, :, my_block], spec_sem.at[field]
        )

    def spec_start(field):
        for row in range(local_rows):
            each_peer(lambda offset: spec_copy(field, row, offset).start())
            own_spec(field, row).start()

    def row_step(field):
        @pl.when(stays)
        def _():
            wait_all(relay_buf.at[field], relay_sem.at[field])
            for core in BITS:
                forward_copy(field, core).start()

        if field == 1:
            @pl.when(jnp.logical_and(outer, stays))
            def _():
                hand_copy(1).start()

        if field == 2:
            @pl.when(jnp.logical_and(inner, stays))
            def _():
                for n in WEIGHT_ORDER[1:5]:
                    own_weight(n).start()

        wait_all(slab_in.at[:, field], slab_sem.at[field])
        values = [
            (slab_in[y // in_rows, field, y % in_rows], None) for y in range(total_rows)
        ]
        for k, (real, imag) in enumerate(short_transform(values, -1)):
            local, device = place(k, my_h)
            spec_out[field, local, device, 0] = real
            spec_out[field, local, device, 1] = jnp.zeros_like(real) if imag is None else imag
        spec_start(field)

    for field in range(3):
        row_step(field)

    @pl.when(outer)
    def _():
        hand_copy(4).start()
        hand_copy(2).start()

    weight_pass_on((0, 3, 1))

    cos_f, sin_f, cos_b, sin_b = 0, 1, 2, 3

    def side_by_side(pieces, axis):
        return pieces[0] if len(pieces) == 1 else jnp.concatenate(pieces, axis=axis)

    def long_forward(pieces):
        y = matrix_left(table_ref, 0, side_by_side(pieces, 1))
        c, s = twiddle_ref[cos_f], twiddle_ref[sin_f]
        turned = []
        for n in range(len(pieces)):
            yr, yi = y[:SIDE, n * SIDE:(n + 1) * SIDE], y[SIDE:, n * SIDE:(n + 1) * SIDE]
            turned.append(jnp.concatenate([yr * c - yi * s, yr * s + yi * c], axis=1))
        z = matrix_right(table_ref, 1, side_by_side(turned, 0))
        return [
            (z[n * SIDE:(n + 1) * SIDE, :SIDE], z[n * SIDE:(n + 1) * SIDE, SIDE:])
            for n in range(len(pieces))
        ]

    def long_inverse(pairs):
        stacks = [jnp.concatenate([pair[0], pair[1]], axis=1) for pair in pairs]
        u = matrix_right(table_ref, 0, side_by_side(stacks, 0))
        c, s = twiddle_ref[cos_b], twiddle_ref[sin_b]
        turned = []
        for n in range(len(pairs)):
            ur, ui = u[n * SIDE:(n + 1) * SIDE, :SIDE], u[n * SIDE:(n + 1) * SIDE, SIDE:]
            turned.append(jnp.concatenate([ur * c - ui * s, ur * s + ui * c], axis=0))
        x = matrix_left(table_ref, 1, side_by_side(turned, 1))
        return [
            x[:, n * SIDE:(n + 1) * SIDE].reshape((2, groups) + TILE)
            for n in range(len(pairs))
        ]

    def legs_copy(row, g, offset):
        first, count = LEG_GROUPS[g]
        return send(
            offset, legs_out.at[row, first:first + count, :, peer_block(offset)],
            legs_in.at[row, me, first:first + count],
            (legs_left, legs_sem.at[g]),
        )

    def own_legs(row, g):
        first, count = LEG_GROUPS[g]
        return pltpu.make_async_copy(
            legs_out.at[row, first:first + count, :, my_block],
            legs_in.at[row, me, first:first + count],
            legs_sem.at[g],
        )

    def wait_weights(group, row):
        members = WEIGHT_GROUPS[group]

        @pl.when(jnp.logical_or(row == 1, inner))
        def _():
            wait_all(weights.at[0:len(members), row], weight_sem.at[row, group])

    def slopes(row):
        along_x = (2 * freq_cols).astype(jnp.float32) / NC
        along_y = (2 * row_frequency(row)).astype(jnp.float32) / total_rows
        return along_x, along_y

    def both_rows(field):
        wait_all(spec_in.at[field], spec_sem.at[field])
        pairs = long_forward([spec_in[field, row].reshape(2 * SIDE, SIDE) for row in range(local_rows)])
        for row, pair in enumerate(pairs):
            modes[field, row, 0], modes[field, row, 1] = pair

    def leg_step(n, row):
        scaled = row_ratio * row_frequency(row)
        radius_sq = freq_cols * freq_cols + scaled * scaled
        floor = jnp.maximum(radius_sq, 1).astype(jnp.float32)
        cos2 = (freq_cols * freq_cols - scaled * scaled).astype(jnp.float32) / floor
        sin2 = (2 * freq_cols * scaled).astype(jnp.float32) / floor
        along_x, along_y = slopes(row)
        raising, lowering = (-along_y, along_x), (along_y, along_x)
        rot = (cos2, sin2)

        def temp_legs():
            t_bar = (weights[0, row] * modes[0, row, 0], weights[0, row] * modes[0, row, 1])
            return t_bar, complex_mul((weights[3, row] * t_bar[0], weights[3, row] * t_bar[1]), raising)

        def e_modes():
            return tuple(
                -weights[1, row] * (cos2 * modes[1, row, n] + sin2 * modes[2, row, n]) for n in range(2)
            )

        def spin_legs():
            e_bar = e_modes()
            w = complex_mul((-weights[4, row] * e_bar[0], -weights[4, row] * e_bar[1]), rot)
            return complex_mul(w, raising), complex_mul(w, lowering)

        def pol_leg():
            e_bar = e_modes()
            b_bar = tuple(
                weights[2, row] * (sin2 * modes[1, row, n] - cos2 * modes[2, row, n]) for n in range(2)
            )
            return (complex_mul((b_bar[1] - e_bar[0], -(e_bar[1] + b_bar[0])), rot),)

        wait_weights(n, row)
        for k, leg_map in enumerate(long_inverse((temp_legs, spin_legs, pol_leg)[n]())):
            legs_out[row, LEG_GROUPS[n][0] + k] = leg_map
        each_peer(lambda offset: legs_copy(row, n, offset).start())
        own_legs(row, n).start()

    wait_all(table_ref, load_sem.at[2])
    wait_all(twiddle_ref, load_sem.at[3])
    both_rows(0)

    @pl.when(outer)
    def _():
        leg_step(0, 0)
        leg_step(0, 1)

    both_rows(1)
    both_rows(2)
    weight_pass_on((4, 2))

    @pl.when(inner)
    def _():
        leg_step(0, 0)

    def later_steps(row, carry):
        @pl.when(jnp.logical_and(inner, row == 1))
        def _():
            leg_step(0, 1)

        leg_step(1, row)
        leg_step(2, row)
        return carry

    lax.fori_loop(0, local_rows, later_steps, 0)

    @pl.when(inner)
    def _():
        own_weight(5).start()
        near_copy(5).start()

    @pl.when(outer)
    def _():
        across(5, weights.at[5, 0], 1, weight_left).start()

    def map_step(n, carry):
        values = [
            (legs_in[place(k, my_h) + (n, 0)], legs_in[place(k, my_h) + (n, 1)])
            for k in range(total_rows)
        ]
        for y, (real, imag) in enumerate(short_transform(values, 1)):
            maps[n, 0, y] = real
            maps[n, 1, y] = imag
        return carry

    for g, (first, count) in enumerate(LEG_GROUPS):
        wait_all(legs_in.at[:, :, first:first + count], legs_sem.at[g])
        lax.fori_loop(first, first + count, map_step, 0)

    def product_step(y, carry):
        a, g, h3, h1, p = [(maps[n, 0, y], maps[n, 1, y]) for n in range(5)]
        ag, ph, hp = complex_mul(a, g), conj_mul(p, h3), conj_mul(h1, p)
        current[0, y] = ag[0] + 0.5 * (ph[0] + hp[0])
        current[1, y] = ag[1] + 0.5 * (ph[1] + hp[1])
        return carry

    lax.fori_loop(0, total_rows, product_step, 0)

    values = [(current[0, y], current[1, y]) for y in range(total_rows)]
    for k, (real, imag) in enumerate(short_transform(values, -1)):
        cur_out[place(k, my_h) + (0,)] = real
        cur_out[place(k, my_h) + (1,)] = imag

    def cur_copy(row, offset):
        return send(
            offset, cur_out.at[row, peer_of(offset)], cur_in.at[row, :, my_block],
            (cur_left, cur_sem.at[row]),
        )

    def own_cur(row):
        return pltpu.make_async_copy(
            cur_out.at[row, me], cur_in.at[row, :, my_block], cur_sem.at[row]
        )

    def cur_start(row, carry):
        each_peer(lambda offset: cur_copy(row, offset).start())
        own_cur(row).start()
        return carry

    lax.fori_loop(0, local_rows, cur_start, 0)

    HOME_OFFSETS = sorted(PEERS, key=lambda offset: -offset[0])
    ORIGIN = (0, 0, 0, 0)

    def part_of(sub):
        return slice(sub * TILE[0] // 2, (sub + 1) * TILE[0] // 2)

    def est_copy(row, offset, sub):
        r, z = row_of(offset), 2 * h_at[offset[0]] + l_at[offset[2]]
        return remote(
            est_out.at[row, :, z * rows_count + r, part_of(sub)], est_in.at[row, me, :, part_of(sub)],
            (est_left, est_sem.at[sub]), my_h, r, z,
        )

    def own_est(row, sub):
        return pltpu.make_async_copy(
            est_out.at[row, :, my_z * rows_count + my_r, part_of(sub)], est_in.at[row, me, :, part_of(sub)],
            est_sem.at[sub],
        )

    def est_start(row, sub):
        for offset in HOME_OFFSETS:
            est_copy(row, offset, sub).start()

        @pl.when(stays)
        def _():
            own_est(row, sub).start()

        @pl.when(jnp.logical_not(stays))
        def _():
            est_copy(row, ORIGIN, sub).start()

    def estimate_step(row):
        wait_all(cur_in.at[row], cur_sem.at[row])
        wait_weights(3, row)
        (modes,) = long_forward([cur_in[row].reshape(2 * SIDE, SIDE)])
        along_x, along_y = slopes(row)
        w = weights[5, row]
        estimate = complex_mul((w * modes[0], w * modes[1]), (along_y, along_x))
        (est_out[row],) = long_inverse([estimate])
        est_start(row, 0)

    for row in range(local_rows):
        estimate_step(row)
    for row in range(local_rows):
        est_start(row, 1)

    def fin_copy(offset, sub):
        r = row_of(offset)
        return remote(
            fin_out.at[r, :, :, part_of(sub)], fin_in.at[my_r, :, :, part_of(sub)],
            (fin_left, fin_sem.at[sub]), my_x, r, my_z,
        )

    def own_fin(sub):
        return pltpu.make_async_copy(
            fin_out.at[my_r, :, :, part_of(sub)], fin_in.at[my_r, :, :, part_of(sub)], fin_sem.at[sub]
        )

    for sub in range(2):
        wait_all(est_in.at[:, :, :, part_of(sub)], est_sem.at[sub])
        values = []
        for k in range(total_rows):
            local, device = place(k, my_x)
            values.append(tuple(est_in[local, device, part, part_of(sub)] for part in range(2)))
        for y, pair in enumerate(short_transform(values, 1)):
            for part in range(2):
                fin_out[y // in_rows, part, y % in_rows, part_of(sub)] = pair[part]
        for offset in ROW_OFFSETS[1:]:
            fin_copy(offset, sub).start()
        own_fin(sub).start()

    others = groups - 1

    @pl.when(stays)
    def _():
        wait_all(slab_out.at[0:3], slab_left)
        wait_all(relay_buf, forward_left)
        wait_all(est_out.at[:, :, 0:others], est_left)

    @pl.when(jnp.logical_not(stays))
    def _():
        wait_all(slab_out.at[0:2], slab_left)
        wait_all(relay_buf, relay_left)
        wait_all(est_out, est_left)

    @pl.when(inner)
    def _():
        wait_all(relay_weights.at[0:5], pass_left)
        wait_all(relay_weights, extra_left)

    wait_all(weights.at[:, 0], weight_left)
    wait_all(spec_out.at[:, :, 0:others], spec_left)
    wait_all(legs_out.at[:, :, :, 0:others], legs_left)
    wait_all(cur_out.at[:, 0:others], cur_left)
    for sub in range(2):
        wait_all(fin_in.at[:, :, :, part_of(sub)], fin_sem.at[sub])
        for part in range(2):
            for t in range(tiles):
                if t % TILE[0] * 2 // TILE[0] == sub:
                    out_ref[part, :, t * SIDE:(t + 1) * SIDE] = fin_in[t // TILE[0], part, :, t % TILE[0], :]

    wait_all(fin_out.at[0:3], fin_left)


def long_tables(total_rows):
    index = np.arange(SIDE)
    angle = 2.0 * np.pi * (index[:, None] * index[None, :] % SIDE) / SIDE
    c, s = np.cos(angle), np.sin(angle)
    forward = np.block([[c, s], [-s, c]]).astype(np.float32)
    tables = np.stack([forward, forward.T])
    top = tables.astype(jnp.bfloat16)
    rest = (tables - top.astype(np.float32)).astype(jnp.bfloat16)
    turn = 2.0 * np.pi * (index[:, None] * index[None, :]) / NC
    scale = 1.0 / (NC * total_rows)
    twiddle = np.stack(
        [np.cos(turn), -np.sin(turn), scale * np.cos(turn), scale * np.sin(turn)]
    ).astype(np.float32)
    return np.stack([top, rest], axis=1), twiddle


def fused_body(rows_count, fields_count, sky_maps, band_cuts, filters, wiener, response):
    groups = rows_count * fields_count
    local_rows = response.shape[0]
    total_rows = local_rows * groups
    in_rows = total_rows // rows_count
    table, twiddle = long_tables(total_rows)
    vmem = pl.BlockSpec(memory_space=pltpu.VMEM)
    f32 = jnp.float32
    dma = pltpu.SemaphoreType.DMA
    slab = pltpu.VMEM((rows_count, 3, in_rows) + TILE, f32)
    chunk = pltpu.VMEM((local_rows, groups, 2) + TILE, f32)
    lines = pltpu.VMEM((local_rows, 2, groups) + TILE, f32)
    final = pltpu.VMEM((rows_count, 2, in_rows) + TILE, f32)
    return pl.pallas_call(
        lens_kernel,
        out_shape=jax.ShapeDtypeStruct((2,) + sky_maps.shape[1:], f32),
        in_specs=[pl.BlockSpec(memory_space=pltpu.SMEM)] + [pl.BlockSpec(memory_space=pl.ANY)] * 6,
        out_specs=vmem,
        scratch_shapes=[
            pltpu.VMEM(table.shape, table.dtype), pltpu.VMEM(twiddle.shape, f32),
            pltpu.VMEM(sky_maps.shape, f32),
            pltpu.VMEM((6, local_rows, NC), f32),
            pltpu.VMEM((6, local_rows, SIDE, SIDE), f32),
            slab, slab,
            pltpu.VMEM((3, 2, in_rows) + TILE, f32),
            pltpu.VMEM((6, SIDE, SIDE), f32),
            pltpu.VMEM((3, local_rows, groups, 2) + TILE, f32),
            pltpu.VMEM((3, local_rows, 2, groups) + TILE, f32),
            pltpu.VMEM((6, 3, SIDE, SIDE), f32),
            pltpu.VMEM((3, local_rows, 2, SIDE, SIDE), f32),
            pltpu.VMEM((local_rows, 5, 2, groups) + TILE, f32),
            pltpu.VMEM((local_rows, groups, 5, 2) + TILE, f32),
            pltpu.VMEM((5, 2, total_rows) + TILE, f32),
            pltpu.VMEM((2, total_rows) + TILE, f32),
            chunk, lines, lines, chunk, final, final,
            dma((3,)), dma((3,)), dma((3,)), dma((local_rows, len(WEIGHT_GROUPS))), dma((6,)), dma((len(LEG_GROUPS),)),
            dma((local_rows,)), dma((2,)), dma((2,)), dma((11,)), dma((4,)),
        ],
        compiler_params=pltpu.CompilerParams(
            collective_id=0, has_side_effects=True, vmem_limit_bytes=60 * 1024 * 1024
        ),
        name="lens",
    )(band_cuts, sky_maps, filters, wiener, response, jnp.asarray(table), jnp.asarray(twiddle))


def solution(mesh):
    placed = (
        P("sims", "rows", "fields"),
        P(),
        P(None, ("rows", "fields"), None),
        P(None, ("rows", "fields"), None),
        P(("rows", "fields"), None),
    )
    rows_count, fields_count = mesh.shape["rows"], mesh.shape["fields"]
    groups = rows_count * fields_count

    def choose(sky_maps, *rest):
        fits = (
            NC == SIDE * SIDE
            and (mesh.shape["sims"], rows_count, fields_count) == (2, 4, 4)
            and NC // groups == TILE[0] * TILE[1]
            and sky_maps.shape[0] == 3
            and sky_maps.shape[1] * rows_count == 32
        )
        if fits:
            return fused_body(rows_count, fields_count, sky_maps, *rest)
        return body(sky_maps, *rest)

    return jax.shard_map(
        choose, mesh=mesh, in_specs=placed, out_specs=P("sims", "rows", "fields"), check_vma=False
    )
```

```python
import functools
import math

import jax
import jax.numpy as jnp
import numpy as np
from jax import lax
from jax.experimental import pallas as pl
from jax.experimental.pallas import tpu as pltpu
from jax.sharding import PartitionSpec as P

NC = 16384


exact_mode = lax.Precision.HIGHEST


def split_factor(length):
    best_first = 1
    for divisor in range(1, math.isqrt(length) + 1):
        if length % divisor == 0:
            best_first = divisor
    return (best_first, length // best_first)


def phase_table(left_index, right_index, period, direction):
    product = left_index[:, None] * right_index[None, :] % period
    angles = direction * 2.0 * math.pi / period * product.astype(jnp.float32)
    return (jnp.cos(angles), jnp.sin(angles))


def complex_einsum(formula, data_pair, table_pair):
    data_real, data_imag = data_pair
    table_real, table_imag = table_pair
    real_out = jnp.einsum(formula, data_real, table_real, precision=exact_mode)
    imag_out = jnp.einsum(formula, data_real, table_imag, precision=exact_mode)
    if data_imag is not None:
        real_out = real_out - jnp.einsum(formula, data_imag, table_imag, precision=exact_mode)
        imag_out = imag_out + jnp.einsum(formula, data_imag, table_real, precision=exact_mode)
    return (real_out, imag_out)


def complex_mul(left_pair, right_pair):
    return (
        left_pair[0] * right_pair[0] - left_pair[1] * right_pair[1],
        left_pair[0] * right_pair[1] + left_pair[1] * right_pair[0],
    )


def conj_mul(left_pair, right_pair):
    return (
        left_pair[0] * right_pair[0] + left_pair[1] * right_pair[1],
        left_pair[0] * right_pair[1] - left_pair[1] * right_pair[0],
    )


def row_transform(data_pair, direction):
    batch_len, length, block_width = data_pair[0].shape
    outer_len, inner_len = split_factor(length)
    outer_ids = jnp.arange(outer_len, dtype=jnp.int32)
    inner_ids = jnp.arange(inner_len, dtype=jnp.int32)
    real_in = data_pair[0].reshape(batch_len, outer_len, inner_len, block_width)
    imag_in = None
    if data_pair[1] is not None:
        imag_in = data_pair[1].reshape(batch_len, outer_len, inner_len, block_width)
    middle = complex_einsum(
        "bjmc,jk->bkmc", (real_in, imag_in), phase_table(outer_ids, outer_ids, outer_len, direction)
    )
    twiddle = phase_table(outer_ids, inner_ids, length, direction)
    middle = complex_mul(middle, (twiddle[0][None, :, :, None], twiddle[1][None, :, :, None]))
    result = complex_einsum(
        "bkmc,mq->bqkc", middle, phase_table(inner_ids, inner_ids, inner_len, direction)
    )
    norm_factor = 1.0 if direction < 0 else 1.0 / length
    return (
        result[0].reshape(batch_len, length, block_width) * norm_factor,
        result[1].reshape(batch_len, length, block_width) * norm_factor,
    )


def block_order(groups, fields_count):
    positions = jnp.arange(groups, dtype=jnp.int32)
    blocks = positions % fields_count * (groups // fields_count) + positions // fields_count
    return (positions, blocks)


def column_forward(data_pair, groups, fields_count):
    batch_len, local_rows, total_len = data_pair[0].shape
    block_width = total_len // groups
    positions, blocks = block_order(groups, fields_count)
    column_ids = jnp.arange(block_width, dtype=jnp.int32)
    shaped = (
        data_pair[0].reshape(batch_len, local_rows, groups, block_width),
        data_pair[1].reshape(batch_len, local_rows, groups, block_width),
    )
    middle = complex_einsum("brpc,pk->brkc", shaped, phase_table(blocks, positions, groups, -1.0))
    twiddle = phase_table(positions, column_ids, total_len, -1.0)
    middle = complex_mul(middle, (twiddle[0][None, None], twiddle[1][None, None]))
    result = complex_einsum(
        "brkc,cq->brqk", middle, phase_table(column_ids, column_ids, block_width, -1.0)
    )
    return (
        result[0].reshape(batch_len, local_rows, total_len),
        result[1].reshape(batch_len, local_rows, total_len),
    )


def column_inverse(data_pair, groups, fields_count):
    batch_len, local_rows, total_len = data_pair[0].shape
    block_width = total_len // groups
    positions, blocks = block_order(groups, fields_count)
    column_ids = jnp.arange(block_width, dtype=jnp.int32)
    shaped = (
        data_pair[0].reshape(batch_len, local_rows, block_width, groups),
        data_pair[1].reshape(batch_len, local_rows, block_width, groups),
    )
    middle = complex_einsum(
        "brqk,qc->brkc", shaped, phase_table(column_ids, column_ids, block_width, 1.0)
    )
    twiddle = phase_table(positions, column_ids, total_len, 1.0)
    middle = complex_mul(middle, (twiddle[0][None, None], twiddle[1][None, None]))
    result = complex_einsum("brkc,kp->brpc", middle, phase_table(positions, blocks, groups, 1.0))
    norm_factor = 1.0 / total_len
    return (
        result[0].reshape(batch_len, local_rows, total_len) * norm_factor,
        result[1].reshape(batch_len, local_rows, total_len) * norm_factor,
    )


def body(sky_maps, band_cuts, filters, wiener, response):
    rows_count = lax.axis_size("rows")
    fields_count = lax.axis_size("fields")
    groups = rows_count * fields_count
    local_rows = filters.shape[1]
    total_rows = local_rows * groups
    row_ratio = NC // total_rows

    def forward_columns(stacked):
        return jnp.stack(column_forward((stacked[0], stacked[1]), groups, fields_count))

    def inverse_rows(stacked):
        return jnp.stack(row_transform((stacked[0], stacked[1]), 1.0))

    def inverse_columns(stacked):
        return jnp.stack(column_inverse((stacked[0], stacked[1]), groups, fields_count))

    def to_frequency(stacked):
        batch_len = stacked.shape[1]
        block_width = stacked.shape[3]
        shaped = stacked.reshape(
            2, batch_len, rows_count, fields_count, local_rows, 1, 1, block_width
        )
        arrived = lax.all_to_all(
            lax.all_to_all(shaped, "rows", split_axis=2, concat_axis=5, tiled=True),
            "fields",
            split_axis=3,
            concat_axis=6,
            tiled=True,
        )
        result = forward_columns(arrived.reshape(2, batch_len, local_rows, groups * block_width))
        return result

    def to_space(stacked):
        batch_len = stacked.shape[1]
        block_width = stacked.shape[3] // groups
        shaped = stacked.reshape(
            2, batch_len, 1, 1, local_rows, rows_count, fields_count, block_width
        )
        arrived = lax.all_to_all(
            lax.all_to_all(shaped, "rows", split_axis=5, concat_axis=2, tiled=True),
            "fields",
            split_axis=6,
            concat_axis=3,
            tiled=True,
        )
        result = inverse_rows(arrived.reshape(2, batch_len, total_rows, block_width))
        return result

    slab_spectra = jnp.stack(
        row_transform(
            (lax.all_to_all(sky_maps, "rows", split_axis=2, concat_axis=1, tiled=True), None), -1.0
        )
    )
    sky_spectra = to_frequency(slab_spectra)
    row_ids = lax.axis_index(("rows", "fields")) * local_rows + jnp.arange(
        local_rows, dtype=jnp.int32
    )
    freq_rows = jnp.where(row_ids < total_rows // 2, row_ids, row_ids - total_rows)[:, None]
    column_ids = jnp.arange(NC, dtype=jnp.int32)
    freq_cols = jnp.where(column_ids < NC // 2, column_ids, column_ids - NC)[None, :]
    scaled_rows = row_ratio * freq_rows
    radius_sq = freq_cols * freq_cols + scaled_rows * scaled_rows

    def band_mask(lower_cut, upper_cut):
        inside = (radius_sq >= lower_cut * lower_cut) & (radius_sq <= upper_cut * upper_cut)
        return inside.astype(jnp.float32)

    mask_temp = band_mask(band_cuts[0], band_cuts[1])
    mask_pol = band_mask(band_cuts[2], band_cuts[3])
    mask_out = band_mask(band_cuts[4], band_cuts[5])
    radius_floor = jnp.maximum(radius_sq, 1).astype(jnp.float32)
    cos_two = (freq_cols * freq_cols - scaled_rows * scaled_rows).astype(jnp.float32) / radius_floor
    sin_two = (2 * freq_cols * scaled_rows).astype(jnp.float32) / radius_floor
    along_x = (2 * freq_cols).astype(jnp.float32) / NC
    along_y = (2 * freq_rows).astype(jnp.float32) / total_rows
    raising = (-along_y + 0.0 * along_x, along_x + 0.0 * along_y)
    lowering = (along_y + 0.0 * along_x, along_x + 0.0 * along_y)
    rotation = (cos_two, sin_two)
    temp_modes = (sky_spectra[0, 0], sky_spectra[1, 0])
    stokes_q = (sky_spectra[0, 1], sky_spectra[1, 1])
    stokes_u = (sky_spectra[0, 2], sky_spectra[1, 2])
    e_modes = (
        -(cos_two * stokes_q[0] + sin_two * stokes_u[0]),
        -(cos_two * stokes_q[1] + sin_two * stokes_u[1]),
    )
    b_modes = (
        sin_two * stokes_q[0] - cos_two * stokes_u[0],
        sin_two * stokes_q[1] - cos_two * stokes_u[1],
    )
    temp_weight = mask_temp * filters[0]
    e_weight = mask_pol * filters[1]
    b_weight = mask_pol * filters[2]
    temp_bar = (temp_weight * temp_modes[0], temp_weight * temp_modes[1])
    e_bar = (e_weight * e_modes[0], e_weight * e_modes[1])
    b_bar = (b_weight * b_modes[0], b_weight * b_modes[1])
    grad_temp = complex_mul(raising, (wiener[0] * temp_bar[0], wiener[0] * temp_bar[1]))
    pol_sum = complex_mul((e_bar[0] - b_bar[1], e_bar[1] + b_bar[0]), rotation)
    pol_bar = (-pol_sum[0], -pol_sum[1])
    pol_rot = complex_mul((wiener[1] * e_bar[0], wiener[1] * e_bar[1]), rotation)
    pol_wiener = (-pol_rot[0], -pol_rot[1])
    spin_three = complex_mul(raising, pol_wiener)
    spin_one = complex_mul(lowering, pol_wiener)
    leg_spectra = jnp.stack(
        [
            jnp.stack([temp_bar[0], grad_temp[0], pol_bar[0], spin_three[0], spin_one[0]]),
            jnp.stack([temp_bar[1], grad_temp[1], pol_bar[1], spin_three[1], spin_one[1]]),
        ]
    )
    leg_maps = to_space(inverse_columns(leg_spectra))
    temp_leg = (leg_maps[0, 0], leg_maps[1, 0])
    grad_leg = (leg_maps[0, 1], leg_maps[1, 1])
    pol_leg = (leg_maps[0, 2], leg_maps[1, 2])
    three_leg = (leg_maps[0, 3], leg_maps[1, 3])
    one_leg = (leg_maps[0, 4], leg_maps[1, 4])
    temp_term = complex_mul(temp_leg, grad_leg)
    raise_term = conj_mul(pol_leg, three_leg)
    lower_term = conj_mul(one_leg, pol_leg)
    current = (
        temp_term[0] + 0.5 * (raise_term[0] + lower_term[0]),
        temp_term[1] + 0.5 * (raise_term[1] + lower_term[1]),
    )
    current_rows = jnp.stack(row_transform((current[0][None], current[1][None]), -1.0))
    current_modes = to_frequency(current_rows)
    out_weight = mask_out * response
    estimate_modes = complex_mul(
        lowering, (out_weight * current_modes[0, 0], out_weight * current_modes[1, 0])
    )
    estimate_stack = jnp.stack([estimate_modes[0][None], estimate_modes[1][None]])
    estimate_maps = to_space(inverse_columns(estimate_stack))
    slab_result = estimate_maps[:, 0]
    return lax.all_to_all(slab_result, "rows", split_axis=1, concat_axis=2, tiled=True)


SIDE = 128
TILE = (8, 128)
LEG_GROUPS = ((0, 2), (2, 2), (4, 1))
WEIGHT_GROUPS = ((0, 3), (1, 4), (2,), (5,))
MESH = pl.DeviceIdType.MESH


def add_pair(a, b):
    imag = a[1] if b[1] is None else b[1] if a[1] is None else a[1] + b[1]
    return (a[0] + b[0], imag)


def sub_pair(a, b):
    imag = a[1] if b[1] is None else -b[1] if a[1] is None else a[1] - b[1]
    return (a[0] - b[0], imag)


def turn_pair(value, step, length, direction):
    real, imag = value
    if step == 0:
        return value
    if 4 * step == length:
        if imag is None:
            return (jnp.zeros_like(real), real if direction > 0 else -real)
        return (-imag, real) if direction > 0 else (imag, -real)
    angle = 2.0 * math.pi * step / length
    c, s = math.cos(angle), direction * math.sin(angle)
    if imag is None:
        return (real * c, real * s)
    if 8 * step == length:
        if direction > 0:
            return ((real - imag) * c, (real + imag) * c)
        return ((real + imag) * c, (imag - real) * c)
    if 8 * step == 3 * length:
        if direction > 0:
            return ((real + imag) * c, (imag - real) * c)
        return ((real - imag) * c, (real + imag) * c)
    return (real * c - imag * s, real * s + imag * c)


def short_transform(values, direction):
    length = len(values)
    if length == 1:
        return values
    even = short_transform(values[0::2], direction)
    odd = short_transform(values[1::2], direction)
    low, high = [], []
    for step in range(length // 2):
        turned = turn_pair(odd[step], step, length, direction)
        low.append(add_pair(even[step], turned))
        high.append(sub_pair(even[step], turned))
    return low + high


def split_number(x):
    top = x.astype(jnp.bfloat16)
    return top, (x - top.astype(jnp.float32)).astype(jnp.bfloat16)


def dot32(a, b):
    return jnp.dot(a, b, preferred_element_type=jnp.float32)


def matrix_left(table_ref, which, x):
    top, rest = split_number(x)
    m_top, m_rest = table_ref[which, 0], table_ref[which, 1]
    return dot32(m_top, top) + (dot32(m_top, rest) + dot32(m_rest, top))


def matrix_right(table_ref, which, x):
    top, rest = split_number(x)
    m_top, m_rest = table_ref[which, 0], table_ref[which, 1]
    return dot32(top, m_top) + (dot32(top, m_rest) + dot32(rest, m_top))


BITS = (0, 1)
SUBS = 2
OFFSETS = [
    (c, a1, e, a0) for a0 in BITS for c, a1, e in
    ((1, 1, 1), (1, 0, 0), (0, 1, 0), (0, 0, 1), (1, 1, 0), (0, 1, 1), (1, 0, 1), (0, 0, 0))
]
PEERS = sorted((offset for offset in OFFSETS if any(offset)), key=lambda offset: -sum(offset[:3]))
WEIGHT_ORDER = (0, 3, 1, 4, 2, 5)


def lens_kernel(
    cuts_ref, sky_hbm, filters_hbm, wiener_hbm, response_hbm, table_hbm, twiddle_hbm, out_ref,
    table_ref, twiddle_ref, sky_ref, raw, weight_ref, slab_out, slab_in, relay_buf, relay_weights, spec_out, spec_in, weights, modes, legs_out, legs_in,
    maps, cur_out, cur_in, est_out, est_in, fin_out, fin_in,
    slab_sem, relay_sem, spec_sem, weight_sem, hand_sem, legs_sem, cur_sem, est_sem, fin_sem, send_sem, load_sem,
):
    rows_count, fields_count, local_rows = 4, 4, 2
    groups = rows_count * fields_count
    total_rows = groups * local_rows
    in_rows = total_rows // rows_count
    row_ratio = NC // total_rows
    my_x, my_r, my_z = (lax.axis_index(name) for name in ("sims", "rows", "fields"))
    my_y, my_c, my_h, my_l = my_r // 2, my_r % 2, my_z // 2, my_z % 2
    x_at, y_at, c_at, h_at, l_at = ((bit, 1 - bit) for bit in (my_x, my_y, my_c, my_h, my_l))
    me = my_r * fields_count + 2 * my_x + my_l
    my_block = (2 * my_x + my_l) * rows_count + my_r
    stays = my_x == my_h

    outer = my_l == my_h
    inner = my_l != my_h
    home_row = in_rows * my_r + 4 * my_h + 2 * my_l + my_x

    def signed(row):
        return jnp.where(row < total_rows // 2, row, row - total_rows)

    def row_of(offset):
        return 2 * y_at[offset[1]] + c_at[offset[3]]

    def peer_of(offset):
        return row_of(offset) * fields_count + 2 * x_at[offset[0]] + l_at[offset[2]]

    def peer_block(offset):
        return (2 * x_at[offset[0]] + l_at[offset[2]]) * rows_count + row_of(offset)

    def remote(src, dst, sems, x, r, z):
        return pltpu.make_async_remote_copy(
            src_ref=src, dst_ref=dst, send_sem=sems[0], recv_sem=sems[1],
            device_id={"sims": x, "rows": r, "fields": z}, device_id_type=MESH,
        )

    def send(offset, src, dst, sems):
        return remote(src, dst, sems, x_at[offset[0]], row_of(offset), 2 * my_h + l_at[offset[2]])

    def send_home(offset, src, dst, sems):
        return remote(src, dst, sems, my_h, row_of(offset), 2 * x_at[offset[0]] + l_at[offset[2]])

    def each_peer(body):
        for offset in PEERS:
            body(offset)

    def wait_all(ref, sem):
        pltpu.make_async_copy(ref, ref, sem).wait()

    for src, dst, n in (
        (sky_hbm, sky_ref, 0),
        (filters_hbm, raw.at[0:3], 1),
        (wiener_hbm, raw.at[3:5], 1),
        (response_hbm, raw.at[5], 1),
        (table_hbm, table_ref, 2),
        (twiddle_hbm, twiddle_ref, 3),
    ):
        pltpu.make_async_copy(src, dst, load_sem.at[n]).start()

    (
        slab_left, relay_left, forward_left, spec_left, weight_left, legs_left, cur_left, est_left, fin_left,
        extra_left, pass_left,
    ) = (send_sem.at[n] for n in range(11))

    barrier = pltpu.get_barrier_semaphore()
    for h in BITS:
        for c, a1, e, a0 in OFFSETS:
            if h or c or a1 or e or a0:
                pl.semaphore_signal(
                    barrier, inc=1, device_id_type=MESH,
                    device_id={"sims": x_at[c], "rows": 2 * y_at[a1] + c_at[a0], "fields": 2 * h_at[h] + l_at[e]},
                )
    wait_all(sky_ref, load_sem.at[0])
    tiles = sky_ref.shape[2] // SIDE
    for field in range(3):
        for t in range(tiles):
            slab_out[t // 8, field, :, t % 8, :] = sky_ref[field, :, t * SIDE:(t + 1) * SIDE]
    pl.semaphore_wait(barrier, 2 * groups - 1)

    ROW_OFFSETS = [(0, a1, 0, a0) for a1 in BITS for a0 in BITS]

    def slab_copy(field, offset):
        r = row_of(offset)
        return send_home(
            offset, slab_out.at[r, field], slab_in.at[my_r, field],
            (slab_left, slab_sem.at[field]),
        )

    def own_slab(field):
        return pltpu.make_async_copy(slab_out.at[my_r, field], slab_in.at[my_r, field], slab_sem.at[field])

    def relay_copy(field):
        return remote(
            slab_out.at[pl.ds(2 * y_at[1], 2), field], relay_buf.at[field],
            (relay_left, relay_sem.at[field]), x_at[1], my_r, my_z,
        )

    def forward_copy(field, core):
        a0 = core
        return remote(
            relay_buf.at[field, c_at[a0]], slab_in.at[my_r, field],
            (forward_left, slab_sem.at[field]),
            my_x, 2 * y_at[1] + c_at[a0], 2 * h_at[1] + my_l,
        )

    @pl.when(stays)
    def _():
        for field in range(3):
            own_slab(field).start()
            for offset in ROW_OFFSETS[1:]:
                slab_copy(field, offset).start()

    def slab_start(field):
        relay_copy(field).start()
        for offset in ROW_OFFSETS[:2]:
            slab_copy(field, offset).start()

    @pl.when(jnp.logical_not(stays))
    def _():
        slab_start(0)

    low_index = lax.broadcasted_iota(jnp.int32, (SIDE, SIDE), 0)
    high_index = lax.broadcasted_iota(jnp.int32, (SIDE, SIDE), 1)
    column_ids = low_index + SIDE * high_index
    freq_cols = jnp.where(column_ids < NC // 2, column_ids, column_ids - NC)

    def row_frequency(row):
        return signed(in_rows * my_r + 4 * my_l + 2 * (my_h + row - 2 * my_h * row) + my_x)

    wait_all(raw, load_sem.at[1])

    def spread(n, carry):
        for j in range(8):
            start = pl.multiple_of((n * 8 + j) * SIDE, SIDE)
            weight_ref[:, :, n * 8 + j, :] = raw[:, :, pl.ds(start, SIDE)]
        return carry

    lax.fori_loop(0, SIDE // 8, spread, 0)
    scaled_home = row_ratio * signed(home_row)
    radius_home = freq_cols * freq_cols + scaled_home * scaled_home

    def mask(n):
        low, high = cuts_ref[2 * n], cuts_ref[2 * n + 1]
        inside = (radius_home >= low * low) & (radius_home <= high * high)
        return inside.astype(jnp.float32)

    home_slot = jnp.where(inner, 2, 0)

    def group_of(n):
        return [n in members for members in WEIGHT_GROUPS].index(True)

    def across(n, source, slot, left):
        return remote(
            source, weights.at[n, slot], (left, weight_sem.at[slot, group_of(n)]),
            my_x, my_r, 2 * h_at[1] + my_h,
        )

    def own_weight(n):
        return across(n, weights.at[n, home_slot], 0, weight_left)

    def near_copy(n):
        return remote(
            weights.at[n, home_slot], weights.at[n, 1], (extra_left, weight_sem.at[1, group_of(n)]),
            my_x, my_r, 2 * my_h + l_at[1],
        )

    def hand_copy(n):
        return remote(
            weights.at[n, home_slot], relay_weights.at[n], (weight_left, hand_sem.at[n]),
            my_x, my_r, 2 * my_h + l_at[1],
        )

    def weight_pass_on(members):
        @pl.when(inner)
        def _():
            for n in members:
                wait_all(relay_weights.at[n], hand_sem.at[n])
                across(n, relay_weights.at[n], 1, pass_left).start()

    pol = mask(1)
    weights[0, home_slot] = mask(0) * weight_ref[0, my_x].T
    weights[1, home_slot] = pol * weight_ref[1, my_x].T
    weights[2, home_slot] = pol * weight_ref[2, my_x].T
    weights[3, home_slot] = weight_ref[3, my_x].T
    weights[4, home_slot] = weight_ref[4, my_x].T
    weights[5, home_slot] = mask(2) * weight_ref[5, my_x].T
    @pl.when(jnp.logical_and(inner, jnp.logical_not(stays)))
    def _():
        slab_start(1)
        slab_start(2)
        for n in WEIGHT_ORDER[:5]:
            near_copy(n).start()
            own_weight(n).start()

    @pl.when(jnp.logical_and(outer, jnp.logical_not(stays)))
    def _():
        hand_copy(0).start()
        slab_start(1)
        hand_copy(3).start()
        slab_start(2)
        hand_copy(1).start()

    @pl.when(jnp.logical_and(inner, stays))
    def _():
        own_weight(0).start()
        for n in WEIGHT_ORDER[:5]:
            near_copy(n).start()

    @pl.when(jnp.logical_and(outer, stays))
    def _():
        hand_copy(0).start()
        hand_copy(3).start()

    def place(k, half):
        return 1 - half if k // 2 % 2 else half, k // in_rows * fields_count + 2 * (k % 2) + k // 4 % 2

    def spec_copy(field, row, offset):
        return send(
            offset, spec_out.at[field, row, peer_of(offset)], spec_in.at[field, row, :, my_block],
            (spec_left, spec_sem.at[field]),
        )

    def own_spec(field, row):
        return pltpu.make_async_copy(
            spec_out.at[field, row, me], spec_in.at[field, row, :, my_block], spec_sem.at[field]
        )

    def spec_start(field):
        for row in range(local_rows):
            each_peer(lambda offset: spec_copy(field, row, offset).start())
            own_spec(field, row).start()

    def row_step(field):
        @pl.when(stays)
        def _():
            wait_all(relay_buf.at[field], relay_sem.at[field])
            for core in BITS:
                forward_copy(field, core).start()

        if field == 1:
            @pl.when(jnp.logical_and(outer, stays))
            def _():
                hand_copy(1).start()

        if field == 2:
            @pl.when(jnp.logical_and(inner, stays))
            def _():
                for n in WEIGHT_ORDER[1:5]:
                    own_weight(n).start()

        wait_all(slab_in.at[:, field], slab_sem.at[field])
        values = [
            (slab_in[y // in_rows, field, y % in_rows], None) for y in range(total_rows)
        ]
        for k, (real, imag) in enumerate(short_transform(values, -1)):
            local, device = place(k, my_h)
            spec_out[field, local, device, 0] = real
            spec_out[field, local, device, 1] = jnp.zeros_like(real) if imag is None else imag
        spec_start(field)

    for field in range(3):
        row_step(field)

    @pl.when(outer)
    def _():
        hand_copy(4).start()
        hand_copy(2).start()

    weight_pass_on((0, 3, 1))

    cos_f, sin_f, cos_b, sin_b = 0, 1, 2, 3

    def side_by_side(pieces, axis):
        return pieces[0] if len(pieces) == 1 else jnp.concatenate(pieces, axis=axis)

    def long_forward(pieces):
        y = matrix_left(table_ref, 0, side_by_side(pieces, 1))
        c, s = twiddle_ref[cos_f], twiddle_ref[sin_f]
        turned = []
        for n in range(len(pieces)):
            yr, yi = y[:SIDE, n * SIDE:(n + 1) * SIDE], y[SIDE:, n * SIDE:(n + 1) * SIDE]
            turned.append(jnp.concatenate([yr * c - yi * s, yr * s + yi * c], axis=1))
        z = matrix_right(table_ref, 1, side_by_side(turned, 0))
        return [
            (z[n * SIDE:(n + 1) * SIDE, :SIDE], z[n * SIDE:(n + 1) * SIDE, SIDE:])
            for n in range(len(pieces))
        ]

    def long_inverse(pairs):
        stacks = [jnp.concatenate([pair[0], pair[1]], axis=1) for pair in pairs]
        u = matrix_right(table_ref, 0, side_by_side(stacks, 0))
        c, s = twiddle_ref[cos_b], twiddle_ref[sin_b]
        turned = []
        for n in range(len(pairs)):
            ur, ui = u[n * SIDE:(n + 1) * SIDE, :SIDE], u[n * SIDE:(n + 1) * SIDE, SIDE:]
            turned.append(jnp.concatenate([ur * c - ui * s, ur * s + ui * c], axis=0))
        x = matrix_left(table_ref, 1, side_by_side(turned, 1))
        return [
            x[:, n * SIDE:(n + 1) * SIDE].reshape((2, groups) + TILE)
            for n in range(len(pairs))
        ]

    def legs_copy(row, g, offset):
        first, count = LEG_GROUPS[g]
        return send(
            offset, legs_out.at[row, first:first + count, :, peer_block(offset)],
            legs_in.at[row, me, first:first + count],
            (legs_left, legs_sem.at[g]),
        )

    def own_legs(row, g):
        first, count = LEG_GROUPS[g]
        return pltpu.make_async_copy(
            legs_out.at[row, first:first + count, :, my_block],
            legs_in.at[row, me, first:first + count],
            legs_sem.at[g],
        )

    def wait_weights(group, row):
        members = WEIGHT_GROUPS[group]

        @pl.when(jnp.logical_or(row == 1, inner))
        def _():
            wait_all(weights.at[0:len(members), row], weight_sem.at[row, group])

    def slopes(row):
        along_x = (2 * freq_cols).astype(jnp.float32) / NC
        along_y = (2 * row_frequency(row)).astype(jnp.float32) / total_rows
        return along_x, along_y

    def both_rows(field):
        wait_all(spec_in.at[field], spec_sem.at[field])
        pairs = long_forward([spec_in[field, row].reshape(2 * SIDE, SIDE) for row in range(local_rows)])
        for row, pair in enumerate(pairs):
            modes[field, row, 0], modes[field, row, 1] = pair

    def leg_step(n, row):
        scaled = row_ratio * row_frequency(row)
        radius_sq = freq_cols * freq_cols + scaled * scaled
        floor = jnp.maximum(radius_sq, 1).astype(jnp.float32)
        cos2 = (freq_cols * freq_cols - scaled * scaled).astype(jnp.float32) / floor
        sin2 = (2 * freq_cols * scaled).astype(jnp.float32) / floor
        along_x, along_y = slopes(row)
        raising, lowering = (-along_y, along_x), (along_y, along_x)
        rot = (cos2, sin2)

        def temp_legs():
            t_bar = (weights[0, row] * modes[0, row, 0], weights[0, row] * modes[0, row, 1])
            return t_bar, complex_mul((weights[3, row] * t_bar[0], weights[3, row] * t_bar[1]), raising)

        def e_modes():
            return tuple(
                -weights[1, row] * (cos2 * modes[1, row, n] + sin2 * modes[2, row, n]) for n in range(2)
            )

        def spin_legs():
            e_bar = e_modes()
            w = complex_mul((-weights[4, row] * e_bar[0], -weights[4, row] * e_bar[1]), rot)
            return complex_mul(w, raising), complex_mul(w, lowering)

        def pol_leg():
            e_bar = e_modes()
            b_bar = tuple(
                weights[2, row] * (sin2 * modes[1, row, n] - cos2 * modes[2, row, n]) for n in range(2)
            )
            return (complex_mul((b_bar[1] - e_bar[0], -(e_bar[1] + b_bar[0])), rot),)

        wait_weights(n, row)
        for k, leg_map in enumerate(long_inverse((temp_legs, spin_legs, pol_leg)[n]())):
            legs_out[row, LEG_GROUPS[n][0] + k] = leg_map
        each_peer(lambda offset: legs_copy(row, n, offset).start())
        own_legs(row, n).start()

    wait_all(table_ref, load_sem.at[2])
    wait_all(twiddle_ref, load_sem.at[3])
    both_rows(0)

    @pl.when(outer)
    def _():
        leg_step(0, 0)
        leg_step(0, 1)

    both_rows(1)
    both_rows(2)
    weight_pass_on((4, 2))

    @pl.when(inner)
    def _():
        leg_step(0, 0)

    def later_steps(row, carry):
        @pl.when(jnp.logical_and(inner, row == 1))
        def _():
            leg_step(0, 1)

        leg_step(1, row)
        leg_step(2, row)
        return carry

    lax.fori_loop(0, local_rows, later_steps, 0)

    @pl.when(inner)
    def _():
        own_weight(5).start()

    @pl.when(outer)
    def _():
        across(5, weights.at[5, 0], 1, weight_left).start()

    def map_step(n, carry):
        values = [
            (legs_in[place(k, my_h) + (n, 0)], legs_in[place(k, my_h) + (n, 1)])
            for k in range(total_rows)
        ]
        for y, (real, imag) in enumerate(short_transform(values, 1)):
            maps[n, 0, y] = real
            maps[n, 1, y] = imag
        return carry

    for g, (first, count) in enumerate(LEG_GROUPS):
        wait_all(legs_in.at[:, :, first:first + count], legs_sem.at[g])
        lax.fori_loop(first, first + count, map_step, 0)

    def product(y):
        a, g, h3, h1, p = [(maps[n, 0, y], maps[n, 1, y]) for n in range(5)]
        ag, ph, hp = complex_mul(a, g), conj_mul(p, h3), conj_mul(h1, p)
        return ag[0] + 0.5 * (ph[0] + hp[0]), ag[1] + 0.5 * (ph[1] + hp[1])

    values = [product(y) for y in range(total_rows)]
    for k, (real, imag) in enumerate(short_transform(values, -1)):
        cur_out[place(k, my_h) + (0,)] = real
        cur_out[place(k, my_h) + (1,)] = imag

    def cur_copy(row, offset):
        return send(
            offset, cur_out.at[row, peer_of(offset)], cur_in.at[row, :, my_block],
            (cur_left, cur_sem.at[row]),
        )

    def own_cur(row):
        return pltpu.make_async_copy(
            cur_out.at[row, me], cur_in.at[row, :, my_block], cur_sem.at[row]
        )

    def cur_start(row, carry):
        each_peer(lambda offset: cur_copy(row, offset).start())
        own_cur(row).start()
        return carry

    lax.fori_loop(0, local_rows, cur_start, 0)

    @pl.when(inner)
    def _():
        near_copy(5).start()


    HOME_OFFSETS = sorted(PEERS, key=lambda offset: -offset[0])
    ORIGIN = (0, 0, 0, 0)

    def part_of(sub):
        return slice(sub * TILE[0] // SUBS, (sub + 1) * TILE[0] // SUBS)

    def est_copy(row, offset, sub):
        r, z = row_of(offset), 2 * h_at[offset[0]] + l_at[offset[2]]
        return remote(
            est_out.at[row, :, z * rows_count + r, part_of(sub)], est_in.at[row, me, :, part_of(sub)],
            (est_left, est_sem.at[sub]), my_h, r, z,
        )

    def own_est(row, sub):
        return pltpu.make_async_copy(
            est_out.at[row, :, my_z * rows_count + my_r, part_of(sub)], est_in.at[row, me, :, part_of(sub)],
            est_sem.at[sub],
        )

    def est_start(row, sub):
        for offset in HOME_OFFSETS:
            est_copy(row, offset, sub).start()

        @pl.when(stays)
        def _():
            own_est(row, sub).start()

        @pl.when(jnp.logical_not(stays))
        def _():
            est_copy(row, ORIGIN, sub).start()

    def estimate_step(row):
        wait_all(cur_in.at[row], cur_sem.at[row])
        wait_weights(3, row)
        (modes,) = long_forward([cur_in[row].reshape(2 * SIDE, SIDE)])
        along_x, along_y = slopes(row)
        w = weights[5, row]
        estimate = complex_mul((w * modes[0], w * modes[1]), (along_y, along_x))
        (est_out[row],) = long_inverse([estimate])
        est_start(row, 0)

    for row in range(local_rows):
        estimate_step(row)
    for sub in range(1, SUBS):
        for row in range(local_rows):
            est_start(row, sub)

    def fin_copy(offset, sub):
        r = row_of(offset)
        return remote(
            fin_out.at[r, :, :, part_of(sub)], fin_in.at[my_r, :, :, part_of(sub)],
            (fin_left, fin_sem.at[sub]), my_x, r, my_z,
        )

    def own_fin(sub):
        return pltpu.make_async_copy(
            fin_out.at[my_r, :, :, part_of(sub)], fin_in.at[my_r, :, :, part_of(sub)], fin_sem.at[sub]
        )

    for sub in range(SUBS):
        wait_all(est_in.at[:, :, :, part_of(sub)], est_sem.at[sub])
        values = []
        for k in range(total_rows):
            local, device = place(k, my_x)
            values.append(tuple(est_in[local, device, part, part_of(sub)] for part in range(2)))
        for y, pair in enumerate(short_transform(values, 1)):
            for part in range(2):
                fin_out[y // in_rows, part, y % in_rows, part_of(sub)] = pair[part]
        for offset in ROW_OFFSETS[1:]:
            fin_copy(offset, sub).start()
        own_fin(sub).start()

    others = groups - 1

    @pl.when(stays)
    def _():
        wait_all(slab_out.at[0:3], slab_left)
        wait_all(relay_buf, forward_left)
        wait_all(est_out.at[:, :, 0:others], est_left)

    @pl.when(jnp.logical_not(stays))
    def _():
        wait_all(slab_out.at[0:2], slab_left)
        wait_all(relay_buf, relay_left)
        wait_all(est_out, est_left)

    @pl.when(inner)
    def _():
        wait_all(relay_weights.at[0:5], pass_left)
        wait_all(relay_weights, extra_left)

    wait_all(weights.at[:, 0], weight_left)
    wait_all(spec_out.at[:, :, 0:others], spec_left)
    wait_all(legs_out.at[:, :, :, 0:others], legs_left)
    wait_all(cur_out.at[:, 0:others], cur_left)
    for sub in range(SUBS):
        wait_all(fin_in.at[:, :, :, part_of(sub)], fin_sem.at[sub])
        for part in range(2):
            for t in range(tiles):
                if t % TILE[0] * SUBS // TILE[0] == sub:
                    out_ref[part, :, t * SIDE:(t + 1) * SIDE] = fin_in[t // TILE[0], part, :, t % TILE[0], :]

    wait_all(fin_out.at[0:3], fin_left)


def long_tables(total_rows):
    index = np.arange(SIDE)
    angle = 2.0 * np.pi * (index[:, None] * index[None, :] % SIDE) / SIDE
    c, s = np.cos(angle), np.sin(angle)
    forward = np.block([[c, s], [-s, c]]).astype(np.float32)
    tables = np.stack([forward, forward.T])
    top = tables.astype(jnp.bfloat16)
    rest = (tables - top.astype(np.float32)).astype(jnp.bfloat16)
    turn = 2.0 * np.pi * (index[:, None] * index[None, :]) / NC
    scale = 1.0 / (NC * total_rows)
    twiddle = np.stack(
        [np.cos(turn), -np.sin(turn), scale * np.cos(turn), scale * np.sin(turn)]
    ).astype(np.float32)
    return np.stack([top, rest], axis=1), twiddle


def fused_body(rows_count, fields_count, sky_maps, band_cuts, filters, wiener, response):
    groups = rows_count * fields_count
    local_rows = response.shape[0]
    total_rows = local_rows * groups
    in_rows = total_rows // rows_count
    table, twiddle = long_tables(total_rows)
    vmem = pl.BlockSpec(memory_space=pltpu.VMEM)
    f32 = jnp.float32
    dma = pltpu.SemaphoreType.DMA
    slab = pltpu.VMEM((rows_count, 3, in_rows) + TILE, f32)
    chunk = pltpu.VMEM((local_rows, groups, 2) + TILE, f32)
    lines = pltpu.VMEM((local_rows, 2, groups) + TILE, f32)
    final = pltpu.VMEM((rows_count, 2, in_rows) + TILE, f32)
    return pl.pallas_call(
        lens_kernel,
        out_shape=jax.ShapeDtypeStruct((2,) + sky_maps.shape[1:], f32),
        in_specs=[pl.BlockSpec(memory_space=pltpu.SMEM)] + [pl.BlockSpec(memory_space=pl.ANY)] * 6,
        out_specs=vmem,
        scratch_shapes=[
            pltpu.VMEM(table.shape, table.dtype), pltpu.VMEM(twiddle.shape, f32),
            pltpu.VMEM(sky_maps.shape, f32),
            pltpu.VMEM((6, local_rows, NC), f32),
            pltpu.VMEM((6, local_rows, SIDE, SIDE), f32),
            slab, slab,
            pltpu.VMEM((3, 2, in_rows) + TILE, f32),
            pltpu.VMEM((6, SIDE, SIDE), f32),
            pltpu.VMEM((3, local_rows, groups, 2) + TILE, f32),
            pltpu.VMEM((3, local_rows, 2, groups) + TILE, f32),
            pltpu.VMEM((6, 3, SIDE, SIDE), f32),
            pltpu.VMEM((3, local_rows, 2, SIDE, SIDE), f32),
            pltpu.VMEM((local_rows, 5, 2, groups) + TILE, f32),
            pltpu.VMEM((local_rows, groups, 5, 2) + TILE, f32),
            pltpu.VMEM((5, 2, total_rows) + TILE, f32),
            chunk, lines, lines, chunk, final, final,
            dma((3,)), dma((3,)), dma((3,)), dma((local_rows, len(WEIGHT_GROUPS))), dma((6,)), dma((len(LEG_GROUPS),)),
            dma((local_rows,)), dma((SUBS,)), dma((SUBS,)), dma((11,)), dma((4,)),
        ],
        compiler_params=pltpu.CompilerParams(
            collective_id=0, has_side_effects=True, vmem_limit_bytes=60 * 1024 * 1024
        ),
        name="lens",
    )(band_cuts, sky_maps, filters, wiener, response, jnp.asarray(table), jnp.asarray(twiddle))


def solution(mesh):
    placed = (
        P("sims", "rows", "fields"),
        P(),
        P(None, ("rows", "fields"), None),
        P(None, ("rows", "fields"), None),
        P(("rows", "fields"), None),
    )
    rows_count, fields_count = mesh.shape["rows"], mesh.shape["fields"]
    groups = rows_count * fields_count

    def choose(sky_maps, *rest):
        fits = (
            NC == SIDE * SIDE
            and (mesh.shape["sims"], rows_count, fields_count) == (2, 4, 4)
            and NC // groups == TILE[0] * TILE[1]
            and sky_maps.shape[0] == 3
            and sky_maps.shape[1] * rows_count == 32
        )
        if fits:
            return fused_body(rows_count, fields_count, sky_maps, *rest)
        return body(sky_maps, *rest)

    return jax.shard_map(
        choose, mesh=mesh, in_specs=placed, out_specs=P("sims", "rows", "fields"), check_vma=False
    )
```

```python
import functools
import math

import jax
import jax.numpy as jnp
import numpy as np
from jax import lax
from jax.experimental import pallas as pl
from jax.experimental.pallas import tpu as pltpu
from jax.sharding import PartitionSpec as P

NC = 16384


exact_mode = lax.Precision.HIGHEST


def split_factor(length):
    best_first = 1
    for divisor in range(1, math.isqrt(length) + 1):
        if length % divisor == 0:
            best_first = divisor
    return (best_first, length // best_first)


def phase_table(left_index, right_index, period, direction):
    product = left_index[:, None] * right_index[None, :] % period
    angles = direction * 2.0 * math.pi / period * product.astype(jnp.float32)
    return (jnp.cos(angles), jnp.sin(angles))


def complex_einsum(formula, data_pair, table_pair):
    data_real, data_imag = data_pair
    table_real, table_imag = table_pair
    real_out = jnp.einsum(formula, data_real, table_real, precision=exact_mode)
    imag_out = jnp.einsum(formula, data_real, table_imag, precision=exact_mode)
    if data_imag is not None:
        real_out = real_out - jnp.einsum(formula, data_imag, table_imag, precision=exact_mode)
        imag_out = imag_out + jnp.einsum(formula, data_imag, table_real, precision=exact_mode)
    return (real_out, imag_out)


def complex_mul(left_pair, right_pair):
    return (
        left_pair[0] * right_pair[0] - left_pair[1] * right_pair[1],
        left_pair[0] * right_pair[1] + left_pair[1] * right_pair[0],
    )


def conj_mul(left_pair, right_pair):
    return (
        left_pair[0] * right_pair[0] + left_pair[1] * right_pair[1],
        left_pair[0] * right_pair[1] - left_pair[1] * right_pair[0],
    )


def row_transform(data_pair, direction):
    batch_len, length, block_width = data_pair[0].shape
    outer_len, inner_len = split_factor(length)
    outer_ids = jnp.arange(outer_len, dtype=jnp.int32)
    inner_ids = jnp.arange(inner_len, dtype=jnp.int32)
    real_in = data_pair[0].reshape(batch_len, outer_len, inner_len, block_width)
    imag_in = None
    if data_pair[1] is not None:
        imag_in = data_pair[1].reshape(batch_len, outer_len, inner_len, block_width)
    middle = complex_einsum(
        "bjmc,jk->bkmc", (real_in, imag_in), phase_table(outer_ids, outer_ids, outer_len, direction)
    )
    twiddle = phase_table(outer_ids, inner_ids, length, direction)
    middle = complex_mul(middle, (twiddle[0][None, :, :, None], twiddle[1][None, :, :, None]))
    result = complex_einsum(
        "bkmc,mq->bqkc", middle, phase_table(inner_ids, inner_ids, inner_len, direction)
    )
    norm_factor = 1.0 if direction < 0 else 1.0 / length
    return (
        result[0].reshape(batch_len, length, block_width) * norm_factor,
        result[1].reshape(batch_len, length, block_width) * norm_factor,
    )


def block_order(groups, fields_count):
    positions = jnp.arange(groups, dtype=jnp.int32)
    blocks = positions % fields_count * (groups // fields_count) + positions // fields_count
    return (positions, blocks)


def column_forward(data_pair, groups, fields_count):
    batch_len, local_rows, total_len = data_pair[0].shape
    block_width = total_len // groups
    positions, blocks = block_order(groups, fields_count)
    column_ids = jnp.arange(block_width, dtype=jnp.int32)
    shaped = (
        data_pair[0].reshape(batch_len, local_rows, groups, block_width),
        data_pair[1].reshape(batch_len, local_rows, groups, block_width),
    )
    middle = complex_einsum("brpc,pk->brkc", shaped, phase_table(blocks, positions, groups, -1.0))
    twiddle = phase_table(positions, column_ids, total_len, -1.0)
    middle = complex_mul(middle, (twiddle[0][None, None], twiddle[1][None, None]))
    result = complex_einsum(
        "brkc,cq->brqk", middle, phase_table(column_ids, column_ids, block_width, -1.0)
    )
    return (
        result[0].reshape(batch_len, local_rows, total_len),
        result[1].reshape(batch_len, local_rows, total_len),
    )


def column_inverse(data_pair, groups, fields_count):
    batch_len, local_rows, total_len = data_pair[0].shape
    block_width = total_len // groups
    positions, blocks = block_order(groups, fields_count)
    column_ids = jnp.arange(block_width, dtype=jnp.int32)
    shaped = (
        data_pair[0].reshape(batch_len, local_rows, block_width, groups),
        data_pair[1].reshape(batch_len, local_rows, block_width, groups),
    )
    middle = complex_einsum(
        "brqk,qc->brkc", shaped, phase_table(column_ids, column_ids, block_width, 1.0)
    )
    twiddle = phase_table(positions, column_ids, total_len, 1.0)
    middle = complex_mul(middle, (twiddle[0][None, None], twiddle[1][None, None]))
    result = complex_einsum("brkc,kp->brpc", middle, phase_table(positions, blocks, groups, 1.0))
    norm_factor = 1.0 / total_len
    return (
        result[0].reshape(batch_len, local_rows, total_len) * norm_factor,
        result[1].reshape(batch_len, local_rows, total_len) * norm_factor,
    )


def body(sky_maps, band_cuts, filters, wiener, response):
    rows_count = lax.axis_size("rows")
    fields_count = lax.axis_size("fields")
    groups = rows_count * fields_count
    local_rows = filters.shape[1]
    total_rows = local_rows * groups
    row_ratio = NC // total_rows

    def forward_columns(stacked):
        return jnp.stack(column_forward((stacked[0], stacked[1]), groups, fields_count))

    def inverse_rows(stacked):
        return jnp.stack(row_transform((stacked[0], stacked[1]), 1.0))

    def inverse_columns(stacked):
        return jnp.stack(column_inverse((stacked[0], stacked[1]), groups, fields_count))

    def to_frequency(stacked):
        batch_len = stacked.shape[1]
        block_width = stacked.shape[3]
        shaped = stacked.reshape(
            2, batch_len, rows_count, fields_count, local_rows, 1, 1, block_width
        )
        arrived = lax.all_to_all(
            lax.all_to_all(shaped, "rows", split_axis=2, concat_axis=5, tiled=True),
            "fields",
            split_axis=3,
            concat_axis=6,
            tiled=True,
        )
        result = forward_columns(arrived.reshape(2, batch_len, local_rows, groups * block_width))
        return result

    def to_space(stacked):
        batch_len = stacked.shape[1]
        block_width = stacked.shape[3] // groups
        shaped = stacked.reshape(
            2, batch_len, 1, 1, local_rows, rows_count, fields_count, block_width
        )
        arrived = lax.all_to_all(
            lax.all_to_all(shaped, "rows", split_axis=5, concat_axis=2, tiled=True),
            "fields",
            split_axis=6,
            concat_axis=3,
            tiled=True,
        )
        result = inverse_rows(arrived.reshape(2, batch_len, total_rows, block_width))
        return result

    slab_spectra = jnp.stack(
        row_transform(
            (lax.all_to_all(sky_maps, "rows", split_axis=2, concat_axis=1, tiled=True), None), -1.0
        )
    )
    sky_spectra = to_frequency(slab_spectra)
    row_ids = lax.axis_index(("rows", "fields")) * local_rows + jnp.arange(
        local_rows, dtype=jnp.int32
    )
    freq_rows = jnp.where(row_ids < total_rows // 2, row_ids, row_ids - total_rows)[:, None]
    column_ids = jnp.arange(NC, dtype=jnp.int32)
    freq_cols = jnp.where(column_ids < NC // 2, column_ids, column_ids - NC)[None, :]
    scaled_rows = row_ratio * freq_rows
    radius_sq = freq_cols * freq_cols + scaled_rows * scaled_rows

    def band_mask(lower_cut, upper_cut):
        inside = (radius_sq >= lower_cut * lower_cut) & (radius_sq <= upper_cut * upper_cut)
        return inside.astype(jnp.float32)

    mask_temp = band_mask(band_cuts[0], band_cuts[1])
    mask_pol = band_mask(band_cuts[2], band_cuts[3])
    mask_out = band_mask(band_cuts[4], band_cuts[5])
    radius_floor = jnp.maximum(radius_sq, 1).astype(jnp.float32)
    cos_two = (freq_cols * freq_cols - scaled_rows * scaled_rows).astype(jnp.float32) / radius_floor
    sin_two = (2 * freq_cols * scaled_rows).astype(jnp.float32) / radius_floor
    along_x = (2 * freq_cols).astype(jnp.float32) / NC
    along_y = (2 * freq_rows).astype(jnp.float32) / total_rows
    raising = (-along_y + 0.0 * along_x, along_x + 0.0 * along_y)
    lowering = (along_y + 0.0 * along_x, along_x + 0.0 * along_y)
    rotation = (cos_two, sin_two)
    temp_modes = (sky_spectra[0, 0], sky_spectra[1, 0])
    stokes_q = (sky_spectra[0, 1], sky_spectra[1, 1])
    stokes_u = (sky_spectra[0, 2], sky_spectra[1, 2])
    e_modes = (
        -(cos_two * stokes_q[0] + sin_two * stokes_u[0]),
        -(cos_two * stokes_q[1] + sin_two * stokes_u[1]),
    )
    b_modes = (
        sin_two * stokes_q[0] - cos_two * stokes_u[0],
        sin_two * stokes_q[1] - cos_two * stokes_u[1],
    )
    temp_weight = mask_temp * filters[0]
    e_weight = mask_pol * filters[1]
    b_weight = mask_pol * filters[2]
    temp_bar = (temp_weight * temp_modes[0], temp_weight * temp_modes[1])
    e_bar = (e_weight * e_modes[0], e_weight * e_modes[1])
    b_bar = (b_weight * b_modes[0], b_weight * b_modes[1])
    grad_temp = complex_mul(raising, (wiener[0] * temp_bar[0], wiener[0] * temp_bar[1]))
    pol_sum = complex_mul((e_bar[0] - b_bar[1], e_bar[1] + b_bar[0]), rotation)
    pol_bar = (-pol_sum[0], -pol_sum[1])
    pol_rot = complex_mul((wiener[1] * e_bar[0], wiener[1] * e_bar[1]), rotation)
    pol_wiener = (-pol_rot[0], -pol_rot[1])
    spin_three = complex_mul(raising, pol_wiener)
    spin_one = complex_mul(lowering, pol_wiener)
    leg_spectra = jnp.stack(
        [
            jnp.stack([temp_bar[0], grad_temp[0], pol_bar[0], spin_three[0], spin_one[0]]),
            jnp.stack([temp_bar[1], grad_temp[1], pol_bar[1], spin_three[1], spin_one[1]]),
        ]
    )
    leg_maps = to_space(inverse_columns(leg_spectra))
    temp_leg = (leg_maps[0, 0], leg_maps[1, 0])
    grad_leg = (leg_maps[0, 1], leg_maps[1, 1])
    pol_leg = (leg_maps[0, 2], leg_maps[1, 2])
    three_leg = (leg_maps[0, 3], leg_maps[1, 3])
    one_leg = (leg_maps[0, 4], leg_maps[1, 4])
    temp_term = complex_mul(temp_leg, grad_leg)
    raise_term = conj_mul(pol_leg, three_leg)
    lower_term = conj_mul(one_leg, pol_leg)
    current = (
        temp_term[0] + 0.5 * (raise_term[0] + lower_term[0]),
        temp_term[1] + 0.5 * (raise_term[1] + lower_term[1]),
    )
    current_rows = jnp.stack(row_transform((current[0][None], current[1][None]), -1.0))
    current_modes = to_frequency(current_rows)
    out_weight = mask_out * response
    estimate_modes = complex_mul(
        lowering, (out_weight * current_modes[0, 0], out_weight * current_modes[1, 0])
    )
    estimate_stack = jnp.stack([estimate_modes[0][None], estimate_modes[1][None]])
    estimate_maps = to_space(inverse_columns(estimate_stack))
    slab_result = estimate_maps[:, 0]
    return lax.all_to_all(slab_result, "rows", split_axis=1, concat_axis=2, tiled=True)


SIDE = 128
TILE = (8, 128)
LEG_GROUPS = ((0, 2), (2, 2), (4, 1))
WEIGHT_GROUPS = ((0, 3), (1, 4), (2,), (5,))
MESH = pl.DeviceIdType.MESH


def add_pair(a, b):
    imag = a[1] if b[1] is None else b[1] if a[1] is None else a[1] + b[1]
    return (a[0] + b[0], imag)


def sub_pair(a, b):
    imag = a[1] if b[1] is None else -b[1] if a[1] is None else a[1] - b[1]
    return (a[0] - b[0], imag)


def turn_pair(value, step, length, direction):
    real, imag = value
    if step == 0:
        return value
    if 4 * step == length:
        if imag is None:
            return (jnp.zeros_like(real), real if direction > 0 else -real)
        return (-imag, real) if direction > 0 else (imag, -real)
    angle = 2.0 * math.pi * step / length
    c, s = math.cos(angle), direction * math.sin(angle)
    if imag is None:
        return (real * c, real * s)
    if 8 * step == length:
        if direction > 0:
            return ((real - imag) * c, (real + imag) * c)
        return ((real + imag) * c, (imag - real) * c)
    if 8 * step == 3 * length:
        if direction > 0:
            return ((real + imag) * c, (imag - real) * c)
        return ((real - imag) * c, (real + imag) * c)
    return (real * c - imag * s, real * s + imag * c)


def short_transform(values, direction):
    length = len(values)
    if length == 1:
        return values
    even = short_transform(values[0::2], direction)
    odd = short_transform(values[1::2], direction)
    low, high = [], []
    for step in range(length // 2):
        turned = turn_pair(odd[step], step, length, direction)
        low.append(add_pair(even[step], turned))
        high.append(sub_pair(even[step], turned))
    return low + high


def split_number(x):
    top = x.astype(jnp.bfloat16)
    return top, (x - top.astype(jnp.float32)).astype(jnp.bfloat16)


def dot32(a, b):
    return jnp.dot(a, b, preferred_element_type=jnp.float32)


def matrix_left(table_ref, which, x):
    top, rest = split_number(x)
    m_top, m_rest = table_ref[which, 0], table_ref[which, 1]
    return dot32(m_top, top) + (dot32(m_top, rest) + dot32(m_rest, top))


def matrix_right(table_ref, which, x):
    top, rest = split_number(x)
    m_top, m_rest = table_ref[which, 0], table_ref[which, 1]
    return dot32(top, m_top) + (dot32(top, m_rest) + dot32(rest, m_top))


BITS = (0, 1)
SUBS = 2
OFFSETS = [
    (c, a1, e, a0) for a0 in BITS for c, a1, e in
    ((1, 1, 1), (1, 0, 0), (0, 1, 0), (0, 0, 1), (1, 1, 0), (0, 1, 1), (1, 0, 1), (0, 0, 0))
]
PEERS = sorted((offset for offset in OFFSETS if any(offset)), key=lambda offset: -sum(offset[:3]))
WEIGHT_ORDER = (0, 3, 1, 4, 2, 5)


def lens_kernel(
    cuts_ref, sky_hbm, filters_hbm, wiener_hbm, response_hbm, table_hbm, twiddle_hbm, out_ref,
    table_ref, twiddle_ref, sky_ref, raw, weight_ref, slab_out, slab_in, relay_buf, relay_weights, spec_out, spec_in, weights, modes, legs_out, legs_in,
    maps, cur_out, cur_in, est_out, est_in, fin_out, fin_in,
    slab_sem, relay_sem, spec_sem, weight_sem, hand_sem, legs_sem, cur_sem, est_sem, fin_sem, send_sem, load_sem,
):
    rows_count, fields_count, local_rows = 4, 4, 2
    groups = rows_count * fields_count
    total_rows = groups * local_rows
    in_rows = total_rows // rows_count
    row_ratio = NC // total_rows
    my_x, my_r, my_z = (lax.axis_index(name) for name in ("sims", "rows", "fields"))
    my_y, my_c, my_h, my_l = my_r // 2, my_r % 2, my_z // 2, my_z % 2
    x_at, y_at, c_at, h_at, l_at = ((bit, 1 - bit) for bit in (my_x, my_y, my_c, my_h, my_l))
    me = my_r * fields_count + 2 * my_x + my_l
    my_block = (2 * my_x + my_l) * rows_count + my_r
    stays = my_x == my_h

    outer = my_l == my_h
    inner = my_l != my_h
    home_row = in_rows * my_r + 4 * my_h + 2 * my_l + my_x

    def signed(row):
        return jnp.where(row < total_rows // 2, row, row - total_rows)

    def row_of(offset):
        return 2 * y_at[offset[1]] + c_at[offset[3]]

    def peer_of(offset):
        return row_of(offset) * fields_count + 2 * x_at[offset[0]] + l_at[offset[2]]

    def peer_block(offset):
        return (2 * x_at[offset[0]] + l_at[offset[2]]) * rows_count + row_of(offset)

    def remote(src, dst, sems, x, r, z):
        return pltpu.make_async_remote_copy(
            src_ref=src, dst_ref=dst, send_sem=sems[0], recv_sem=sems[1],
            device_id={"sims": x, "rows": r, "fields": z}, device_id_type=MESH,
        )

    def send(offset, src, dst, sems):
        return remote(src, dst, sems, x_at[offset[0]], row_of(offset), 2 * my_h + l_at[offset[2]])

    def send_home(offset, src, dst, sems):
        return remote(src, dst, sems, my_h, row_of(offset), 2 * x_at[offset[0]] + l_at[offset[2]])

    def each_peer(body):
        for offset in PEERS:
            body(offset)

    def wait_all(ref, sem):
        pltpu.make_async_copy(ref, ref, sem).wait()

    for src, dst, n in (
        (sky_hbm, sky_ref, 0),
        (filters_hbm, raw.at[0:3], 1),
        (wiener_hbm, raw.at[3:5], 1),
        (response_hbm, raw.at[5], 1),
        (table_hbm, table_ref, 2),
        (twiddle_hbm, twiddle_ref, 3),
    ):
        pltpu.make_async_copy(src, dst, load_sem.at[n]).start()

    (
        slab_left, relay_left, forward_left, spec_left, weight_left, legs_left, cur_left, est_left, fin_left,
        extra_left, pass_left,
    ) = (send_sem.at[n] for n in range(11))

    barrier = pltpu.get_barrier_semaphore()
    for h in BITS:
        for c, a1, e, a0 in OFFSETS:
            if h or c or a1 or e or a0:
                pl.semaphore_signal(
                    barrier, inc=1, device_id_type=MESH,
                    device_id={"sims": x_at[c], "rows": 2 * y_at[a1] + c_at[a0], "fields": 2 * h_at[h] + l_at[e]},
                )
    wait_all(sky_ref, load_sem.at[0])
    tiles = sky_ref.shape[2] // SIDE
    for field in range(3):
        for t in range(tiles):
            slab_out[t // 8, field, :, t % 8, :] = sky_ref[field, :, t * SIDE:(t + 1) * SIDE]
    pl.semaphore_wait(barrier, 2 * groups - 1)

    ROW_OFFSETS = [(0, a1, 0, a0) for a1 in BITS for a0 in BITS]

    def slab_copy(field, offset):
        r = row_of(offset)
        return send_home(
            offset, slab_out.at[r, field], slab_in.at[my_r, field],
            (slab_left, slab_sem.at[field]),
        )

    def own_slab(field):
        return pltpu.make_async_copy(slab_out.at[my_r, field], slab_in.at[my_r, field], slab_sem.at[field])

    def relay_copy(field):
        return remote(
            slab_out.at[pl.ds(2 * y_at[1], 2), field], relay_buf.at[field],
            (relay_left, relay_sem.at[field]), x_at[1], my_r, my_z,
        )

    def forward_copy(field, core):
        a0 = core
        return remote(
            relay_buf.at[field, c_at[a0]], slab_in.at[my_r, field],
            (forward_left, slab_sem.at[field]),
            my_x, 2 * y_at[1] + c_at[a0], 2 * h_at[1] + my_l,
        )

    @pl.when(stays)
    def _():
        for field in range(3):
            own_slab(field).start()
            for offset in ROW_OFFSETS[1:]:
                slab_copy(field, offset).start()

    def slab_start(field):
        relay_copy(field).start()
        for offset in ROW_OFFSETS[:2]:
            slab_copy(field, offset).start()

    @pl.when(jnp.logical_not(stays))
    def _():
        slab_start(0)

    low_index = lax.broadcasted_iota(jnp.int32, (SIDE, SIDE), 0)
    high_index = lax.broadcasted_iota(jnp.int32, (SIDE, SIDE), 1)
    column_ids = low_index + SIDE * high_index
    freq_cols = jnp.where(column_ids < NC // 2, column_ids, column_ids - NC)

    def row_frequency(row):
        return signed(in_rows * my_r + 4 * my_l + 2 * (my_h + row - 2 * my_h * row) + my_x)

    wait_all(raw, load_sem.at[1])

    def spread(n, carry):
        for j in range(8):
            start = pl.multiple_of((n * 8 + j) * SIDE, SIDE)
            weight_ref[:, :, n * 8 + j, :] = raw[:, :, pl.ds(start, SIDE)]
        return carry

    lax.fori_loop(0, SIDE // 8, spread, 0)
    scaled_home = row_ratio * signed(home_row)
    radius_home = freq_cols * freq_cols + scaled_home * scaled_home

    def mask(n):
        low, high = cuts_ref[2 * n], cuts_ref[2 * n + 1]
        inside = (radius_home >= low * low) & (radius_home <= high * high)
        return inside.astype(jnp.float32)

    home_slot = jnp.where(inner, 2, 0)

    def group_of(n):
        return [n in members for members in WEIGHT_GROUPS].index(True)

    def across(n, source, slot, left):
        return remote(
            source, weights.at[n, slot], (left, weight_sem.at[slot, group_of(n)]),
            my_x, my_r, 2 * h_at[1] + my_h,
        )

    def own_weight(n):
        return across(n, weights.at[n, home_slot], 0, weight_left)

    def near_copy(n):
        return remote(
            weights.at[n, home_slot], weights.at[n, 1], (extra_left, weight_sem.at[1, group_of(n)]),
            my_x, my_r, 2 * my_h + l_at[1],
        )

    def hand_copy(n):
        return remote(
            weights.at[n, home_slot], relay_weights.at[n], (weight_left, hand_sem.at[n]),
            my_x, my_r, 2 * my_h + l_at[1],
        )

    def weight_pass_on(members):
        @pl.when(inner)
        def _():
            for n in members:
                wait_all(relay_weights.at[n], hand_sem.at[n])
                across(n, relay_weights.at[n], 1, pass_left).start()

    pol = mask(1)
    weights[0, home_slot] = mask(0) * weight_ref[0, my_x].T
    weights[1, home_slot] = pol * weight_ref[1, my_x].T
    weights[2, home_slot] = pol * weight_ref[2, my_x].T
    weights[3, home_slot] = weight_ref[3, my_x].T
    weights[4, home_slot] = weight_ref[4, my_x].T
    weights[5, home_slot] = mask(2) * weight_ref[5, my_x].T
    @pl.when(jnp.logical_and(inner, jnp.logical_not(stays)))
    def _():
        slab_start(1)
        slab_start(2)
        for n in WEIGHT_ORDER[:5]:
            near_copy(n).start()
            own_weight(n).start()

    @pl.when(jnp.logical_and(outer, jnp.logical_not(stays)))
    def _():
        hand_copy(0).start()
        slab_start(1)
        hand_copy(3).start()
        slab_start(2)
        hand_copy(1).start()

    @pl.when(jnp.logical_and(inner, stays))
    def _():
        own_weight(0).start()
        for n in WEIGHT_ORDER[:5]:
            near_copy(n).start()

    @pl.when(jnp.logical_and(outer, stays))
    def _():
        hand_copy(0).start()
        hand_copy(3).start()

    def place(k, half):
        return 1 - half if k // 2 % 2 else half, k // in_rows * fields_count + 2 * (k % 2) + k // 4 % 2

    def spec_copy(field, row, offset):
        return send(
            offset, spec_out.at[field, row, peer_of(offset)], spec_in.at[field, row, :, my_block],
            (spec_left, spec_sem.at[field]),
        )

    def own_spec(field, row):
        return pltpu.make_async_copy(
            spec_out.at[field, row, me], spec_in.at[field, row, :, my_block], spec_sem.at[field]
        )

    def spec_start(field):
        for row in range(local_rows):
            each_peer(lambda offset: spec_copy(field, row, offset).start())
            own_spec(field, row).start()

    def row_step(field):
        @pl.when(stays)
        def _():
            wait_all(relay_buf.at[field], relay_sem.at[field])
            for core in BITS:
                forward_copy(field, core).start()

        if field == 1:
            @pl.when(jnp.logical_and(outer, stays))
            def _():
                hand_copy(1).start()

        if field == 2:
            @pl.when(jnp.logical_and(inner, stays))
            def _():
                for n in WEIGHT_ORDER[1:5]:
                    own_weight(n).start()

        wait_all(slab_in.at[:, field], slab_sem.at[field])
        values = [
            (slab_in[y // in_rows, field, y % in_rows], None) for y in range(total_rows)
        ]
        for k, (real, imag) in enumerate(short_transform(values, -1)):
            local, device = place(k, my_h)
            spec_out[field, local, device, 0] = real
            spec_out[field, local, device, 1] = jnp.zeros_like(real) if imag is None else imag
        spec_start(field)

    for field in range(3):
        row_step(field)

    @pl.when(outer)
    def _():
        hand_copy(4).start()
        hand_copy(2).start()

    weight_pass_on((0, 3, 1))

    cos_f, sin_f, cos_b, sin_b = 0, 1, 2, 3

    def side_by_side(pieces, axis):
        return pieces[0] if len(pieces) == 1 else jnp.concatenate(pieces, axis=axis)

    def long_forward(pieces):
        y = matrix_left(table_ref, 0, side_by_side(pieces, 1))
        c, s = twiddle_ref[cos_f], twiddle_ref[sin_f]
        turned = []
        for n in range(len(pieces)):
            yr, yi = y[:SIDE, n * SIDE:(n + 1) * SIDE], y[SIDE:, n * SIDE:(n + 1) * SIDE]
            turned.append(jnp.concatenate([yr * c - yi * s, yr * s + yi * c], axis=1))
        z = matrix_right(table_ref, 1, side_by_side(turned, 0))
        return [
            (z[n * SIDE:(n + 1) * SIDE, :SIDE], z[n * SIDE:(n + 1) * SIDE, SIDE:])
            for n in range(len(pieces))
        ]

    def long_inverse(pairs):
        stacks = [jnp.concatenate([pair[0], pair[1]], axis=1) for pair in pairs]
        u = matrix_right(table_ref, 0, side_by_side(stacks, 0))
        c, s = twiddle_ref[cos_b], twiddle_ref[sin_b]
        turned = []
        for n in range(len(pairs)):
            ur, ui = u[n * SIDE:(n + 1) * SIDE, :SIDE], u[n * SIDE:(n + 1) * SIDE, SIDE:]
            turned.append(jnp.concatenate([ur * c - ui * s, ur * s + ui * c], axis=0))
        x = matrix_left(table_ref, 1, side_by_side(turned, 1))
        return [
            x[:, n * SIDE:(n + 1) * SIDE].reshape((2, groups) + TILE)
            for n in range(len(pairs))
        ]

    def legs_copy(row, g, offset):
        first, count = LEG_GROUPS[g]
        return send(
            offset, legs_out.at[row, first:first + count, :, peer_block(offset)],
            legs_in.at[row, me, first:first + count],
            (legs_left, legs_sem.at[g]),
        )

    def own_legs(row, g):
        first, count = LEG_GROUPS[g]
        return pltpu.make_async_copy(
            legs_out.at[row, first:first + count, :, my_block],
            legs_in.at[row, me, first:first + count],
            legs_sem.at[g],
        )

    def wait_weights(group, row):
        members = WEIGHT_GROUPS[group]

        @pl.when(jnp.logical_or(row == 1, inner))
        def _():
            wait_all(weights.at[0:len(members), row], weight_sem.at[row, group])

    def slopes(row):
        along_x = (2 * freq_cols).astype(jnp.float32) / NC
        along_y = (2 * row_frequency(row)).astype(jnp.float32) / total_rows
        return along_x, along_y

    def both_rows(field):
        wait_all(spec_in.at[field], spec_sem.at[field])
        pairs = long_forward([spec_in[field, row].reshape(2 * SIDE, SIDE) for row in range(local_rows)])
        for row, pair in enumerate(pairs):
            modes[field, row, 0], modes[field, row, 1] = pair

    def leg_step(n, row):
        scaled = row_ratio * row_frequency(row)
        radius_sq = freq_cols * freq_cols + scaled * scaled
        floor = jnp.maximum(radius_sq, 1).astype(jnp.float32)
        cos2 = (freq_cols * freq_cols - scaled * scaled).astype(jnp.float32) / floor
        sin2 = (2 * freq_cols * scaled).astype(jnp.float32) / floor
        along_x, along_y = slopes(row)
        raising, lowering = (-along_y, along_x), (along_y, along_x)
        rot = (cos2, sin2)

        def temp_legs():
            t_bar = (weights[0, row] * modes[0, row, 0], weights[0, row] * modes[0, row, 1])
            return t_bar, complex_mul((weights[3, row] * t_bar[0], weights[3, row] * t_bar[1]), raising)

        def e_modes():
            return tuple(
                -weights[1, row] * (cos2 * modes[1, row, n] + sin2 * modes[2, row, n]) for n in range(2)
            )

        def spin_legs():
            e_bar = e_modes()
            w = complex_mul((-weights[4, row] * e_bar[0], -weights[4, row] * e_bar[1]), rot)
            return complex_mul(w, raising), complex_mul(w, lowering)

        def pol_leg():
            e_bar = e_modes()
            b_bar = tuple(
                weights[2, row] * (sin2 * modes[1, row, n] - cos2 * modes[2, row, n]) for n in range(2)
            )
            return (complex_mul((b_bar[1] - e_bar[0], -(e_bar[1] + b_bar[0])), rot),)

        wait_weights(n, row)
        for k, leg_map in enumerate(long_inverse((temp_legs, spin_legs, pol_leg)[n]())):
            legs_out[row, LEG_GROUPS[n][0] + k] = leg_map
        each_peer(lambda offset: legs_copy(row, n, offset).start())
        own_legs(row, n).start()

    wait_all(table_ref, load_sem.at[2])
    wait_all(twiddle_ref, load_sem.at[3])
    both_rows(0)

    @pl.when(outer)
    def _():
        leg_step(0, 0)
        leg_step(0, 1)

    both_rows(1)
    both_rows(2)
    weight_pass_on((4, 2))

    @pl.when(inner)
    def _():
        leg_step(0, 0)

    def later_steps(row, carry):
        @pl.when(jnp.logical_and(inner, row == 1))
        def _():
            leg_step(0, 1)

        leg_step(1, row)
        leg_step(2, row)
        return carry

    lax.fori_loop(0, local_rows, later_steps, 0)

    @pl.when(inner)
    def _():
        own_weight(5).start()

    @pl.when(outer)
    def _():
        across(5, weights.at[5, 0], 1, weight_left).start()

    def map_step(n, carry):
        values = [
            (legs_in[place(k, my_h) + (n, 0)], legs_in[place(k, my_h) + (n, 1)])
            for k in range(total_rows)
        ]
        for y, (real, imag) in enumerate(short_transform(values, 1)):
            maps[n, 0, y] = real
            maps[n, 1, y] = imag
        return carry

    for g, (first, count) in enumerate(LEG_GROUPS):
        wait_all(legs_in.at[:, :, first:first + count], legs_sem.at[g])
        lax.fori_loop(first, first + count, map_step, 0)

    def product(y):
        a, g, h3, h1, p = [(maps[n, 0, y], maps[n, 1, y]) for n in range(5)]
        ag, ph, hp = complex_mul(a, g), conj_mul(p, h3), conj_mul(h1, p)
        return ag[0] + 0.5 * (ph[0] + hp[0]), ag[1] + 0.5 * (ph[1] + hp[1])

    values = [product(y) for y in range(total_rows)]
    for k, (real, imag) in enumerate(short_transform(values, -1)):
        cur_out[place(k, my_h) + (0,)] = real
        cur_out[place(k, my_h) + (1,)] = imag

    def cur_copy(row, offset):
        return send(
            offset, cur_out.at[row, peer_of(offset)], cur_in.at[row, :, my_block],
            (cur_left, cur_sem.at[row]),
        )

    def own_cur(row):
        return pltpu.make_async_copy(
            cur_out.at[row, me], cur_in.at[row, :, my_block], cur_sem.at[row]
        )

    def cur_start(row, carry):
        each_peer(lambda offset: cur_copy(row, offset).start())
        own_cur(row).start()
        return carry

    for row in range(local_rows):
        cur_start(row, 0)

    @pl.when(inner)
    def _():
        near_copy(5).start()


    HOME_OFFSETS = sorted(PEERS, key=lambda offset: -offset[0])
    ORIGIN = (0, 0, 0, 0)

    def part_of(sub):
        return slice(sub * TILE[0] // SUBS, (sub + 1) * TILE[0] // SUBS)

    def est_copy(row, offset, sub):
        r, z = row_of(offset), 2 * h_at[offset[0]] + l_at[offset[2]]
        return remote(
            est_out.at[row, :, z * rows_count + r, part_of(sub)], est_in.at[row, me, :, part_of(sub)],
            (est_left, est_sem.at[sub]), my_h, r, z,
        )

    def own_est(row, sub):
        return pltpu.make_async_copy(
            est_out.at[row, :, my_z * rows_count + my_r, part_of(sub)], est_in.at[row, me, :, part_of(sub)],
            est_sem.at[sub],
        )

    def est_start(row, sub):
        for offset in HOME_OFFSETS:
            est_copy(row, offset, sub).start()

        @pl.when(stays)
        def _():
            own_est(row, sub).start()

        @pl.when(jnp.logical_not(stays))
        def _():
            est_copy(row, ORIGIN, sub).start()

    def estimate_step(row):
        wait_all(cur_in.at[row], cur_sem.at[row])
        wait_weights(3, row)
        (modes,) = long_forward([cur_in[row].reshape(2 * SIDE, SIDE)])
        along_x, along_y = slopes(row)
        w = weights[5, row]
        estimate = complex_mul((w * modes[0], w * modes[1]), (along_y, along_x))
        (est_out[row],) = long_inverse([estimate])
        est_start(row, 0)

    for row in range(local_rows):
        estimate_step(row)
    for sub in range(1, SUBS):
        for row in range(local_rows):
            est_start(row, sub)

    def fin_copy(offset, sub):
        r = row_of(offset)
        return remote(
            fin_out.at[r, :, :, part_of(sub)], fin_in.at[my_r, :, :, part_of(sub)],
            (fin_left, fin_sem.at[sub]), my_x, r, my_z,
        )

    def own_fin(sub):
        return pltpu.make_async_copy(
            fin_out.at[my_r, :, :, part_of(sub)], fin_in.at[my_r, :, :, part_of(sub)], fin_sem.at[sub]
        )

    for sub in range(SUBS):
        wait_all(est_in.at[:, :, :, part_of(sub)], est_sem.at[sub])
        values = []
        for k in range(total_rows):
            local, device = place(k, my_x)
            values.append(tuple(est_in[local, device, part, part_of(sub)] for part in range(2)))
        for y, pair in enumerate(short_transform(values, 1)):
            for part in range(2):
                fin_out[y // in_rows, part, y % in_rows, part_of(sub)] = pair[part]
        for offset in ROW_OFFSETS[1:]:
            fin_copy(offset, sub).start()
        own_fin(sub).start()

    others = groups - 1

    @pl.when(stays)
    def _():
        wait_all(slab_out.at[0:3], slab_left)
        wait_all(relay_buf, forward_left)
        wait_all(est_out.at[:, :, 0:others], est_left)

    @pl.when(jnp.logical_not(stays))
    def _():
        wait_all(slab_out.at[0:2], slab_left)
        wait_all(relay_buf, relay_left)
        wait_all(est_out, est_left)

    @pl.when(inner)
    def _():
        wait_all(relay_weights.at[0:5], pass_left)
        wait_all(relay_weights, extra_left)

    wait_all(weights.at[:, 0], weight_left)
    wait_all(spec_out.at[:, :, 0:others], spec_left)
    wait_all(legs_out.at[:, :, :, 0:others], legs_left)
    wait_all(cur_out.at[:, 0:others], cur_left)
    for sub in range(SUBS):
        wait_all(fin_in.at[:, :, :, part_of(sub)], fin_sem.at[sub])
        for part in range(2):
            for t in range(tiles):
                if t % TILE[0] * SUBS // TILE[0] == sub:
                    out_ref[part, :, t * SIDE:(t + 1) * SIDE] = fin_in[t // TILE[0], part, :, t % TILE[0], :]

    wait_all(fin_out.at[0:3], fin_left)


def long_tables(total_rows):
    index = np.arange(SIDE)
    angle = 2.0 * np.pi * (index[:, None] * index[None, :] % SIDE) / SIDE
    c, s = np.cos(angle), np.sin(angle)
    forward = np.block([[c, s], [-s, c]]).astype(np.float32)
    tables = np.stack([forward, forward.T])
    top = tables.astype(jnp.bfloat16)
    rest = (tables - top.astype(np.float32)).astype(jnp.bfloat16)
    turn = 2.0 * np.pi * (index[:, None] * index[None, :]) / NC
    scale = 1.0 / (NC * total_rows)
    twiddle = np.stack(
        [np.cos(turn), -np.sin(turn), scale * np.cos(turn), scale * np.sin(turn)]
    ).astype(np.float32)
    return np.stack([top, rest], axis=1), twiddle


def fused_body(rows_count, fields_count, sky_maps, band_cuts, filters, wiener, response):
    groups = rows_count * fields_count
    local_rows = response.shape[0]
    total_rows = local_rows * groups
    in_rows = total_rows // rows_count
    table, twiddle = long_tables(total_rows)
    vmem = pl.BlockSpec(memory_space=pltpu.VMEM)
    f32 = jnp.float32
    dma = pltpu.SemaphoreType.DMA
    slab = pltpu.VMEM((rows_count, 3, in_rows) + TILE, f32)
    chunk = pltpu.VMEM((local_rows, groups, 2) + TILE, f32)
    lines = pltpu.VMEM((local_rows, 2, groups) + TILE, f32)
    final = pltpu.VMEM((rows_count, 2, in_rows) + TILE, f32)
    return pl.pallas_call(
        lens_kernel,
        out_shape=jax.ShapeDtypeStruct((2,) + sky_maps.shape[1:], f32),
        in_specs=[pl.BlockSpec(memory_space=pltpu.SMEM)] + [pl.BlockSpec(memory_space=pl.ANY)] * 6,
        out_specs=vmem,
        scratch_shapes=[
            pltpu.VMEM(table.shape, table.dtype), pltpu.VMEM(twiddle.shape, f32),
            pltpu.VMEM(sky_maps.shape, f32),
            pltpu.VMEM((6, local_rows, NC), f32),
            pltpu.VMEM((6, local_rows, SIDE, SIDE), f32),
            slab, slab,
            pltpu.VMEM((3, 2, in_rows) + TILE, f32),
            pltpu.VMEM((6, SIDE, SIDE), f32),
            pltpu.VMEM((3, local_rows, groups, 2) + TILE, f32),
            pltpu.VMEM((3, local_rows, 2, groups) + TILE, f32),
            pltpu.VMEM((6, 3, SIDE, SIDE), f32),
            pltpu.VMEM((3, local_rows, 2, SIDE, SIDE), f32),
            pltpu.VMEM((local_rows, 5, 2, groups) + TILE, f32),
            pltpu.VMEM((local_rows, groups, 5, 2) + TILE, f32),
            pltpu.VMEM((5, 2, total_rows) + TILE, f32),
            chunk, lines, lines, chunk, final, final,
            dma((3,)), dma((3,)), dma((3,)), dma((local_rows, len(WEIGHT_GROUPS))), dma((6,)), dma((len(LEG_GROUPS),)),
            dma((local_rows,)), dma((SUBS,)), dma((SUBS,)), dma((11,)), dma((4,)),
        ],
        compiler_params=pltpu.CompilerParams(
            collective_id=0, has_side_effects=True, vmem_limit_bytes=60 * 1024 * 1024
        ),
        name="lens",
    )(band_cuts, sky_maps, filters, wiener, response, jnp.asarray(table), jnp.asarray(twiddle))


def solution(mesh):
    placed = (
        P("sims", "rows", "fields"),
        P(),
        P(None, ("rows", "fields"), None),
        P(None, ("rows", "fields"), None),
        P(("rows", "fields"), None),
    )
    rows_count, fields_count = mesh.shape["rows"], mesh.shape["fields"]
    groups = rows_count * fields_count

    def choose(sky_maps, *rest):
        fits = (
            NC == SIDE * SIDE
            and (mesh.shape["sims"], rows_count, fields_count) == (2, 4, 4)
            and NC // groups == TILE[0] * TILE[1]
            and sky_maps.shape[0] == 3
            and sky_maps.shape[1] * rows_count == 32
        )
        if fits:
            return fused_body(rows_count, fields_count, sky_maps, *rest)
        return body(sky_maps, *rest)

    return jax.shard_map(
        choose, mesh=mesh, in_specs=placed, out_specs=P("sims", "rows", "fields"), check_vma=False
    )
```
